32 devices in a mesh: seq: 8 (over z, y), frame: 4 (over x, core).
Axes of the slice: x: 2, y: 2, z: 4, core: 2. Of those that a mesh axis runs over, the one named last changes fastest.
Arguments:
- patches: bfloat16 [3072, 1280], P('frame'), may hold values from -4 to 4
- vit_gain: float32 [1280], replicated, may hold values from 0.5 to 1.5
- vision_qkv: bfloat16 [1280, 3840], P(None, 'seq')
- vision_out: bfloat16 [1280, 1280], P('seq'), may hold values from -0.15625 to 0.15625
- video_ids: int32 [768], replicated, may hold values from 0 to 2, never falling along the last dimension, each value on 1 to 480 neighbouring positions
- merge_gain: float32 [1280], replicated, may hold values from 0.5 to 1.5
- merge_up: bfloat16 [5120, 5120], P(None, 'seq'), may hold values from -0.078125 to 0.078125
- merge_down: bfloat16 [5120, 8192], P('seq')
- vision_pos: int32 [768], replicated, may hold values from 0 to 4095, as said below
- text_embed: bfloat16 [4096, 8192], P(('seq', 'frame')), may hold values from -6 to 6
- llm_gain: float32 [8192], replicated, may hold values from 0.5 to 1.5
- query_weight: bfloat16 [8192, 2048], P(None, 'frame')
- keyvalue_weight: bfloat16 [8192, 1024], P(None, 'frame')
Outputs:
- context: bfloat16 [4096, 2048], P('seq', 'frame')
The draws below stay inside these ranges and needn't reach their ends.
Inputs may be any that keep to these rules, and one draw needn't show every extreme that they name: `vision_pos`: distinct positions. Of the tokens in rows f * 192 to (f + 1) * 192 - 1, for any f, at most 36 lie in one block of 512 positions that starts at a multiple of 512; some block holds exactly 36 of them for every f. `video_ids`: the tokens of one video are consecutive rows.
All inputs are finite; a program needn't handle non-finite values.
Results may differ from the reference program's by a relative error of at most 0.02.
Values may be sent and summed in bfloat16 or wider, within the bound.
A program may use at most 128 MiB of HBM per device.

```python
import math
import jax
import jax.numpy as jnp
import numpy as np
from jax import lax

VIT_HEADS = 16
VIT_HDIM = 80
D_VIT = 1280
MRG_HID = 5120
D = 8192
HDIM = 128
QPK = 4
KV_HEADS = 4
VIS_DEV = 192
SEQ_DEV = 512
VIS = 768
PATCHES = 3072
D_MRG = 5120
SEQ = 4096


def draw_vision_qkv(key, part):
    base = jax.random.normal(jax.random.fold_in(key, 3), (D_VIT, VIT_HEADS, 3, VIT_HDIM), jnp.float32) * D_VIT ** (-0.5)
    lifted = base * jnp.array([1.6, 1.6, 1.0], jnp.float32)[None, None, :, None]
    return lifted.reshape(D_VIT, VIT_HEADS * 3 * VIT_HDIM).astype(jnp.bfloat16)


def draw_merge_down(key, part):
    base = jax.random.normal(jax.random.fold_in(key, 41), (MRG_HID, D), jnp.float32) * MRG_HID ** (-0.5)
    direction = jax.random.normal(jax.random.fold_in(key, 42), (D,), jnp.float32)
    lift = 3.0 / MRG_HID
    return (base + lift * direction[None, :]).astype(jnp.bfloat16)


def language_weights(key):
    query_part = jax.random.normal(jax.random.fold_in(key, 21), (D, KV_HEADS, QPK, HDIM), jnp.float32) * (1.6 * D ** (-0.5))
    pair_part = jax.random.normal(jax.random.fold_in(key, 22), (D, KV_HEADS, 2, HDIM), jnp.float32) * D ** (-0.5)
    pair_part = pair_part * jnp.array([1.6, 1.0], jnp.float32)[None, None, :, None]
    return (query_part, pair_part)


def draw_query_weight(key, part):
    query_part, pair_part = language_weights(key)
    return query_part.reshape(D, KV_HEADS * QPK * HDIM).astype(jnp.bfloat16)


def draw_keyvalue_weight(key, part):
    query_part, pair_part = language_weights(key)
    return pair_part.reshape(D, KV_HEADS * 2 * HDIM).astype(jnp.bfloat16)


def draw_vision_pos(key, part):
    frame_total = VIS // VIS_DEV
    block_total = SEQ // SEQ_DEV
    share = VIS_DEV // (2 * block_total)
    order_key = jax.random.fold_in(key, 31)
    place_key = jax.random.fold_in(key, 32)
    hot_block = jax.random.randint(jax.random.fold_in(key, 33), (), 0, block_total).astype(jnp.int32)
    ranking = jax.vmap(lambda single: jax.random.permutation(single, block_total))(jax.random.split(order_key, frame_total)).astype(jnp.int32)
    block_ids = jnp.arange(block_total, dtype=jnp.int32)[None, :]
    hot_rank = jnp.sum(jnp.where(block_ids == hot_block, ranking, 0), axis=1, keepdims=True)
    ranking = jnp.where(block_ids == hot_block, 0, jnp.where(ranking == 0, hot_rank, ranking))
    counts = jnp.where(ranking < block_total // 2, 3 * share, share).astype(jnp.int32)
    block_ends = jnp.cumsum(counts, axis=1)
    block_starts = block_ends - counts
    token_ids = jnp.arange(VIS_DEV, dtype=jnp.int32)
    chosen = jnp.sum((block_ends[:, None, :] <= token_ids[None, :, None]).astype(jnp.int32), axis=2)
    within_own = token_ids[None, :] - jnp.take_along_axis(block_starts, chosen, axis=1)
    earlier = jnp.cumsum(counts, axis=0) - counts
    within = jnp.take_along_axis(earlier, chosen, axis=1) + within_own
    layout = jax.vmap(lambda single: jax.random.permutation(single, SEQ_DEV))(jax.random.split(place_key, block_total)).astype(jnp.int32)
    spots = layout[chosen, within]
    return (chosen * SEQ_DEV + spots).reshape(VIS).astype(jnp.int32)


def shard_levels(stream_key, extent, cuts, low, high):
    def one(axis_at, parts):
        heights = jax.random.uniform(jax.random.fold_in(jax.random.fold_in(stream_key, 6), axis_at), (parts,), jnp.float32, low / len(cuts), high / len(cuts))
        return jnp.repeat(jnp.exp(heights), extent[axis_at] // parts).reshape((-1,) + (1,) * (len(extent) - axis_at - 1))

    level = one(*cuts[0])
    for cut in cuts[1:]:
        level = level * one(*cut)
    return level


def length_profile(number_of, total, limit, slope):
    loads = [(1 << 20) // math.isqrt(grade ** slope) + 1 for grade in range(2, number_of + 1)]
    rest, given = total - limit - (number_of - 1), [1] * (number_of - 1)
    while rest > 0:
        candidates = [i for i in range(number_of - 1) if given[i] < limit]
        mass, budget = sum([loads[i] for i in candidates]), rest
        for i in candidates:
            addition = min(limit - given[i], max(1, budget * loads[i] // mass), rest)
            given[i] = given[i] + addition
            rest = rest - addition
    return np.array([limit] + given)


def uneven_parts(own_key, count, total, most, skew):
    if count == 2:
        one = jax.random.randint(own_key, (), max(1, total - most), min(most, total - 1) + 1)
        return jnp.stack([one, total - one])
    sizes = jnp.asarray(length_profile(count, total, most, skew), jnp.int32)
    pairs = (count - 1) // 2
    donor, receiver = sizes[1:1 + 2 * pairs:2], sizes[2:2 + 2 * pairs:2]
    slack = jnp.minimum(donor - 1, most - receiver)
    shifted = jax.random.randint(jax.random.fold_in(own_key, 1), (pairs,), 0, 1 << 20) % (slack + 1)
    sizes = sizes.at[1:1 + 2 * pairs:2].set(donor - shifted).at[2:2 + 2 * pairs:2].set(receiver + shifted)
    return sizes[jax.random.permutation(jax.random.fold_in(own_key, 2), count)]


def scatter_about(own_key, extent, width, most, shards=(), kind=jnp.bfloat16):
    loudness = shard_levels(own_key, extent, shards, -0.22, 0.18) if shards else 1.0
    entries = jax.random.normal(own_key, extent, jnp.float32) * width * loudness
    return jnp.minimum(jnp.maximum(entries, -most), most).astype(kind)


def setup_inputs(seed: int = 0) -> dict:
    seeds = jax.random.split(jax.random.key(seed), 14)
    patches = scatter_about(seeds[0], (PATCHES, D_VIT), 0.5, 4.0, ((0, 4),))
    vit_gain = jnp.clip(1.0 + 0.1 * jax.random.normal(seeds[1], (D_VIT,), jnp.float32), 0.5, 1.5)
    vision_qkv = draw_vision_qkv(jax.random.fold_in(seeds[13], 71), 0)
    vision_out = scatter_about(seeds[3], (D_VIT, D_VIT), D_VIT ** -0.5, 0.15625, ((0, 8),))
    video_ids = jnp.searchsorted(jnp.cumsum(uneven_parts(seeds[4], 3, VIS, 5 * VIS // 8, 0)), jnp.arange(VIS), side="right").astype(jnp.int32)
    merge_gain = jnp.clip(1.0 + 0.1 * jax.random.normal(seeds[5], (D_VIT,), jnp.float32), 0.5, 1.5)
    merge_up = scatter_about(seeds[6], (D_MRG, MRG_HID), D_MRG ** -0.5, 0.078125, ((1, 8),))
    merge_down = draw_merge_down(jax.random.fold_in(seeds[13], 71), 0)
    vision_pos = draw_vision_pos(jax.random.fold_in(seeds[13], 71), 0)
    text_embed = scatter_about(seeds[9], (SEQ, D), 1.0, 6.0, ((0, 32),))
    llm_gain = jnp.clip(1.0 + 0.1 * jax.random.normal(seeds[10], (D,), jnp.float32), 0.5, 1.5)
    query_weight = draw_query_weight(jax.random.fold_in(seeds[13], 71), 0)
    keyvalue_weight = draw_keyvalue_weight(jax.random.fold_in(seeds[13], 71), 0)
    return dict(patches=patches, vit_gain=vit_gain, vision_qkv=vision_qkv, vision_out=vision_out, video_ids=video_ids, merge_gain=merge_gain, merge_up=merge_up, merge_down=merge_down, vision_pos=vision_pos, text_embed=text_embed, llm_gain=llm_gain, query_weight=query_weight, keyvalue_weight=keyvalue_weight)


epsilon = 1e-06
rope_base = 1000000.0

def rms_scale(matrix, scales):
    widened = matrix.astype(jnp.float32)
    factor = lax.rsqrt(lax.optimization_barrier(jnp.mean(widened * widened, axis=-1, keepdims=True)) + epsilon)
    return widened * factor * scales

def rotary(tensor, positions):
    head_width = tensor.shape[-1]
    half_width = head_width // 2
    inverse = rope_base ** (-2.0 * jnp.arange(half_width, dtype=jnp.float32) / head_width)
    angles = positions.astype(jnp.float32)[:, None] * inverse[None, :]
    cosine = jnp.cos(angles)[:, None, :]
    sine_part = jnp.sin(angles)[:, None, :]
    first_half = tensor[..., :half_width]
    second_half = tensor[..., half_width:]
    return jnp.concatenate([first_half * cosine - second_half * sine_part, second_half * cosine + first_half * sine_part], axis=-1)

def attend_all(queries, key_rows, value_rows, allowed, score_scale):
    scores = jnp.dot(queries, key_rows.T, preferred_element_type=jnp.float32) * score_scale
    scores = jnp.where(allowed, scores, -jnp.inf)
    highest = lax.optimization_barrier(jnp.max(scores, axis=1, keepdims=True))
    weights = jnp.exp(scores - highest)
    row_sum = lax.optimization_barrier(jnp.sum(weights, axis=1, keepdims=True))
    mixed = jnp.dot(weights.astype(jnp.bfloat16), value_rows, preferred_element_type=jnp.float32)
    return mixed / row_sum

def reference(patches, vit_gain, vision_qkv, vision_out, video_ids, merge_gain, merge_up, merge_down, vision_pos, text_embed, llm_gain, query_weight, keyvalue_weight):
    normed_patches = rms_scale(patches, vit_gain).astype(jnp.bfloat16)
    projected = jnp.dot(normed_patches, vision_qkv, preferred_element_type=jnp.float32).astype(jnp.bfloat16)
    projected = projected.reshape(PATCHES, VIT_HEADS, 3, VIT_HDIM)
    stacked = jnp.transpose(projected, (2, 1, 0, 3))
    patch_video = jnp.repeat(video_ids, 4)
    same_video = patch_video[:, None] == patch_video[None, :]
    vit_heads_out = lax.map(lambda triple: attend_all(triple[0], triple[1], triple[2], same_video, VIT_HDIM ** (-0.5)), (stacked[0], stacked[1], stacked[2]))
    vit_context = jnp.transpose(vit_heads_out, (1, 0, 2)).reshape(PATCHES, D_VIT).astype(jnp.bfloat16)
    vit_output = patches.astype(jnp.float32) + jnp.dot(vit_context, vision_out, preferred_element_type=jnp.float32)
    merged_input = rms_scale(vit_output, merge_gain).astype(jnp.bfloat16).reshape(VIS, 4 * D_VIT)
    merge_hidden = jax.nn.gelu(jnp.dot(merged_input, merge_up, preferred_element_type=jnp.float32), approximate=False).astype(jnp.bfloat16)
    vision = jnp.dot(merge_hidden, merge_down, preferred_element_type=jnp.float32).astype(jnp.bfloat16)
    embedded = text_embed.at[vision_pos].set(vision)
    normed_tokens = rms_scale(embedded, llm_gain).astype(jnp.bfloat16)
    positions = jnp.arange(SEQ, dtype=jnp.int32)
    query_full = jnp.dot(normed_tokens, query_weight, preferred_element_type=jnp.float32).reshape(SEQ, KV_HEADS * QPK, HDIM)
    llm_query = rotary(query_full, positions).astype(jnp.bfloat16)
    pair_full = jnp.dot(normed_tokens, keyvalue_weight, preferred_element_type=jnp.float32).reshape(SEQ, KV_HEADS, 2, HDIM)
    llm_keys = rotary(pair_full[:, :, 0], positions).astype(jnp.bfloat16)
    llm_values = pair_full[:, :, 1].astype(jnp.bfloat16)
    causal = positions[:, None] >= positions[None, :]
    key_heads = jnp.repeat(jnp.transpose(llm_keys, (1, 0, 2)), QPK, axis=0)
    value_heads = jnp.repeat(jnp.transpose(llm_values, (1, 0, 2)), QPK, axis=0)
    llm_heads_out = lax.map(lambda triple: attend_all(triple[0], triple[1], triple[2], causal, HDIM ** (-0.5)), (jnp.transpose(llm_query, (1, 0, 2)), key_heads, value_heads))
    return jnp.transpose(llm_heads_out, (1, 0, 2)).reshape(SEQ, KV_HEADS * QPK * HDIM).astype(jnp.bfloat16)
```

```python
import functools
import math

import jax
import jax.numpy as jnp
from jax import lax
from jax.experimental import pallas as pl
from jax.experimental.pallas import tpu as pltpu
from jax.sharding import PartitionSpec as P

VIT_HDIM = 80
HDIM = 128


epsilon = 1e-06
rope_base = 1000000.0
lowest = -1e30
vmem_limit = 56 * 1024 * 1024


def rms_scale(matrix, scales):
    widened = matrix.astype(jnp.float32)
    factor = lax.rsqrt(jnp.mean(widened * widened, axis=-1, keepdims=True) + epsilon)
    return widened * factor * scales


MESH = pl.DeviceIdType.MESH
ANY = pl.BlockSpec(memory_space=pl.ANY)
VMEM = pl.BlockSpec(memory_space=pltpu.VMEM)


def ring_grid(count):
    narrow = 1 << ((count.bit_length() - 1) // 2)
    return count // narrow, narrow


def ring_position(index, count):
    tall, narrow = ring_grid(count)
    if narrow < 2 or tall % 2:
        return index
    row, column = lax.div(index, narrow), lax.rem(index, narrow)
    odd = lax.rem(row, 2)
    inner = lax.div(column + narrow - 1, narrow)
    along = (column - 1) * (1 - odd) + (narrow - 1 - column) * odd
    return (1 - inner) * (count - 1 - row) + inner * (row * (narrow - 1) + along)


def ring_index(position, count):
    tall, narrow = ring_grid(count)
    if narrow < 2 or tall % 2:
        return position
    back = lax.div(position, tall * (narrow - 1))
    row, along = lax.div(position, narrow - 1), lax.rem(position, narrow - 1)
    odd = lax.rem(row, 2)
    column = 1 + along * (1 - odd) + (narrow - 2 - along) * odd
    return (1 - back) * (row * narrow + column) + back * (count - 1 - position) * narrow


class Ring:
    def __init__(self, count):
        self.count = count
        self.here = ring_position(lax.axis_index("seq"), count)
        self.right = {"seq": self.index(1)}
        self.left = {"seq": self.index(-1)}

    def index(self, offset):
        return ring_index(lax.rem(self.here + (offset + 2 * self.count), self.count), self.count)


def greet(partners):
    barrier = pltpu.get_barrier_semaphore()
    for partner in partners:
        pl.semaphore_signal(barrier, inc=1, device_id=partner, device_id_type=MESH)
    pl.semaphore_wait(barrier, len(partners))


def remote(source, target, send, recv, partner):
    return pltpu.make_async_remote_copy(
        src_ref=source,
        dst_ref=target,
        send_sem=send,
        recv_sem=recv,
        device_id=partner,
        device_id_type=MESH,
    )


class RingGather:
    def __init__(self, ring, block, out, send, recv, pieces):
        self.ring, self.block, self.out, self.send, self.recv = ring, block, out, send, recv
        self.pieces = pieces
        self.steps = ring.count // 2

    def moves(self, step):
        last = step == self.steps - 1
        for piece in range(self.pieces):
            if not last or piece < self.pieces // 2:
                yield 0, piece
            if not last or piece >= self.pieces // 2:
                yield 1, piece

    def copy(self, step, way, piece):
        offset = -step if way == 0 else step
        owner = self.ring.index(offset)
        source = self.block.at[piece] if step == 0 else self.out(owner, piece)
        return remote(
            source,
            self.out(owner, piece),
            self.send.at[way, step, piece],
            self.recv.at[way, step, piece],
            self.ring.right if way == 0 else self.ring.left,
        )

    def start(self):
        for way, piece in self.moves(0):
            self.copy(0, way, piece).start()

    def advance(self, step, landed=None):
        ahead = list(self.moves(step + 1)) if step + 1 < self.steps else []
        for way, piece in self.moves(step):
            self.copy(step, way, piece).wait_recv()
            if (way, piece) in ahead:
                self.copy(step + 1, way, piece).start()
            if landed is not None:
                landed(self.ring.index(-(step + 1) if way == 0 else step + 1), piece, way, step)

    def finish(self):
        for step in range(self.steps):
            for way, piece in self.moves(step):
                self.copy(step, way, piece).wait_send()


def ring_sems(count, pieces):
    return [pltpu.SemaphoreType.DMA((2, count // 2, pieces))] * 2


class FrameGather:
    def __init__(self, count, block, out, sends, recvs, pieces):
        self.block, self.out, self.pieces = block, out, pieces
        self.sends, self.recvs = sends, recvs
        self.chips = count // 2
        me = lax.axis_index("frame")
        self.me, self.chip, self.core = me, lax.div(me, 2), lax.rem(me, 2)
        self.twin = {"frame": self.chip * 2 + 1 - self.core}

    def peer(self, distance):
        return lax.rem(self.chip + distance + self.chips, self.chips) * 2 + self.core

    def partners(self):
        return [self.twin] + [{"frame": self.peer(d)} for d in range(1, self.chips)]

    def across(self, distance, piece):
        return remote(
            self.block.at[piece],
            self.out.at[self.me, piece],
            self.sends.at[0, distance, piece],
            self.recvs.at[0, distance, piece],
            {"frame": self.peer(distance)},
        )

    def inside(self, distance, piece):
        slot = self.peer(-distance)
        return remote(
            self.block.at[piece] if distance == 0 else self.out.at[slot, piece],
            self.out.at[slot, piece],
            self.sends.at[1, distance, piece],
            self.recvs.at[1, distance, piece],
            self.twin,
        )

    def start(self):
        for piece in range(self.pieces):
            for d in range(1, self.chips):
                self.across(d, piece).start()
        for piece in range(self.pieces):
            self.inside(0, piece).start()

    def relay(self, piece):
        for d in range(1, self.chips):
            self.across(d, piece).wait_recv()
            self.inside(d, piece).start()

    def finish(self):
        for piece in range(self.pieces):
            for d in range(self.chips):
                self.inside(d, piece).wait()
                if d:
                    self.across(d, piece).wait_send()


def frame_sems(count, pieces):
    return [pltpu.SemaphoreType.DMA((2, count // 2, pieces))] * 2


def comm_params(collective):
    return pltpu.CompilerParams(
        collective_id=collective, has_side_effects=True, vmem_limit_bytes=vmem_limit
    )


def ring_gather_kernel(count, block, out, send, recv, own):
    ring = Ring(count)
    gather = RingGather(ring, block, lambda i, piece: out.at[i, piece], send, recv, block.shape[0])
    greet([ring.left, ring.right])
    gather.start()
    keep = pltpu.make_async_copy(block, out.at[ring.index(0)], own)
    keep.start()
    for step in range(gather.steps):
        gather.advance(step)
    keep.wait()
    gather.finish()


def ring_gather(block, count, collective):
    pieces = block.shape[0]
    return pl.pallas_call(
        functools.partial(ring_gather_kernel, count),
        in_specs=[VMEM],
        out_specs=ANY,
        out_shape=jax.ShapeDtypeStruct((count,) + block.shape, block.dtype),
        scratch_shapes=ring_sems(count, pieces) + [pltpu.SemaphoreType.DMA],
        compiler_params=comm_params(collective),
    )(block)


def frame_gather_kernel(count, block, out, send, recv, own):
    gather = FrameGather(count, block, out, send, recv, block.shape[0])
    greet(gather.partners())
    gather.start()
    keep = pltpu.make_async_copy(block, out.at[gather.me], own)
    keep.start()
    for piece in range(gather.pieces):
        gather.relay(piece)
    keep.wait()
    gather.finish()


def frame_gather(block, count, collective):
    pieces = block.shape[0]
    return pl.pallas_call(
        functools.partial(frame_gather_kernel, count),
        in_specs=[VMEM],
        out_specs=ANY,
        out_shape=jax.ShapeDtypeStruct((count,) + block.shape, block.dtype),
        scratch_shapes=frame_sems(count, pieces) + [pltpu.SemaphoreType.DMA],
        compiler_params=comm_params(collective),
    )(block)


def front_kernel(seq_count, frame_count, pair, weight, pair_out, weight_out, *sems):
    fsend, frecv, rsend, rrecv, tsend, trecv, own = sems
    ring = Ring(seq_count)
    frames = FrameGather(frame_count, pair, pair_out, fsend, frecv, pair.shape[0])
    core, twin = frames.core, frames.twin
    quarter = weight.shape[1]
    half = weight.at[core]
    gather = RingGather(
        ring, half, lambda i, piece: weight_out.at[i, core, piece], rsend, rrecv, quarter
    )
    greet([ring.left, ring.right] + frames.partners())
    frames.start()
    gather.start()
    here = ring.index(0)
    keep = [
        pltpu.make_async_copy(pair, pair_out.at[frames.me], own.at[0]),
        pltpu.make_async_copy(weight, weight_out.at[here], own.at[1]),
    ]
    for copy in keep:
        copy.start()
    handed = []

    def landed(index, piece, way, step):
        copy = remote(
            weight_out.at[index, core, piece],
            weight_out.at[index, core, piece],
            tsend.at[way, step, piece],
            trecv.at[way, step, piece],
            twin,
        )
        copy.start()
        handed.append(copy)

    for step in range(max(gather.steps, frames.pieces)):
        if step < frames.pieces:
            frames.relay(step)
        if step < gather.steps:
            gather.advance(step, landed)
    for copy in keep:
        copy.wait()
    frames.finish()
    gather.finish()
    for copy in handed:
        copy.wait()


def front(pair, weight, seq_count, frame_count, collective):
    quarter = 2
    weight = weight.reshape(2, quarter, -1, weight.shape[1])
    pair_out, weight_out = pl.pallas_call(
        functools.partial(front_kernel, seq_count, frame_count),
        in_specs=[VMEM, VMEM],
        out_specs=[ANY, ANY],
        out_shape=[
            jax.ShapeDtypeStruct((frame_count,) + pair.shape, pair.dtype),
            jax.ShapeDtypeStruct((seq_count,) + weight.shape, weight.dtype),
        ],
        scratch_shapes=frame_sems(frame_count, pair.shape[0])
        + ring_sems(seq_count, quarter) * 2
        + [pltpu.SemaphoreType.DMA((2,))],
        compiler_params=comm_params(collective),
    )(pair, weight)
    return pair_out, weight_out.reshape(-1, weight.shape[-1])


def vit_attention_kernel(own_ref, ids_ref, q_ref, kv_ref, out_ref):
    frames, heads, _, rows = kv_ref.shape
    allowed = ids_ref[...] == own_ref[...]
    for head in range(heads):
        spread = slice(head * VIT_HDIM, (head + 1) * VIT_HDIM)
        queries = q_ref[spread, :]
        scores = jnp.concatenate(
            [
                lax.dot_general(
                    kv_ref[f, head, :VIT_HDIM, :],
                    queries,
                    (((0,), (0,)), ((), ())),
                    preferred_element_type=jnp.float32,
                )
                for f in range(frames)
            ],
            axis=0,
        )
        scores = jnp.where(allowed, scores, lowest)
        highest = jnp.max(scores, axis=0, keepdims=True)
        weights = jnp.exp((scores - highest) * VIT_HDIM ** (-0.5))
        row_sum = jnp.sum(weights, axis=0, keepdims=True)
        weights = weights.astype(jnp.bfloat16)
        mixed = sum(
            jnp.dot(
                kv_ref[f, head, VIT_HDIM:, :],
                weights[f * rows : (f + 1) * rows],
                preferred_element_type=jnp.float32,
            )
            for f in range(frames)
        )
        out_ref[spread, :] = (mixed / row_sum).astype(out_ref.dtype)


def vit_attention(own_ids, all_ids, queries, pairs):
    width, rows = queries.shape
    keys = all_ids.shape[0]
    step = math.gcd(rows, 256)
    return pl.pallas_call(
        vit_attention_kernel,
        grid=(rows // step,),
        in_specs=[
            pl.BlockSpec((1, step), lambda i: (0, i)),
            pl.BlockSpec((keys, 1), lambda i: (0, 0)),
            pl.BlockSpec((width, step), lambda i: (0, i)),
            pl.BlockSpec(pairs.shape, lambda i: (0, 0, 0, 0)),
        ],
        out_specs=pl.BlockSpec((width, step), lambda i: (0, i)),
        out_shape=jax.ShapeDtypeStruct((width, rows), jnp.bfloat16),
        compiler_params=pltpu.CompilerParams(vmem_limit_bytes=vmem_limit),
    )(own_ids[None, :], all_ids[:, None], queries, pairs)


def scatter_kernel(count, hidden, weight, gain, out, held, part, stage, land, load, send, recv):
    ring = Ring(count)
    width = weight.shape[1]
    pieces = held.shape[0]
    span = width // pieces
    share = out.shape[0]
    order = [piece for pair in zip(range(pieces // 2), range(pieces // 2, pieces)) for piece in pair]
    loads = {
        piece: pltpu.make_async_copy(
            weight.at[:, pl.ds(piece * span, span)], held.at[piece], load.at[piece]
        )
        for piece in order
    }
    for piece in order:
        loads[piece].start()
    greet([ring.left, ring.right])
    forward = [piece < pieces // 2 for piece in range(pieces)]

    def hop(piece, step):
        return remote(
            stage.at[piece, step],
            land.at[piece, step],
            send.at[piece, step],
            recv.at[piece, step],
            ring.right if forward[piece] else ring.left,
        )

    for piece in order:
        loads[piece].wait()
        product = jnp.dot(hidden[...], held[piece], preferred_element_type=jnp.float32)
        for i in range(count):
            part[piece, i] = product[i * share : (i + 1) * share]
        first = ring.index(-1 if forward[piece] else 1)
        stage[piece, 0] = part[piece, first].astype(jnp.bfloat16)
        hop(piece, 0).start()

    def body(step, carry):
        for piece in order:
            hop(piece, step - 1).wait_recv()
            turn = -1 - step if forward[piece] else 1 + step
            owner = ring.index(turn)
            total = land[piece, step - 1].astype(jnp.float32) + part[piece, owner]
            stage[piece, step] = total.astype(jnp.bfloat16)
            hop(piece, step).start()
        return carry

    lax.fori_loop(1, count - 1, body, 0)
    here = ring.index(0)
    squares = jnp.zeros((share, 1), jnp.float32)
    for piece in order:
        hop(piece, count - 2).wait_recv()
        total = land[piece, count - 2].astype(jnp.float32) + part[piece, here]
        total = total.astype(jnp.bfloat16).astype(jnp.float32)
        part[piece, here] = total
        squares += jnp.sum(total * total, axis=1, keepdims=True)
    factor = lax.rsqrt(squares / width + epsilon)
    for piece in order:
        columns = slice(piece * span, (piece + 1) * span)
        out[:, columns] = (part[piece, here] * factor * gain[:, columns]).astype(out.dtype)

    def drain(step, carry):
        for piece in order:
            hop(piece, step).wait_send()
        return carry

    lax.fori_loop(0, count - 1, drain, 0)


def scatter(hidden, weight, gain, count, collective):
    rows, depth = hidden.shape
    width = weight.shape[1]
    share = rows // count
    pieces = 4
    span = width // pieces
    return pl.pallas_call(
        functools.partial(scatter_kernel, count),
        in_specs=[VMEM, ANY, VMEM],
        out_specs=VMEM,
        out_shape=jax.ShapeDtypeStruct((share, width), jnp.bfloat16),
        scratch_shapes=[
            pltpu.VMEM((pieces, depth, span), jnp.bfloat16),
            pltpu.VMEM((pieces, count, share, span), jnp.float32),
            pltpu.VMEM((pieces, count - 1, share, span), jnp.bfloat16),
            pltpu.VMEM((pieces, count - 1, share, span), jnp.bfloat16),
            pltpu.SemaphoreType.DMA((pieces,)),
            pltpu.SemaphoreType.DMA((pieces, count - 1)),
            pltpu.SemaphoreType.DMA((pieces, count - 1)),
        ],
        compiler_params=comm_params(collective),
    )(hidden, weight, gain[None, :])


def turns(positions):
    inverse = rope_base ** (-2.0 * jnp.arange(HDIM // 2, dtype=jnp.float32) / HDIM)
    angles = positions.astype(jnp.float32)[:, None] * inverse[None, :]
    cosine, sine_part = jnp.cos(angles), jnp.sin(angles)
    return jnp.concatenate([cosine, cosine], axis=1), jnp.concatenate([-sine_part, sine_part], axis=1)


def project_kernel(blocks, *refs):
    tokens, (where, qw, kw, cosine, sine_part, q_out, pair_out, q_acc, p_acc) = refs[:blocks], refs[blocks:]
    step = pl.program_id(0)
    rows = jnp.concatenate([ref[...] for ref in tokens], axis=0)
    q_part = jnp.dot(rows, qw[...], preferred_element_type=jnp.float32)
    p_part = jnp.dot(rows, kw[...], preferred_element_type=jnp.float32)

    @pl.when(step == 0)
    def _():
        q_acc[...] = q_part
        p_acc[...] = p_part

    @pl.when(step > 0)
    def _():
        q_acc[...] += q_part
        p_acc[...] += p_part

    @pl.when(step == pl.num_programs(0) - 1)
    def _():
        share = tokens[0].shape[0]
        for block in range(blocks):
            source = slice(block * share, (block + 1) * share)
            target = pl.ds(pl.multiple_of(where[block] * share, share), share)
            turn, slide = cosine[target, :], sine_part[target, :]
            for head in range(q_acc.shape[1] // HDIM):
                columns = slice(head * HDIM, (head + 1) * HDIM)
                values = q_acc[source, columns]
                q_out[target, columns] = (
                    values * turn + pltpu.roll(values, HDIM // 2, 1) * slide
                ).astype(q_out.dtype)
            values = p_acc[source, :HDIM]
            pair_out[target, :HDIM] = (
                values * turn + pltpu.roll(values, HDIM // 2, 1) * slide
            ).astype(pair_out.dtype)
            pair_out[target, HDIM:] = p_acc[source, HDIM:].astype(pair_out.dtype)


def project(blocks, where, positions, query_weight, keyvalue_weight):
    share, depth = blocks[0].shape
    rows = share * len(blocks)
    queries, pairs = query_weight.shape[1], keyvalue_weight.shape[1]
    slab = math.gcd(depth, 1024)
    cosine, sine_part = turns(positions)
    whole = lambda shape: pl.BlockSpec(shape, lambda k: (0, 0))
    return pl.pallas_call(
        functools.partial(project_kernel, len(blocks)),
        grid=(depth // slab,),
        in_specs=[pl.BlockSpec((share, slab), lambda k: (0, k))] * len(blocks)
        + [
            pl.BlockSpec(memory_space=pltpu.SMEM),
            pl.BlockSpec((slab, queries), lambda k: (k, 0)),
            pl.BlockSpec((slab, pairs), lambda k: (k, 0)),
            whole((rows, HDIM)),
            whole((rows, HDIM)),
        ],
        out_specs=[whole((rows, queries)), whole((rows, pairs))],
        out_shape=[
            jax.ShapeDtypeStruct((rows, queries), jnp.bfloat16),
            jax.ShapeDtypeStruct((rows, pairs), jnp.bfloat16),
        ],
        scratch_shapes=[
            pltpu.VMEM((rows, queries), jnp.float32),
            pltpu.VMEM((rows, pairs), jnp.float32),
        ],
        compiler_params=pltpu.CompilerParams(vmem_limit_bytes=vmem_limit),
    )(*blocks, where, query_weight, keyvalue_weight, cosine, sine_part)


def causal_kernel(block_ref, q_ref, k_ref, v_ref, out_ref):
    rows = q_ref.shape[0]
    queries = q_ref[...]

    def fold(start, state_in, masked):
        running_max, running_sum, weighted = state_in
        scores = lax.dot_general(
            queries,
            k_ref[pl.ds(start, rows), :],
            (((1,), (1,)), ((), ())),
            preferred_element_type=jnp.float32,
        )
        if masked:
            row_id = lax.broadcasted_iota(jnp.int32, (rows, rows), 0)
            column_id = lax.broadcasted_iota(jnp.int32, (rows, rows), 1)
            scores = jnp.where(row_id >= column_id, scores, lowest)
        new_max = jnp.maximum(running_max, jnp.max(scores, axis=1, keepdims=True))
        weights = jnp.exp((scores - new_max) * HDIM ** (-0.5))
        shrink = jnp.exp((running_max - new_max) * HDIM ** (-0.5))
        running_sum = running_sum * shrink + jnp.sum(weights, axis=1, keepdims=True)
        update = jnp.dot(
            weights.astype(jnp.bfloat16),
            v_ref[pl.ds(start, rows), :],
            preferred_element_type=jnp.float32,
        )
        return (new_max, running_sum, weighted * shrink + update)

    state = (
        jnp.full((rows, 1), lowest, jnp.float32),
        jnp.zeros((rows, 1), jnp.float32),
        jnp.zeros((rows, HDIM), jnp.float32),
    )
    own = block_ref[0]
    state = fold(pl.multiple_of(own * rows, rows), state, True)
    _, running_sum, weighted = lax.fori_loop(
        0, own, lambda i, now: fold(pl.multiple_of(i * rows, rows), now, False), state
    )
    out_ref[...] = (weighted / running_sum).astype(out_ref.dtype)


def causal_attention(block_index, queries, key_rows, value_rows):
    rows, width = queries.shape
    keys = key_rows.shape[0]
    return pl.pallas_call(
        causal_kernel,
        grid=(width // HDIM,),
        in_specs=[
            pl.BlockSpec(memory_space=pltpu.SMEM),
            pl.BlockSpec((rows, HDIM), lambda h: (0, h)),
            pl.BlockSpec((keys, HDIM), lambda h: (0, 0)),
            pl.BlockSpec((keys, HDIM), lambda h: (0, 0)),
        ],
        out_specs=pl.BlockSpec((rows, HDIM), lambda h: (0, h)),
        out_shape=jax.ShapeDtypeStruct((rows, width), jnp.bfloat16),
        compiler_params=pltpu.CompilerParams(vmem_limit_bytes=vmem_limit),
    )(block_index[None], queries, key_rows, value_rows)


def place(token_pos, first, text_rows, vision_rows):
    spots = first + jnp.arange(text_rows.shape[0], dtype=jnp.int32)
    hit = spots[:, None] == token_pos[None, :]
    moved = jnp.dot(hit.astype(jnp.bfloat16), vision_rows, preferred_element_type=jnp.float32)
    taken = jnp.any(hit, axis=1, keepdims=True)
    return jnp.where(taken, moved.astype(jnp.bfloat16), text_rows)


def local(
    patches,
    vit_gain,
    vision_qkv,
    vision_out,
    video_ids,
    merge_gain,
    merge_up,
    merge_down,
    vision_pos,
    text_embed,
    llm_gain,
    query_weight,
    keyvalue_weight,
):
    frame_index = lax.axis_index("frame")
    seq_index = lax.axis_index("seq")
    frame_count = lax.axis_size("frame")
    seq_count = lax.axis_size("seq")
    patch_rows = patches.shape[0]
    local_heads = vision_qkv.shape[1] // (3 * VIT_HDIM)
    barrier = lax.optimization_barrier

    normed_patches = rms_scale(patches, vit_gain).astype(jnp.bfloat16)
    projected = lax.dot_general(
        vision_qkv, normed_patches, (((0,), (1,)), ((), ())), preferred_element_type=jnp.float32
    ).astype(jnp.bfloat16)
    projected = projected.reshape(local_heads, 3 * VIT_HDIM, patch_rows)
    vit_query = projected[:, :VIT_HDIM].reshape(local_heads * VIT_HDIM, patch_rows)
    patch_video = jnp.repeat(video_ids, 4)
    own_video = lax.dynamic_slice_in_dim(patch_video, frame_index * patch_rows, patch_rows)
    pair_all, out_full = front(projected[:, VIT_HDIM:], vision_out, seq_count, frame_count, 1)

    text_own = rms_scale(text_embed, llm_gain).astype(jnp.bfloat16)
    text_own, pair_all = barrier((text_own, pair_all))
    text_blocks, owners = [text_own], [0]
    bit = frame_count // 2
    while bit:
        swap = [(i, i ^ bit) for i in range(frame_count)]
        text_blocks = text_blocks + [lax.ppermute(block, "frame", swap) for block in text_blocks]
        owners = owners + [mask ^ bit for mask in owners]
        bit //= 2

    vit_context = vit_attention(own_video, patch_video, vit_query, pair_all)
    pieces = vit_context.reshape(2, -1, patch_rows)
    context_all = ring_gather(pieces, seq_count, 2).reshape(-1, patch_rows)
    head_total = lax.dot_general(
        context_all, out_full, (((0,), (0,)), ((), ())), preferred_element_type=jnp.float32
    )
    vit_output = patches.astype(jnp.float32) + head_total
    merged_input = (
        rms_scale(vit_output, merge_gain).astype(jnp.bfloat16).reshape(patch_rows // 4, -1)
    )
    merge_hidden = jax.nn.gelu(
        jnp.dot(merged_input, merge_up, preferred_element_type=jnp.float32), approximate=False
    ).astype(jnp.bfloat16)
    vision_normed = scatter(merge_hidden, merge_down, llm_gain, seq_count, 3)

    part_rows = text_embed.shape[0]
    seq_block = part_rows * frame_count
    first = seq_index * seq_block
    where = jnp.bitwise_xor(frame_index, jnp.array(owners, jnp.int32))
    text_blocks[-1], vision_normed = barrier((text_blocks[-1], vision_normed))
    text_query, text_pair = project(
        text_blocks, where, first + jnp.arange(seq_block, dtype=jnp.int32), query_weight, keyvalue_weight
    )
    text_pair_all = ring_gather(text_pair.reshape(2, seq_block // 2, -1), seq_count, 4)
    text_pair_all = text_pair_all.reshape(seq_count * seq_block, -1)

    share = vision_normed.shape[0]
    vision_normed, text_pair_all = barrier((vision_normed, text_pair_all))
    halves = vision_normed.reshape(share, 2, -1).transpose(1, 0, 2)
    vision_tokens = frame_gather(halves, frame_count, 5).transpose(0, 2, 1, 3)
    vision_tokens = vision_tokens.reshape(frame_count * share, -1)
    token_pos = vision_pos.reshape(frame_count, seq_count, share).transpose(1, 0, 2)
    here = lax.dynamic_index_in_dim(token_pos, seq_index, 0, keepdims=False).reshape(-1)
    vision_query, vision_pair = project(
        [vision_tokens], jnp.zeros((1,), jnp.int32), here, query_weight, keyvalue_weight
    )
    vision_both = jnp.concatenate([vision_query, vision_pair], axis=1)
    gathered = ring_gather(vision_both.reshape(2, frame_count * share // 2, -1), seq_count, 6)
    gathered = gathered.reshape(seq_count * frame_count * share, -1)
    width = vision_query.shape[1]
    token_pos = token_pos.reshape(-1)
    llm_query = place(token_pos, first, text_query, gathered[:, :width])
    llm_pair = place(token_pos, 0, text_pair_all, gathered[:, width:])
    return causal_attention(seq_index, llm_query, llm_pair[:, :HDIM], llm_pair[:, HDIM:])


def solution(mesh):
    return jax.shard_map(
        local,
        mesh=mesh,
        in_specs=(
            P("frame", None),
            P(),
            P(None, "seq"),
            P("seq", None),
            P(),
            P(),
            P(None, "seq"),
            P("seq", None),
            P(),
            P(("seq", "frame"), None),
            P(),
            P(None, "frame"),
            P(None, "frame"),
        ),
        out_specs=P("seq", "frame"),
        check_vma=False,
    )
```

```python
import functools
import math

import jax
import jax.numpy as jnp
from jax import lax
from jax.experimental import pallas as pl
from jax.experimental.pallas import tpu as pltpu
from jax.sharding import PartitionSpec as P

VIT_HDIM = 80
HDIM = 128


epsilon = 1e-06
rope_base = 1000000.0
lowest = -1e30
vmem_limit = 56 * 1024 * 1024


def rms_scale(matrix, scales):
    widened = matrix.astype(jnp.float32)
    factor = lax.rsqrt(jnp.mean(widened * widened, axis=-1, keepdims=True) + epsilon)
    return widened * factor * scales


MESH = pl.DeviceIdType.MESH
ANY = pl.BlockSpec(memory_space=pl.ANY)
VMEM = pl.BlockSpec(memory_space=pltpu.VMEM)


def ring_grid(count):
    narrow = 1 << ((count.bit_length() - 1) // 2)
    return count // narrow, narrow


def ring_position(index, count):
    tall, narrow = ring_grid(count)
    if narrow < 2 or tall % 2:
        return index
    row, column = lax.div(index, narrow), lax.rem(index, narrow)
    odd = lax.rem(row, 2)
    inner = lax.div(column + narrow - 1, narrow)
    along = (column - 1) * (1 - odd) + (narrow - 1 - column) * odd
    return (1 - inner) * (count - 1 - row) + inner * (row * (narrow - 1) + along)


def ring_index(position, count):
    tall, narrow = ring_grid(count)
    if narrow < 2 or tall % 2:
        return position
    back = lax.div(position, tall * (narrow - 1))
    row, along = lax.div(position, narrow - 1), lax.rem(position, narrow - 1)
    odd = lax.rem(row, 2)
    column = 1 + along * (1 - odd) + (narrow - 2 - along) * odd
    return (1 - back) * (row * narrow + column) + back * (count - 1 - position) * narrow


class Ring:
    def __init__(self, count):
        self.count = count
        self.here = ring_position(lax.axis_index("seq"), count)
        self.right = {"seq": self.index(1)}
        self.left = {"seq": self.index(-1)}

    def index(self, offset):
        return ring_index(lax.rem(self.here + (offset + 2 * self.count), self.count), self.count)


def greet(partners):
    barrier = pltpu.get_barrier_semaphore()
    for partner in partners:
        pl.semaphore_signal(barrier, inc=1, device_id=partner, device_id_type=MESH)
    pl.semaphore_wait(barrier, len(partners))


def remote(source, target, send, recv, partner):
    return pltpu.make_async_remote_copy(
        src_ref=source,
        dst_ref=target,
        send_sem=send,
        recv_sem=recv,
        device_id=partner,
        device_id_type=MESH,
    )


class RingGather:
    def __init__(self, ring, block, out, send, recv, pieces):
        self.ring, self.block, self.out, self.send, self.recv = ring, block, out, send, recv
        self.pieces = pieces
        self.steps = ring.count // 2

    def moves(self, step):
        last = step == self.steps - 1
        for piece in range(self.pieces):
            if not last or piece < self.pieces // 2:
                yield 0, piece
            if not last or piece >= self.pieces // 2:
                yield 1, piece

    def copy(self, step, way, piece):
        offset = -step if way == 0 else step
        owner = self.ring.index(offset)
        source = self.block.at[piece] if step == 0 else self.out(owner, piece)
        return remote(
            source,
            self.out(owner, piece),
            self.send.at[way, step, piece],
            self.recv.at[way, step, piece],
            self.ring.right if way == 0 else self.ring.left,
        )

    def start(self):
        for way, piece in self.moves(0):
            self.copy(0, way, piece).start()

    def advance(self, step, landed=None):
        ahead = list(self.moves(step + 1)) if step + 1 < self.steps else []
        for way, piece in self.moves(step):
            self.copy(step, way, piece).wait_recv()
            if (way, piece) in ahead:
                self.copy(step + 1, way, piece).start()
            if landed is not None:
                landed(self.ring.index(-(step + 1) if way == 0 else step + 1), piece, way, step)

    def finish(self):
        for step in range(self.steps):
            for way, piece in self.moves(step):
                self.copy(step, way, piece).wait_send()


def ring_sems(count, pieces):
    return [pltpu.SemaphoreType.DMA((2, count // 2, pieces))] * 2


class FrameGather:
    def __init__(self, count, block, out, sends, recvs, pieces):
        self.block, self.out, self.pieces = block, out, pieces
        self.sends, self.recvs = sends, recvs
        self.chips = count // 2
        me = lax.axis_index("frame")
        self.me, self.chip, self.core = me, lax.div(me, 2), lax.rem(me, 2)
        self.twin = {"frame": self.chip * 2 + 1 - self.core}

    def peer(self, distance):
        return lax.rem(self.chip + distance + self.chips, self.chips) * 2 + self.core

    def partners(self):
        return [self.twin] + [{"frame": self.peer(d)} for d in range(1, self.chips)]

    def across(self, distance, piece):
        return remote(
            self.block.at[piece],
            self.out.at[self.me, piece],
            self.sends.at[0, distance, piece],
            self.recvs.at[0, distance, piece],
            {"frame": self.peer(distance)},
        )

    def inside(self, distance, piece):
        slot = self.peer(-distance)
        return remote(
            self.block.at[piece] if distance == 0 else self.out.at[slot, piece],
            self.out.at[slot, piece],
            self.sends.at[1, distance, piece],
            self.recvs.at[1, distance, piece],
            self.twin,
        )

    def start(self):
        for piece in range(self.pieces):
            for d in range(1, self.chips):
                self.across(d, piece).start()
        for piece in range(self.pieces):
            self.inside(0, piece).start()

    def relay(self, piece):
        for d in range(1, self.chips):
            self.across(d, piece).wait_recv()
            self.inside(d, piece).start()

    def finish(self):
        for piece in range(self.pieces):
            for d in range(self.chips):
                self.inside(d, piece).wait()
                if d:
                    self.across(d, piece).wait_send()


def frame_sems(count, pieces):
    return [pltpu.SemaphoreType.DMA((2, count // 2, pieces))] * 2


def comm_params(collective):
    return pltpu.CompilerParams(
        collective_id=collective, has_side_effects=True, vmem_limit_bytes=vmem_limit
    )


def front_kernel(seq_count, frame_count, pair, weight, pair_out, weight_out, *sems):
    fsend, frecv, rsend, rrecv, tsend, trecv, own = sems
    ring = Ring(seq_count)
    frames = FrameGather(frame_count, pair, pair_out, fsend, frecv, pair.shape[0])
    core, twin = frames.core, frames.twin
    quarter = weight.shape[1]
    half = weight.at[core]
    gather = RingGather(
        ring, half, lambda i, piece: weight_out.at[i, core, piece], rsend, rrecv, quarter
    )
    greet([ring.left, ring.right] + frames.partners())
    frames.start()
    gather.start()
    here = ring.index(0)
    keep = [
        pltpu.make_async_copy(pair, pair_out.at[frames.me], own.at[0]),
        pltpu.make_async_copy(weight, weight_out.at[here], own.at[1]),
    ]
    for copy in keep:
        copy.start()
    handed = []

    def landed(index, piece, way, step):
        copy = remote(
            weight_out.at[index, core, piece],
            weight_out.at[index, core, piece],
            tsend.at[way, step, piece],
            trecv.at[way, step, piece],
            twin,
        )
        copy.start()
        handed.append(copy)

    for step in range(max(gather.steps, frames.pieces)):
        if step < frames.pieces:
            frames.relay(step)
        if step < gather.steps:
            gather.advance(step, landed)
    for copy in keep:
        copy.wait()
    frames.finish()
    gather.finish()
    for copy in handed:
        copy.wait()


def front(pair, weight, seq_count, frame_count, collective):
    quarter = 2
    weight = weight.reshape(2, quarter, -1, weight.shape[1])
    pair_out, weight_out = pl.pallas_call(
        functools.partial(front_kernel, seq_count, frame_count),
        in_specs=[VMEM, VMEM],
        out_specs=[ANY, ANY],
        out_shape=[
            jax.ShapeDtypeStruct((frame_count,) + pair.shape, pair.dtype),
            jax.ShapeDtypeStruct((seq_count,) + weight.shape, weight.dtype),
        ],
        scratch_shapes=frame_sems(frame_count, pair.shape[0])
        + ring_sems(seq_count, quarter) * 2
        + [pltpu.SemaphoreType.DMA((2,))],
        compiler_params=comm_params(collective),
    )(pair, weight)
    return pair_out, weight_out.reshape(-1, weight.shape[-1])


def vit_attention_kernel(own_ref, ids_ref, q_ref, kv_ref, out_ref):
    frames, heads, _, rows = kv_ref.shape
    allowed = ids_ref[...] == own_ref[...]
    for head in range(heads):
        spread = slice(head * VIT_HDIM, (head + 1) * VIT_HDIM)
        queries = q_ref[spread, :]
        scores = jnp.concatenate(
            [
                lax.dot_general(
                    kv_ref[f, head, :VIT_HDIM, :],
                    queries,
                    (((0,), (0,)), ((), ())),
                    preferred_element_type=jnp.float32,
                )
                for f in range(frames)
            ],
            axis=0,
        )
        scores = jnp.where(allowed, scores, lowest)
        highest = jnp.max(scores, axis=0, keepdims=True)
        weights = jnp.exp((scores - highest) * VIT_HDIM ** (-0.5))
        row_sum = jnp.sum(weights, axis=0, keepdims=True)
        weights = weights.astype(jnp.bfloat16)
        mixed = sum(
            jnp.dot(
                kv_ref[f, head, VIT_HDIM:, :],
                weights[f * rows : (f + 1) * rows],
                preferred_element_type=jnp.float32,
            )
            for f in range(frames)
        )
        out_ref[spread, :] = (mixed / row_sum).astype(out_ref.dtype)


def vit_attention(own_ids, all_ids, queries, pairs):
    width, rows = queries.shape
    keys = all_ids.shape[0]
    step = math.gcd(rows, 256)
    return pl.pallas_call(
        vit_attention_kernel,
        grid=(rows // step,),
        in_specs=[
            pl.BlockSpec((1, step), lambda i: (0, i)),
            pl.BlockSpec((keys, 1), lambda i: (0, 0)),
            pl.BlockSpec((width, step), lambda i: (0, i)),
            pl.BlockSpec(pairs.shape, lambda i: (0, 0, 0, 0)),
        ],
        out_specs=pl.BlockSpec((width, step), lambda i: (0, i)),
        out_shape=jax.ShapeDtypeStruct((width, rows), jnp.bfloat16),
        compiler_params=pltpu.CompilerParams(vmem_limit_bytes=vmem_limit),
    )(own_ids[None, :], all_ids[:, None], queries, pairs)


def mid_kernel(count, block, out_weight, patches, gain, up, hidden, held, up_held, total, spread, load, send, recv, own):
    load_up = pltpu.make_async_copy(up, up_held, load)
    load_up.start()
    ring = Ring(count)
    pieces, tall, rows = block.shape
    share = pieces * tall
    gather = RingGather(ring, block, lambda i, piece: held.at[i, piece], send, recv, pieces)
    greet([ring.left, ring.right])
    gather.start()
    keep = pltpu.make_async_copy(block, held.at[ring.index(0)], own)
    keep.start()

    def fold(offsets, first):
        owners = [ring.index(offset) for offset in offsets]
        left = jnp.concatenate([held[i].reshape(share, rows) for i in owners], axis=0)
        right = jnp.concatenate([out_weight[i] for i in owners], axis=0)
        product = lax.dot_general(
            left, right, (((0,), (0,)), ((), ())), preferred_element_type=jnp.float32
        )
        if first:
            total[...] = patches[...].astype(jnp.float32) + product
        else:
            total[...] += product

    half = max(gather.steps // 2, 1)
    keep.wait()
    for step in range(gather.steps):
        gather.advance(step)
        if step == half - 1:
            fold(range(-half, half + 1), True)
    if gather.steps > half:
        rest = list(range(half + 1, gather.steps)) + list(range(-gather.steps, -half))
        fold(rest, False)
    width = total.shape[1]
    values = total[...]
    factor = lax.rsqrt(jnp.mean(values * values, axis=1, keepdims=True) + epsilon)
    values = values * factor * gain[...]
    lanes = spread.shape[2]
    for c in range(width // lanes):
        spread[c] = values[:, c * lanes : (c + 1) * lanes]
    load_up.wait()
    result = sum(
        jnp.dot(
            jnp.concatenate(
                [spread[c, pl.ds(r, rows // 4, stride=4), :] for c in range(width // lanes)], axis=1
            ).astype(jnp.bfloat16),
            up_held[r * width : (r + 1) * width, :],
            preferred_element_type=jnp.float32,
        )
        for r in range(4)
    )
    hidden[...] = (0.5 * result * (1.0 + lax.erf(result * 0.5**0.5))).astype(hidden.dtype)
    gather.finish()


def mid(block, out_weight, patches, gain, up, count, collective):
    pieces, tall, rows = block.shape
    width = patches.shape[1]
    return pl.pallas_call(
        functools.partial(mid_kernel, count),
        in_specs=[VMEM, VMEM, VMEM, VMEM, ANY],
        out_specs=VMEM,
        out_shape=jax.ShapeDtypeStruct((rows // 4, up.shape[1]), jnp.bfloat16),
        scratch_shapes=[
            pltpu.VMEM((count,) + block.shape, block.dtype),
            pltpu.VMEM(up.shape, up.dtype),
            pltpu.VMEM((rows, width), jnp.float32),
            pltpu.VMEM((width // 128, rows, 128), jnp.float32),
            pltpu.SemaphoreType.DMA,
        ]
        + ring_sems(count, pieces)
        + [pltpu.SemaphoreType.DMA],
        compiler_params=comm_params(collective),
    )(block, out_weight.reshape(count, pieces * tall, width), patches, gain[None, :], up)


def finish_kernel(seq_count, frame_count, tokens, text, qw, kw, cosine, sine_part, text_out, out, *scratch):
    held, q_held, k_held, mine, load, fsend, frecv, tsend, trecv, vsend, vrecv, own = scratch
    parts, share, span = tokens.shape
    loads = []
    for part in range(parts):
        slab = pl.ds(part * span, span)
        loads.append(pltpu.make_async_copy(qw.at[slab], q_held.at[slab], load.at[0, part]))
        loads.append(pltpu.make_async_copy(kw.at[slab], k_held.at[slab], load.at[1, part]))
    for copy in loads:
        copy.start()
    ring = Ring(seq_count)
    here = ring.index(0)
    frames = FrameGather(frame_count, tokens, held, fsend, frecv, parts)
    texts = RingGather(ring, text, lambda i, piece: text_out.at[i, piece], tsend, trecv, text.shape[0])
    visions = RingGather(ring, mine, lambda i, piece: out.at[i, piece], vsend, vrecv, mine.shape[0])
    greet([ring.left, ring.right] + frames.partners())
    frames.start()
    texts.start()
    keep = [
        pltpu.make_async_copy(tokens, held.at[frames.me], own.at[0]),
        pltpu.make_async_copy(text, text_out.at[here], own.at[1]),
    ]
    for copy in keep:
        copy.start()
    early = texts.steps // 2
    for part in range(parts):
        frames.relay(part)
        if part % 2 and part // 2 < early:
            texts.advance(part // 2)
    for copy in keep:
        copy.wait()
    frames.finish()
    for copy in loads:
        copy.wait()
    q_total, k_total = None, None
    for part in range(parts):
        rows = jnp.concatenate([held[f, part] for f in range(frame_count)], axis=0)
        slab = slice(part * span, (part + 1) * span)
        q_part = jnp.dot(rows, q_held[slab], preferred_element_type=jnp.float32)
        k_part = jnp.dot(rows, k_held[slab], preferred_element_type=jnp.float32)
        q_total = q_part if part == 0 else q_total + q_part
        k_total = k_part if part == 0 else k_total + k_part
    turn, slide = cosine[...], sine_part[...]

    def turned(values):
        return values * turn + pltpu.roll(values, HDIM // 2, 1) * slide

    queries = q_total.shape[1]
    columns = [turned(q_total[:, c : c + HDIM]) for c in range(0, queries, HDIM)]
    columns += [turned(k_total[:, :HDIM]), k_total[:, HDIM:]]
    pieces, tall = mine.shape[:2]
    for i, values in enumerate(columns):
        for piece in range(pieces):
            mine[piece, :, i * HDIM : (i + 1) * HDIM] = values[
                piece * tall : (piece + 1) * tall
            ].astype(mine.dtype)
    visions.start()
    last = pltpu.make_async_copy(mine, out.at[here], own.at[0])
    last.start()
    done = min(early, parts // 2)
    for step in range(max(texts.steps - done, visions.steps)):
        if done + step < texts.steps:
            texts.advance(done + step)
        if step < visions.steps:
            visions.advance(step)
    last.wait()
    texts.finish()
    visions.finish()


def finish(tokens, text, positions, query_weight, keyvalue_weight, seq_count, frame_count, collective):
    parts, share, span = tokens.shape
    rows = frame_count * share
    width = query_weight.shape[1] + keyvalue_weight.shape[1]
    text = text.reshape(2, -1, text.shape[1])
    mine = (2, rows // 2, width)
    cosine, sine_part = turns(positions)
    text_out, out = pl.pallas_call(
        functools.partial(finish_kernel, seq_count, frame_count),
        in_specs=[VMEM, VMEM, ANY, ANY, VMEM, VMEM],
        out_specs=[ANY, ANY],
        out_shape=[
            jax.ShapeDtypeStruct((seq_count,) + text.shape, text.dtype),
            jax.ShapeDtypeStruct((seq_count,) + mine, text.dtype),
        ],
        scratch_shapes=[
            pltpu.VMEM((frame_count,) + tokens.shape, tokens.dtype),
            pltpu.VMEM(query_weight.shape, query_weight.dtype),
            pltpu.VMEM(keyvalue_weight.shape, keyvalue_weight.dtype),
            pltpu.VMEM(mine, text.dtype),
            pltpu.SemaphoreType.DMA((2, parts)),
        ]
        + frame_sems(frame_count, parts)
        + ring_sems(seq_count, 2) * 2
        + [pltpu.SemaphoreType.DMA((2,))],
        compiler_params=comm_params(collective),
    )(tokens, text, query_weight, keyvalue_weight, cosine, sine_part)
    return text_out.reshape(-1, text.shape[-1]), out.reshape(-1, width)


def scatter_kernel(count, hidden, weight, gain, out, held, part, stage, land, load, send, recv):
    ring = Ring(count)
    width = weight.shape[1]
    pieces = held.shape[0]
    span = width // pieces
    share = out.shape[1]
    order = [piece for pair in zip(range(pieces // 2), range(pieces // 2, pieces)) for piece in pair]
    loads = {
        piece: pltpu.make_async_copy(
            weight.at[:, pl.ds(piece * span, span)], held.at[piece], load.at[piece]
        )
        for piece in order
    }
    for piece in order:
        loads[piece].start()
    greet([ring.left, ring.right])
    forward = [piece < pieces // 2 for piece in range(pieces)]

    def hop(piece, step):
        return remote(
            stage.at[piece, step],
            land.at[piece, step],
            send.at[piece, step],
            recv.at[piece, step],
            ring.right if forward[piece] else ring.left,
        )

    for piece in order:
        loads[piece].wait()
        product = jnp.dot(hidden[...], held[piece], preferred_element_type=jnp.float32)
        for i in range(count):
            part[piece, i] = product[i * share : (i + 1) * share]
        first = ring.index(-1 if forward[piece] else 1)
        stage[piece, 0] = part[piece, first].astype(jnp.bfloat16)
        hop(piece, 0).start()

    def body(step, carry):
        for piece in order:
            hop(piece, step - 1).wait_recv()
            turn = -1 - step if forward[piece] else 1 + step
            owner = ring.index(turn)
            total = land[piece, step - 1].astype(jnp.float32) + part[piece, owner]
            stage[piece, step] = total.astype(jnp.bfloat16)
            hop(piece, step).start()
        return carry

    lax.fori_loop(1, count - 1, body, 0)
    here = ring.index(0)
    squares = jnp.zeros((share, 1), jnp.float32)
    for piece in order:
        hop(piece, count - 2).wait_recv()
        total = land[piece, count - 2].astype(jnp.float32) + part[piece, here]
        total = total.astype(jnp.bfloat16).astype(jnp.float32)
        part[piece, here] = total
        squares += jnp.sum(total * total, axis=1, keepdims=True)
    factor = lax.rsqrt(squares / width + epsilon)
    for piece in order:
        columns = slice(piece * span, (piece + 1) * span)
        out[piece] = (part[piece, here] * factor * gain[:, columns]).astype(out.dtype)

    def drain(step, carry):
        for piece in order:
            hop(piece, step).wait_send()
        return carry

    lax.fori_loop(0, count - 1, drain, 0)


def scatter(hidden, weight, gain, count, collective):
    rows, depth = hidden.shape
    width = weight.shape[1]
    share = rows // count
    pieces = 4
    span = width // pieces
    return pl.pallas_call(
        functools.partial(scatter_kernel, count),
        in_specs=[VMEM, ANY, VMEM],
        out_specs=VMEM,
        out_shape=jax.ShapeDtypeStruct((pieces, share, span), jnp.bfloat16),
        scratch_shapes=[
            pltpu.VMEM((pieces, depth, span), jnp.bfloat16),
            pltpu.VMEM((pieces, count, share, span), jnp.float32),
            pltpu.VMEM((pieces, count - 1, share, span), jnp.bfloat16),
            pltpu.VMEM((pieces, count - 1, share, span), jnp.bfloat16),
            pltpu.SemaphoreType.DMA((pieces,)),
            pltpu.SemaphoreType.DMA((pieces, count - 1)),
            pltpu.SemaphoreType.DMA((pieces, count - 1)),
        ],
        compiler_params=comm_params(collective),
    )(hidden, weight, gain[None, :])


def turns(positions):
    inverse = rope_base ** (-2.0 * jnp.arange(HDIM // 2, dtype=jnp.float32) / HDIM)
    angles = positions.astype(jnp.float32)[:, None] * inverse[None, :]
    cosine, sine_part = jnp.cos(angles), jnp.sin(angles)
    return jnp.concatenate([cosine, cosine], axis=1), jnp.concatenate([-sine_part, sine_part], axis=1)


def project_kernel(blocks, *refs):
    tokens, (where, qw, kw, cosine, sine_part, q_out, pair_out, q_acc, p_acc) = refs[:blocks], refs[blocks:]
    step = pl.program_id(0)
    rows = jnp.concatenate([ref[...] for ref in tokens], axis=0)
    q_part = jnp.dot(rows, qw[...], preferred_element_type=jnp.float32)
    p_part = jnp.dot(rows, kw[...], preferred_element_type=jnp.float32)

    @pl.when(step == 0)
    def _():
        q_acc[...] = q_part
        p_acc[...] = p_part

    @pl.when(step > 0)
    def _():
        q_acc[...] += q_part
        p_acc[...] += p_part

    @pl.when(step == pl.num_programs(0) - 1)
    def _():
        share = tokens[0].shape[0]
        for block in range(blocks):
            source = slice(block * share, (block + 1) * share)
            target = pl.ds(pl.multiple_of(where[block] * share, share), share)
            turn, slide = cosine[target, :], sine_part[target, :]
            for head in range(q_acc.shape[1] // HDIM):
                columns = slice(head * HDIM, (head + 1) * HDIM)
                values = q_acc[source, columns]
                q_out[target, columns] = (
                    values * turn + pltpu.roll(values, HDIM // 2, 1) * slide
                ).astype(q_out.dtype)
            values = p_acc[source, :HDIM]
            pair_out[target, :HDIM] = (
                values * turn + pltpu.roll(values, HDIM // 2, 1) * slide
            ).astype(pair_out.dtype)
            pair_out[target, HDIM:] = p_acc[source, HDIM:].astype(pair_out.dtype)


def project(blocks, where, positions, query_weight, keyvalue_weight):
    share, depth = blocks[0].shape
    rows = share * len(blocks)
    queries, pairs = query_weight.shape[1], keyvalue_weight.shape[1]
    slab = math.gcd(depth, 1024)
    cosine, sine_part = turns(positions)
    whole = lambda shape: pl.BlockSpec(shape, lambda k: (0, 0))
    return pl.pallas_call(
        functools.partial(project_kernel, len(blocks)),
        grid=(depth // slab,),
        in_specs=[pl.BlockSpec((share, slab), lambda k: (0, k))] * len(blocks)
        + [
            pl.BlockSpec(memory_space=pltpu.SMEM),
            pl.BlockSpec((slab, queries), lambda k: (k, 0)),
            pl.BlockSpec((slab, pairs), lambda k: (k, 0)),
            whole((rows, HDIM)),
            whole((rows, HDIM)),
        ],
        out_specs=[whole((rows, queries)), whole((rows, pairs))],
        out_shape=[
            jax.ShapeDtypeStruct((rows, queries), jnp.bfloat16),
            jax.ShapeDtypeStruct((rows, pairs), jnp.bfloat16),
        ],
        scratch_shapes=[
            pltpu.VMEM((rows, queries), jnp.float32),
            pltpu.VMEM((rows, pairs), jnp.float32),
        ],
        compiler_params=pltpu.CompilerParams(vmem_limit_bytes=vmem_limit),
    )(*blocks, where, query_weight, keyvalue_weight, cosine, sine_part)


def causal_kernel(block_ref, q_ref, k_ref, v_ref, out_ref):
    rows = q_ref.shape[0]
    queries = q_ref[...]

    def fold(start, state_in, masked):
        running_max, running_sum, weighted = state_in
        scores = lax.dot_general(
            queries,
            k_ref[pl.ds(start, rows), :],
            (((1,), (1,)), ((), ())),
            preferred_element_type=jnp.float32,
        )
        if masked:
            row_id = lax.broadcasted_iota(jnp.int32, (rows, rows), 0)
            column_id = lax.broadcasted_iota(jnp.int32, (rows, rows), 1)
            scores = jnp.where(row_id >= column_id, scores, lowest)
        new_max = jnp.maximum(running_max, jnp.max(scores, axis=1, keepdims=True))
        weights = jnp.exp((scores - new_max) * HDIM ** (-0.5))
        shrink = jnp.exp((running_max - new_max) * HDIM ** (-0.5))
        running_sum = running_sum * shrink + jnp.sum(weights, axis=1, keepdims=True)
        update = jnp.dot(
            weights.astype(jnp.bfloat16),
            v_ref[pl.ds(start, rows), :],
            preferred_element_type=jnp.float32,
        )
        return (new_max, running_sum, weighted * shrink + update)

    state = (
        jnp.full((rows, 1), lowest, jnp.float32),
        jnp.zeros((rows, 1), jnp.float32),
        jnp.zeros((rows, HDIM), jnp.float32),
    )
    own = block_ref[0]
    state = fold(pl.multiple_of(own * rows, rows), state, True)
    _, running_sum, weighted = lax.fori_loop(
        0, own, lambda i, now: fold(pl.multiple_of(i * rows, rows), now, False), state
    )
    out_ref[...] = (weighted / running_sum).astype(out_ref.dtype)


def causal_attention(block_index, queries, key_rows, value_rows):
    rows, width = queries.shape
    keys = key_rows.shape[0]
    return pl.pallas_call(
        causal_kernel,
        grid=(width // HDIM,),
        in_specs=[
            pl.BlockSpec(memory_space=pltpu.SMEM),
            pl.BlockSpec((rows, HDIM), lambda h: (0, h)),
            pl.BlockSpec((keys, HDIM), lambda h: (0, 0)),
            pl.BlockSpec((keys, HDIM), lambda h: (0, 0)),
        ],
        out_specs=pl.BlockSpec((rows, HDIM), lambda h: (0, h)),
        out_shape=jax.ShapeDtypeStruct((rows, width), jnp.bfloat16),
        compiler_params=pltpu.CompilerParams(vmem_limit_bytes=vmem_limit),
    )(block_index[None], queries, key_rows, value_rows)


def place(token_pos, first, text_rows, vision_rows):
    spots = first + jnp.arange(text_rows.shape[0], dtype=jnp.int32)
    hit = spots[:, None] == token_pos[None, :]
    moved = jnp.dot(hit.astype(jnp.bfloat16), vision_rows, preferred_element_type=jnp.float32)
    taken = jnp.any(hit, axis=1, keepdims=True)
    return jnp.where(taken, moved.astype(jnp.bfloat16), text_rows)


def local(
    patches,
    vit_gain,
    vision_qkv,
    vision_out,
    video_ids,
    merge_gain,
    merge_up,
    merge_down,
    vision_pos,
    text_embed,
    llm_gain,
    query_weight,
    keyvalue_weight,
):
    frame_index = lax.axis_index("frame")
    seq_index = lax.axis_index("seq")
    frame_count = lax.axis_size("frame")
    seq_count = lax.axis_size("seq")
    patch_rows = patches.shape[0]
    local_heads = vision_qkv.shape[1] // (3 * VIT_HDIM)
    barrier = lax.optimization_barrier

    normed_patches = rms_scale(patches, vit_gain).astype(jnp.bfloat16)
    projected = lax.dot_general(
        vision_qkv, normed_patches, (((0,), (1,)), ((), ())), preferred_element_type=jnp.float32
    ).astype(jnp.bfloat16)
    projected = projected.reshape(local_heads, 3 * VIT_HDIM, patch_rows)
    vit_query = projected[:, :VIT_HDIM].reshape(local_heads * VIT_HDIM, patch_rows)
    patch_video = jnp.repeat(video_ids, 4)
    own_video = lax.dynamic_slice_in_dim(patch_video, frame_index * patch_rows, patch_rows)
    pair_all, out_full = front(projected[:, VIT_HDIM:], vision_out, seq_count, frame_count, 1)

    text_own = rms_scale(text_embed, llm_gain).astype(jnp.bfloat16)
    text_own, pair_all = barrier((text_own, pair_all))
    text_blocks, owners = [text_own], [0]
    bit = frame_count // 2
    while bit:
        swap = [(i, i ^ bit) for i in range(frame_count)]
        text_blocks = text_blocks + [lax.ppermute(block, "frame", swap) for block in text_blocks]
        owners = owners + [mask ^ bit for mask in owners]
        bit //= 2

    vit_context = vit_attention(own_video, patch_video, vit_query, pair_all)
    pieces = vit_context.reshape(2, -1, patch_rows)
    merge_hidden = mid(pieces, out_full, patches, merge_gain, merge_up, seq_count, 2)
    vision_normed = scatter(merge_hidden, merge_down, llm_gain, seq_count, 3)

    part_rows = text_embed.shape[0]
    seq_block = part_rows * frame_count
    first = seq_index * seq_block
    where = jnp.bitwise_xor(frame_index, jnp.array(owners, jnp.int32))
    text_blocks[-1], vision_normed = barrier((text_blocks[-1], vision_normed))
    text_query, text_pair = project(
        text_blocks, where, first + jnp.arange(seq_block, dtype=jnp.int32), query_weight, keyvalue_weight
    )
    share = vision_normed.shape[1]
    token_pos = vision_pos.reshape(frame_count, seq_count, share).transpose(1, 0, 2)
    here = lax.dynamic_index_in_dim(token_pos, seq_index, 0, keepdims=False).reshape(-1)
    text_pair_all, gathered = finish(
        vision_normed, text_pair, here, query_weight, keyvalue_weight, seq_count, frame_count, 4
    )
    width = query_weight.shape[1]
    token_pos = token_pos.reshape(-1)
    llm_query = place(token_pos, first, text_query, gathered[:, :width])
    llm_pair = place(token_pos, 0, text_pair_all, gathered[:, width:])
    return causal_attention(seq_index, llm_query, llm_pair[:, :HDIM], llm_pair[:, HDIM:])


def solution(mesh):
    return jax.shard_map(
        local,
        mesh=mesh,
        in_specs=(
            P("frame", None),
            P(),
            P(None, "seq"),
            P("seq", None),
            P(),
            P(),
            P(None, "seq"),
            P("seq", None),
            P(),
            P(("seq", "frame"), None),
            P(),
            P(None, "frame"),
            P(None, "frame"),
        ),
        out_specs=P("seq", "frame"),
        check_vma=False,
    )
```

```python
import functools
import math

import jax
import jax.numpy as jnp
from jax import lax
from jax.experimental import pallas as pl
from jax.experimental.pallas import tpu as pltpu
from jax.sharding import PartitionSpec as P

VIT_HDIM = 80
HDIM = 128


epsilon = 1e-06
rope_base = 1000000.0
lowest = -1e30
vmem_limit = 56 * 1024 * 1024


def rms_scale(matrix, scales):
    widened = matrix.astype(jnp.float32)
    factor = lax.rsqrt(jnp.mean(widened * widened, axis=-1, keepdims=True) + epsilon)
    return widened * factor * scales


MESH = pl.DeviceIdType.MESH
ANY = pl.BlockSpec(memory_space=pl.ANY)
VMEM = pl.BlockSpec(memory_space=pltpu.VMEM)


def ring_grid(count):
    narrow = 1 << ((count.bit_length() - 1) // 2)
    return count // narrow, narrow


def ring_position(index, count):
    tall, narrow = ring_grid(count)
    if narrow < 2 or tall % 2:
        return index
    row, column = lax.div(index, narrow), lax.rem(index, narrow)
    odd = lax.rem(row, 2)
    inner = lax.div(column + narrow - 1, narrow)
    along = (column - 1) * (1 - odd) + (narrow - 1 - column) * odd
    return (1 - inner) * (count - 1 - row) + inner * (row * (narrow - 1) + along)


def ring_index(position, count):
    tall, narrow = ring_grid(count)
    if narrow < 2 or tall % 2:
        return position
    back = lax.div(position, tall * (narrow - 1))
    row, along = lax.div(position, narrow - 1), lax.rem(position, narrow - 1)
    odd = lax.rem(row, 2)
    column = 1 + along * (1 - odd) + (narrow - 2 - along) * odd
    return (1 - back) * (row * narrow + column) + back * (count - 1 - position) * narrow


class Ring:
    def __init__(self, count):
        self.count = count
        self.here = ring_position(lax.axis_index("seq"), count)
        self.right = {"seq": self.index(1)}
        self.left = {"seq": self.index(-1)}

    def index(self, offset):
        return ring_index(lax.rem(self.here + (offset + 2 * self.count), self.count), self.count)


def greet(partners):
    barrier = pltpu.get_barrier_semaphore()
    for partner in partners:
        pl.semaphore_signal(barrier, inc=1, device_id=partner, device_id_type=MESH)
    pl.semaphore_wait(barrier, len(partners))


def remote(source, target, send, recv, partner):
    return pltpu.make_async_remote_copy(
        src_ref=source,
        dst_ref=target,
        send_sem=send,
        recv_sem=recv,
        device_id=partner,
        device_id_type=MESH,
    )


class RingGather:
    def __init__(self, ring, block, out, send, recv, pieces):
        self.ring, self.block, self.out, self.send, self.recv = ring, block, out, send, recv
        self.pieces = pieces
        self.steps = ring.count // 2

    def moves(self, step):
        last = step == self.steps - 1
        for piece in range(self.pieces):
            if not last or piece < self.pieces // 2:
                yield 0, piece
            if not last or piece >= self.pieces // 2:
                yield 1, piece

    def copy(self, step, way, piece):
        offset = -step if way == 0 else step
        owner = self.ring.index(offset)
        source = self.block.at[piece] if step == 0 else self.out(owner, piece)
        return remote(
            source,
            self.out(owner, piece),
            self.send.at[way, step, piece],
            self.recv.at[way, step, piece],
            self.ring.right if way == 0 else self.ring.left,
        )

    def start(self):
        for way, piece in self.moves(0):
            self.copy(0, way, piece).start()

    def advance(self, step, landed=None):
        ahead = list(self.moves(step + 1)) if step + 1 < self.steps else []
        for way, piece in self.moves(step):
            self.copy(step, way, piece).wait_recv()
            if (way, piece) in ahead:
                self.copy(step + 1, way, piece).start()
            if landed is not None:
                landed(self.ring.index(-(step + 1) if way == 0 else step + 1), piece, way, step)

    def finish(self):
        for step in range(self.steps):
            for way, piece in self.moves(step):
                self.copy(step, way, piece).wait_send()


def ring_sems(count, pieces):
    return [pltpu.SemaphoreType.DMA((2, count // 2, pieces))] * 2


class FrameGather:
    def __init__(self, count, block, out, sends, recvs, pieces):
        self.block, self.out, self.pieces = block, out, pieces
        self.sends, self.recvs = sends, recvs
        self.chips = count // 2
        me = lax.axis_index("frame")
        self.me, self.chip, self.core = me, lax.div(me, 2), lax.rem(me, 2)
        self.twin = {"frame": self.chip * 2 + 1 - self.core}

    def peer(self, distance):
        return lax.rem(self.chip + distance + self.chips, self.chips) * 2 + self.core

    def partners(self):
        return [self.twin] + [{"frame": self.peer(d)} for d in range(1, self.chips)]

    def across(self, distance, piece):
        return remote(
            self.block.at[piece],
            self.out.at[self.me, piece],
            self.sends.at[0, distance, piece],
            self.recvs.at[0, distance, piece],
            {"frame": self.peer(distance)},
        )

    def inside(self, distance, piece):
        slot = self.peer(-distance)
        return remote(
            self.block.at[piece] if distance == 0 else self.out.at[slot, piece],
            self.out.at[slot, piece],
            self.sends.at[1, distance, piece],
            self.recvs.at[1, distance, piece],
            self.twin,
        )

    def start(self):
        for piece in range(self.pieces):
            for d in range(1, self.chips):
                self.across(d, piece).start()
        for piece in range(self.pieces):
            self.inside(0, piece).start()

    def relay(self, piece):
        for d in range(1, self.chips):
            self.across(d, piece).wait_recv()
            self.inside(d, piece).start()

    def settle(self, piece):
        for d in range(self.chips):
            self.inside(d, piece).wait_recv()

    def finish(self):
        for piece in range(self.pieces):
            for d in range(self.chips):
                self.inside(d, piece).wait_send()
                if d:
                    self.across(d, piece).wait_send()


def frame_sems(count, pieces):
    return [pltpu.SemaphoreType.DMA((2, count // 2, pieces))] * 2


def comm_params(collective):
    return pltpu.CompilerParams(
        collective_id=collective, has_side_effects=True, vmem_limit_bytes=vmem_limit
    )


def encode_kernel(seq_count, frame_count, patches, gain, weight, low, high, out_weight, context, weight_out, *scratch):
    mine, query, held, flat, peak, mass, blend, fsend, frecv, rsend, rrecv, tsend, trecv, own = scratch
    ring = Ring(seq_count)
    heads, tall, rows = mine.shape
    frames = FrameGather(frame_count, mine, held, fsend, frecv, heads)
    core, twin = frames.core, frames.twin
    pieces = out_weight.shape[1]
    gather = RingGather(
        ring, out_weight.at[core], lambda i, piece: weight_out.at[i, core, piece], rsend, rrecv, pieces
    )
    greet([ring.left, ring.right] + frames.partners())
    gather.start()
    keep = pltpu.make_async_copy(out_weight, weight_out.at[ring.index(0)], own.at[0])
    keep.start()
    handed = []

    def landed(index, piece, way, step):
        spot = weight_out.at[index, core, piece]
        copy = remote(spot, spot, tsend.at[way, step, piece], trecv.at[way, step, piece], twin)
        copy.start()
        handed.append(copy)

    widened = patches[...].astype(jnp.float32)
    factor = lax.rsqrt(jnp.mean(widened * widened, axis=-1, keepdims=True) + epsilon)
    normed = (widened * factor * gain[...]).astype(jnp.bfloat16)
    projected = lax.dot_general(
        weight[...], normed, (((0,), (1,)), ((), ())), preferred_element_type=jnp.float32
    ).astype(jnp.bfloat16)
    for head in range(heads):
        base = head * 3 * VIT_HDIM
        query[head] = projected[base : base + VIT_HDIM]
        mine[head] = projected[base + VIT_HDIM : base + 3 * VIT_HDIM]
    frames.start()
    local = pltpu.make_async_copy(mine, held.at[frames.me], own.at[1])
    local.start()
    local.wait()
    near = [frames.chip * 2, frames.chip * 2 + 1]
    far = [
        lax.rem(frames.chip + d, frames.chips) * 2 + c for d in range(1, frames.chips) for c in range(2)
    ]
    tile = math.gcd(rows, 256)
    scale = VIT_HDIM ** (-0.5) * math.log2(math.e)

    def flatten(slots, head):
        for slot in slots:
            flat[slot, head] = held[slot, head, :VIT_HDIM, :].T

    def attend(slots, head, start):
        columns = slice(start, start + tile)
        queries = query[head, :, columns]
        first, past = low[:, columns], high[:, columns]
        scores = []
        for slot in slots:
            part = jnp.dot(flat[slot, head], queries, preferred_element_type=jnp.float32)
            spot = slot * rows + lax.broadcasted_iota(jnp.int32, part.shape, 0)
            scores.append(jnp.where((spot >= first) & (spot < past), part, lowest))
        scores = jnp.concatenate(scores, axis=0)
        highest = jnp.max(scores, axis=0, keepdims=True)
        weights = jnp.exp2((scores - highest) * scale)
        total = jnp.sum(weights, axis=0, keepdims=True)
        weights = weights.astype(jnp.bfloat16)
        mixed = sum(
            jnp.dot(
                held[slot, head, VIT_HDIM:, :],
                weights[i * rows : (i + 1) * rows],
                preferred_element_type=jnp.float32,
            )
            for i, slot in enumerate(slots)
        )
        return highest, total, mixed

    def first_pass(head):
        flatten(near, head)
        for start in range(0, rows, tile):
            columns = slice(start, start + tile)
            highest, total, mixed = attend(near, head, start)
            peak[head : head + 1, columns] = highest
            mass[head : head + 1, columns] = total
            blend[head, :, columns] = mixed

    def second_pass(head):
        if far:
            flatten(far, head)
        for start in range(0, rows, tile):
            columns = slice(start, start + tile)
            total, mixed = mass[head : head + 1, columns], blend[head, :, columns]
            if far:
                before = peak[head : head + 1, columns]
                highest, more, extra = attend(far, head, start)
                joint = jnp.maximum(before, highest)
                old, new = jnp.exp2((before - joint) * scale), jnp.exp2((highest - joint) * scale)
                total = total * old + more * new
                mixed = mixed * old + extra * new
            context[head, :, columns] = (mixed / total).astype(context.dtype)

    gather.advance(0, landed)
    for head in range(heads):
        frames.inside(0, head).wait_recv()
        first_pass(head)
        frames.relay(head)
        if head + 1 < gather.steps:
            gather.advance(head + 1, landed)
    for head in range(heads):
        for d in range(1, frames.chips):
            frames.inside(d, head).wait_recv()
        second_pass(head)
        if heads + head + 1 < gather.steps:
            gather.advance(heads + head + 1, landed)
    for step in range(2 * heads + 1, gather.steps):
        gather.advance(step, landed)
    keep.wait()
    frames.finish()
    gather.finish()
    for copy in handed:
        copy.wait()


def encode(patches, gain, weight, low, high, out_weight, seq_count, frame_count, collective):
    rows = patches.shape[0]
    heads = weight.shape[1] // (3 * VIT_HDIM)
    half = out_weight.shape[0] // 2
    tall = math.gcd(half, 16)
    pieces = half // tall
    out_weight = out_weight.reshape(2, pieces, tall, -1)
    context, weight_out = pl.pallas_call(
        functools.partial(encode_kernel, seq_count, frame_count),
        in_specs=[VMEM] * 6,
        out_specs=[VMEM, ANY],
        out_shape=[
            jax.ShapeDtypeStruct((heads, VIT_HDIM, rows), jnp.bfloat16),
            jax.ShapeDtypeStruct((seq_count,) + out_weight.shape, out_weight.dtype),
        ],
        scratch_shapes=[
            pltpu.VMEM((heads, 2 * VIT_HDIM, rows), jnp.bfloat16),
            pltpu.VMEM((heads, VIT_HDIM, rows), jnp.bfloat16),
            pltpu.VMEM((frame_count, heads, 2 * VIT_HDIM, rows), jnp.bfloat16),
            pltpu.VMEM((frame_count, heads, rows, VIT_HDIM), jnp.bfloat16),
            pltpu.VMEM((heads, rows), jnp.float32),
            pltpu.VMEM((heads, rows), jnp.float32),
            pltpu.VMEM((heads, VIT_HDIM, rows), jnp.float32),
        ]
        + frame_sems(frame_count, heads)
        + ring_sems(seq_count, pieces) * 2
        + [pltpu.SemaphoreType.DMA((2,))],
        compiler_params=comm_params(collective),
    )(patches, gain[None, :], weight, low[None, :], high[None, :], out_weight)
    return context, weight_out.reshape(seq_count, 2 * half, -1)


def mid_kernel(
    count, frame_count, block, out_weight, patches, gain, text, up, hidden, text_out,
    held, up_held, total, spread, load, send, recv, fsend, frecv, own
):
    load_up = pltpu.make_async_copy(up, up_held, load)
    load_up.start()
    ring = Ring(count)
    pieces, tall, rows = block.shape
    share = pieces * tall
    gather = RingGather(ring, block, lambda i, piece: held.at[i, piece], send, recv, pieces)
    parts = text_out.shape[1]
    frames = FrameGather(frame_count, text, text_out, fsend, frecv, parts)
    greet([ring.left, ring.right] + frames.partners())
    gather.start()
    frames.start()
    keep = pltpu.make_async_copy(block, held.at[ring.index(0)], own.at[0])
    keep.start()
    aside = pltpu.make_async_copy(text.at[pl.ds(0, parts)], text_out.at[frames.me], own.at[1])
    aside.start()

    def fold(offsets, first):
        owners = [ring.index(offset) for offset in offsets]
        left = jnp.concatenate([held[i].reshape(share, rows) for i in owners], axis=0)
        right = jnp.concatenate([out_weight[i] for i in owners], axis=0)
        product = lax.dot_general(
            left, right, (((0,), (0,)), ((), ())), preferred_element_type=jnp.float32
        )
        if first:
            total[...] = patches[...].astype(jnp.float32) + product
        else:
            total[...] += product

    half = max(gather.steps // 2, 1)
    keep.wait()
    for step in range(gather.steps):
        gather.advance(step)
        if step < parts:
            frames.relay(step)
        if step == half - 1:
            fold(range(-half, half + 1), True)
    if gather.steps > half:
        rest = list(range(half + 1, gather.steps)) + list(range(-gather.steps, -half))
        fold(rest, False)
    width = total.shape[1]
    values = total[...]
    factor = lax.rsqrt(jnp.mean(values * values, axis=1, keepdims=True) + epsilon)
    values = values * factor * gain[...]
    lanes = spread.shape[2]
    for c in range(width // lanes):
        spread[c] = values[:, c * lanes : (c + 1) * lanes]
    load_up.wait()
    result = sum(
        jnp.dot(
            jnp.concatenate(
                [spread[c, pl.ds(r, rows // 4, stride=4), :] for c in range(width // lanes)], axis=1
            ).astype(jnp.bfloat16),
            up_held[r * width : (r + 1) * width, :],
            preferred_element_type=jnp.float32,
        )
        for r in range(4)
    )
    hidden[...] = (0.5 * result * (1.0 + lax.erf(result * 0.5**0.5))).astype(hidden.dtype)
    aside.wait()
    for part in range(parts):
        if part >= gather.steps:
            frames.relay(part)
        frames.settle(part)
    frames.finish()
    gather.finish()


def mid(block, out_weight, patches, gain, text, up, count, frame_count, collective):
    pieces, tall, rows = block.shape
    width = patches.shape[1]
    parts = text.shape[0] // 2
    return pl.pallas_call(
        functools.partial(mid_kernel, count, frame_count),
        in_specs=[VMEM] * 5 + [ANY],
        out_specs=[VMEM, ANY],
        out_shape=[
            jax.ShapeDtypeStruct((rows // 4, up.shape[1]), jnp.bfloat16),
            jax.ShapeDtypeStruct((frame_count, parts) + text.shape[1:], text.dtype),
        ],
        scratch_shapes=[
            pltpu.VMEM((count,) + block.shape, block.dtype),
            pltpu.VMEM(up.shape, up.dtype),
            pltpu.VMEM((rows, width), jnp.float32),
            pltpu.VMEM((width // 128, rows, 128), jnp.float32),
            pltpu.SemaphoreType.DMA,
        ]
        + ring_sems(count, pieces)
        + frame_sems(frame_count, parts)
        + [pltpu.SemaphoreType.DMA((2,))],
        compiler_params=comm_params(collective),
    )(block, out_weight, patches, gain[None, :], text, up)


def finish_kernel(seq_count, frame_count, tokens, text, qw, kw, cosine, sine_part, text_out, out, *scratch):
    held, q_held, k_held, mine, load, fsend, frecv, tsend, trecv, vsend, vrecv, own = scratch
    parts, share, span = tokens.shape
    loads = []
    for part in range(parts):
        slab = pl.ds(part * span, span)
        loads.append(pltpu.make_async_copy(qw.at[slab], q_held.at[slab], load.at[0, part]))
        loads.append(pltpu.make_async_copy(kw.at[slab], k_held.at[slab], load.at[1, part]))
    for copy in loads:
        copy.start()
    ring = Ring(seq_count)
    here = ring.index(0)
    frames = FrameGather(frame_count, tokens, held, fsend, frecv, parts)
    texts = RingGather(ring, text, lambda i, piece: text_out.at[i, piece], tsend, trecv, text.shape[0])
    visions = RingGather(ring, mine, lambda i, piece: out.at[i, piece], vsend, vrecv, mine.shape[0])
    greet([ring.left, ring.right] + frames.partners())
    frames.start()
    texts.start()
    keep = [
        pltpu.make_async_copy(tokens, held.at[frames.me], own.at[0]),
        pltpu.make_async_copy(text, text_out.at[here], own.at[1]),
    ]
    for copy in keep:
        copy.start()
    early = texts.steps // 2
    for part in range(parts):
        frames.relay(part)
        if part % 2 and part // 2 < early:
            texts.advance(part // 2)
    for copy in keep:
        copy.wait()
    for part in range(parts):
        frames.settle(part)
    frames.finish()
    for copy in loads:
        copy.wait()
    q_total, k_total = None, None
    for part in range(parts):
        rows = jnp.concatenate([held[f, part] for f in range(frame_count)], axis=0)
        slab = slice(part * span, (part + 1) * span)
        q_part = jnp.dot(rows, q_held[slab], preferred_element_type=jnp.float32)
        k_part = jnp.dot(rows, k_held[slab], preferred_element_type=jnp.float32)
        q_total = q_part if part == 0 else q_total + q_part
        k_total = k_part if part == 0 else k_total + k_part
    turn, slide = cosine[...], sine_part[...]

    def turned(values):
        return values * turn + pltpu.roll(values, HDIM // 2, 1) * slide

    queries = q_total.shape[1]
    columns = [turned(q_total[:, c : c + HDIM]) for c in range(0, queries, HDIM)]
    columns += [turned(k_total[:, :HDIM]), k_total[:, HDIM:]]
    pieces, tall = mine.shape[:2]
    for i, values in enumerate(columns):
        for piece in range(pieces):
            mine[piece, :, i * HDIM : (i + 1) * HDIM] = values[
                piece * tall : (piece + 1) * tall
            ].astype(mine.dtype)
    visions.start()
    last = pltpu.make_async_copy(mine, out.at[here], own.at[0])
    last.start()
    done = min(early, parts // 2)
    for step in range(max(texts.steps - done, visions.steps)):
        if done + step < texts.steps:
            texts.advance(done + step)
        if step < visions.steps:
            visions.advance(step)
    last.wait()
    texts.finish()
    visions.finish()


def finish(tokens, text, positions, query_weight, keyvalue_weight, seq_count, frame_count, collective):
    parts, share, span = tokens.shape
    rows = frame_count * share
    width = query_weight.shape[1] + keyvalue_weight.shape[1]
    text = text.reshape(2, -1, text.shape[1])
    mine = (2, rows // 2, width)
    cosine, sine_part = turns(positions)
    text_out, out = pl.pallas_call(
        functools.partial(finish_kernel, seq_count, frame_count),
        in_specs=[VMEM, VMEM, ANY, ANY, VMEM, VMEM],
        out_specs=[ANY, ANY],
        out_shape=[
            jax.ShapeDtypeStruct((seq_count,) + text.shape, text.dtype),
            jax.ShapeDtypeStruct((seq_count,) + mine, text.dtype),
        ],
        scratch_shapes=[
            pltpu.VMEM((frame_count,) + tokens.shape, tokens.dtype),
            pltpu.VMEM(query_weight.shape, query_weight.dtype),
            pltpu.VMEM(keyvalue_weight.shape, keyvalue_weight.dtype),
            pltpu.VMEM(mine, text.dtype),
            pltpu.SemaphoreType.DMA((2, parts)),
        ]
        + frame_sems(frame_count, parts)
        + ring_sems(seq_count, 2) * 2
        + [pltpu.SemaphoreType.DMA((2,))],
        compiler_params=comm_params(collective),
    )(tokens, text, query_weight, keyvalue_weight, cosine, sine_part)
    return text_out.reshape(-1, text.shape[-1]), out.reshape(-1, width)


def scatter_kernel(
    count, frame_count, hidden, weight, gain, text, near, qw, kw, cosine, sine_part, out, q_out, pair_out, *scratch
):
    held, part, stage, land, q_held, k_held, early, late, sums, load, send, recv, fsend, frecv, own = scratch
    ring = Ring(count)
    width = weight.shape[1]
    pieces = held.shape[0]
    span = width // pieces
    share = out.shape[1]
    order = [piece for pair in zip(range(pieces // 2), range(pieces // 2, pieces)) for piece in pair]
    loads = {
        piece: pltpu.make_async_copy(
            weight.at[:, pl.ds(piece * span, span)], held.at[piece], load.at[piece]
        )
        for piece in order
    }
    for piece in order:
        loads[piece].start()
    extra = [
        pltpu.make_async_copy(near, early, own.at[0]),
        pltpu.make_async_copy(qw, q_held, own.at[1]),
        pltpu.make_async_copy(kw, k_held, own.at[2]),
    ]
    for copy in extra:
        copy.start()
    parts, tall, depth = early.shape[1:]
    last = text.at[pl.ds(text.shape[0] - late.shape[1], late.shape[1])]
    frames = FrameGather(frame_count, last, late, fsend, frecv, late.shape[1])
    greet([ring.left, ring.right] + frames.partners())
    frames.start()
    aside = pltpu.make_async_copy(last, late.at[frames.me], own.at[3])
    aside.start()
    forward = [piece < pieces // 2 for piece in range(pieces)]

    def hop(piece, step):
        return remote(
            stage.at[piece, step],
            land.at[piece, step],
            send.at[piece, step],
            recv.at[piece, step],
            ring.right if forward[piece] else ring.left,
        )

    for piece in order:
        loads[piece].wait()
        product = jnp.dot(hidden[...], held[piece], preferred_element_type=jnp.float32)
        for i in range(count):
            part[piece, i] = product[i * share : (i + 1) * share]
        first = ring.index(-1 if forward[piece] else 1)
        stage[piece, 0] = part[piece, first].astype(jnp.bfloat16)
        hop(piece, 0).start()
    for copy in extra:
        copy.wait()
    sums[...] = jnp.zeros_like(sums)
    slabs = 8
    slab = depth // slabs
    queries = qw.shape[1]

    def project(source, spot, index):
        columns = pl.ds(pl.multiple_of(index * slab, slab), slab)
        rows = source[:, :, :, columns].reshape(-1, slab)
        count_rows = rows.shape[0]
        sums[spot, :, :queries] += jnp.dot(rows, q_held[columns, :], preferred_element_type=jnp.float32)
        sums[spot, :, queries:] += jnp.dot(rows, k_held[columns, :], preferred_element_type=jnp.float32)

    def advance(step, group):
        for piece in group:
            hop(piece, step - 1).wait_recv()
            owner = ring.index(-1 - step if forward[piece] else 1 + step)
            total = land[piece, step - 1].astype(jnp.float32) + part[piece, owner]
            stage[piece, step] = total.astype(jnp.bfloat16)
            hop(piece, step).start()

    groups = [order[:2], order[2:]]
    turn_over = 1 + slabs // 2

    def opening(step, carry):
        for i, group in enumerate(groups):
            advance(step, group)
            project(early, 0, 2 * (step - 1) + i)

        @pl.when(step <= late.shape[1])
        def _():
            frames.relay(step - 1)

        return carry

    lax.fori_loop(1, turn_over, opening, 0)
    aside.wait()
    for piece in range(late.shape[1]):
        frames.settle(piece)
    each = -(-slabs // (2 * (count - 1 - turn_over)))

    def closing(step, carry):
        for i, group in enumerate(groups):
            advance(step, group)
            unit = 2 * (step - turn_over) + i
            start = jnp.minimum(unit * each, slabs)
            stop = jnp.minimum(start + each, slabs)

            def fold(index, inner):
                project(late, 1, index)
                return inner

            lax.fori_loop(start, stop, fold, 0)
        return carry

    lax.fori_loop(turn_over, count - 1, closing, 0)
    block = 2 * parts * tall
    for f in range(frame_count):
        for spot in range(2):
            source = slice(f * parts * tall, (f + 1) * parts * tall)
            begin = f * block + spot * parts * tall
            target = slice(begin, begin + parts * tall)
            turn, slide = cosine[target], sine_part[target]
            for c in range(0, queries + HDIM, HDIM):
                values = sums[spot, source, c : c + HDIM]
                values = (values * turn + pltpu.roll(values, HDIM // 2, 1) * slide).astype(q_out.dtype)
                if c < queries:
                    q_out[target, c : c + HDIM] = values
                else:
                    pair_out[target, :HDIM] = values
            pair_out[target, HDIM:] = sums[spot, source, queries + HDIM :].astype(pair_out.dtype)
    here = ring.index(0)
    squares = jnp.zeros((share, 1), jnp.float32)
    for piece in order:
        hop(piece, count - 2).wait_recv()
        total = land[piece, count - 2].astype(jnp.float32) + part[piece, here]
        total = total.astype(jnp.bfloat16).astype(jnp.float32)
        part[piece, here] = total
        squares += jnp.sum(total * total, axis=1, keepdims=True)
    factor = lax.rsqrt(squares / width + epsilon)
    for piece in order:
        columns = slice(piece * span, (piece + 1) * span)
        out[piece] = (part[piece, here] * factor * gain[:, columns]).astype(out.dtype)

    def drain(step, carry):
        for piece in order:
            hop(piece, step).wait_send()
        return carry

    lax.fori_loop(0, count - 1, drain, 0)
    frames.finish()


def scatter(hidden, weight, gain, text, near, query_weight, keyvalue_weight, positions, count, frame_count, collective):
    rows, depth = hidden.shape
    width = weight.shape[1]
    share = rows // count
    pieces = 4
    span = width // pieces
    parts, tall = text.shape[:2]
    tokens = frame_count * parts * tall
    queries, pairs = query_weight.shape[1], keyvalue_weight.shape[1]
    left = parts - near.shape[1]
    cosine, sine_part = turns(positions)
    return pl.pallas_call(
        functools.partial(scatter_kernel, count, frame_count),
        in_specs=[VMEM, ANY, VMEM, VMEM, ANY, ANY, ANY, VMEM, VMEM],
        out_specs=[VMEM, VMEM, VMEM],
        out_shape=[
            jax.ShapeDtypeStruct((pieces, share, span), jnp.bfloat16),
            jax.ShapeDtypeStruct((tokens, queries), jnp.bfloat16),
            jax.ShapeDtypeStruct((tokens, pairs), jnp.bfloat16),
        ],
        scratch_shapes=[
            pltpu.VMEM((pieces, depth, span), jnp.bfloat16),
            pltpu.VMEM((pieces, count, share, span), jnp.float32),
            pltpu.VMEM((pieces, count - 1, share, span), jnp.bfloat16),
            pltpu.VMEM((pieces, count - 1, share, span), jnp.bfloat16),
            pltpu.VMEM(query_weight.shape, query_weight.dtype),
            pltpu.VMEM(keyvalue_weight.shape, keyvalue_weight.dtype),
            pltpu.VMEM(near.shape, near.dtype),
            pltpu.VMEM((frame_count, left) + text.shape[1:], text.dtype),
            pltpu.VMEM((2, tokens // 2, queries + pairs), jnp.float32),
            pltpu.SemaphoreType.DMA((pieces,)),
            pltpu.SemaphoreType.DMA((pieces, count - 1)),
            pltpu.SemaphoreType.DMA((pieces, count - 1)),
        ]
        + frame_sems(frame_count, left)
        + [pltpu.SemaphoreType.DMA((4,))],
        compiler_params=pltpu.CompilerParams(
            collective_id=collective, has_side_effects=True, vmem_limit_bytes=63 * 1024 * 1024
        ),
    )(hidden, weight, gain[None, :], text, near, query_weight, keyvalue_weight, cosine, sine_part)


def turns(positions):
    inverse = rope_base ** (-2.0 * jnp.arange(HDIM // 2, dtype=jnp.float32) / HDIM)
    angles = positions.astype(jnp.float32)[:, None] * inverse[None, :]
    cosine, sine_part = jnp.cos(angles), jnp.sin(angles)
    return jnp.concatenate([cosine, cosine], axis=1), jnp.concatenate([-sine_part, sine_part], axis=1)


def causal_kernel(block_ref, q_ref, k_ref, v_ref, out_ref):
    rows = q_ref.shape[0]
    queries = q_ref[...]

    def fold(start, state_in, masked):
        running_max, running_sum, weighted = state_in
        scores = lax.dot_general(
            queries,
            k_ref[pl.ds(start, rows), :],
            (((1,), (1,)), ((), ())),
            preferred_element_type=jnp.float32,
        )
        if masked:
            row_id = lax.broadcasted_iota(jnp.int32, (rows, rows), 0)
            column_id = lax.broadcasted_iota(jnp.int32, (rows, rows), 1)
            scores = jnp.where(row_id >= column_id, scores, lowest)
        new_max = jnp.maximum(running_max, jnp.max(scores, axis=1, keepdims=True))
        weights = jnp.exp((scores - new_max) * HDIM ** (-0.5))
        shrink = jnp.exp((running_max - new_max) * HDIM ** (-0.5))
        running_sum = running_sum * shrink + jnp.sum(weights, axis=1, keepdims=True)
        update = jnp.dot(
            weights.astype(jnp.bfloat16),
            v_ref[pl.ds(start, rows), :],
            preferred_element_type=jnp.float32,
        )
        return (new_max, running_sum, weighted * shrink + update)

    state = (
        jnp.full((rows, 1), lowest, jnp.float32),
        jnp.zeros((rows, 1), jnp.float32),
        jnp.zeros((rows, HDIM), jnp.float32),
    )
    own = block_ref[0]
    state = fold(pl.multiple_of(own * rows, rows), state, True)
    _, running_sum, weighted = lax.fori_loop(
        0, own, lambda i, now: fold(pl.multiple_of(i * rows, rows), now, False), state
    )
    out_ref[...] = (weighted / running_sum).astype(out_ref.dtype)


def causal_attention(block_index, queries, key_rows, value_rows):
    rows, width = queries.shape
    keys = key_rows.shape[0]
    return pl.pallas_call(
        causal_kernel,
        grid=(width // HDIM,),
        in_specs=[
            pl.BlockSpec(memory_space=pltpu.SMEM),
            pl.BlockSpec((rows, HDIM), lambda h: (0, h)),
            pl.BlockSpec((keys, HDIM), lambda h: (0, 0)),
            pl.BlockSpec((keys, HDIM), lambda h: (0, 0)),
        ],
        out_specs=pl.BlockSpec((rows, HDIM), lambda h: (0, h)),
        out_shape=jax.ShapeDtypeStruct((rows, width), jnp.bfloat16),
        compiler_params=pltpu.CompilerParams(vmem_limit_bytes=vmem_limit),
    )(block_index[None], queries, key_rows, value_rows)


def place(token_pos, first, text_rows, vision_rows):
    spots = first + jnp.arange(text_rows.shape[0], dtype=jnp.int32)
    hit = spots[:, None] == token_pos[None, :]
    moved = jnp.dot(hit.astype(jnp.bfloat16), vision_rows, preferred_element_type=jnp.float32)
    taken = jnp.any(hit, axis=1, keepdims=True)
    return jnp.where(taken, moved.astype(jnp.bfloat16), text_rows)


def local(
    patches,
    vit_gain,
    vision_qkv,
    vision_out,
    video_ids,
    merge_gain,
    merge_up,
    merge_down,
    vision_pos,
    text_embed,
    llm_gain,
    query_weight,
    keyvalue_weight,
):
    frame_index = lax.axis_index("frame")
    seq_index = lax.axis_index("seq")
    frame_count = lax.axis_size("frame")
    seq_count = lax.axis_size("seq")
    patch_rows = patches.shape[0]
    token_rows = patch_rows // 4
    own_video = lax.dynamic_slice_in_dim(video_ids, frame_index * token_rows, token_rows)
    low = jnp.sum((video_ids[None, :] < own_video[:, None]).astype(jnp.int32), axis=1)
    high = jnp.sum((video_ids[None, :] <= own_video[:, None]).astype(jnp.int32), axis=1)
    context, out_full = encode(
        patches, vit_gain, vision_qkv, jnp.repeat(4 * low, 4), jnp.repeat(4 * high, 4), vision_out,
        seq_count, frame_count, 1,
    )
    part_rows = text_embed.shape[0]
    seq_block = part_rows * frame_count
    first = seq_index * seq_block
    text_own = rms_scale(text_embed, llm_gain).astype(jnp.bfloat16)
    text_own = text_own.reshape(-1, 16, text_own.shape[1])
    merge_hidden, text_near = mid(
        context, out_full, patches, merge_gain, text_own, merge_up, seq_count, frame_count, 2
    )
    vision_normed, text_query, text_pair = scatter(
        merge_hidden, merge_down, llm_gain, text_own, text_near, query_weight, keyvalue_weight,
        first + jnp.arange(seq_block, dtype=jnp.int32), seq_count, frame_count, 3,
    )
    share = vision_normed.shape[1]
    token_pos = vision_pos.reshape(frame_count, seq_count, share).transpose(1, 0, 2)
    here = lax.dynamic_index_in_dim(token_pos, seq_index, 0, keepdims=False).reshape(-1)
    text_pair_all, gathered = finish(
        vision_normed, text_pair, here, query_weight, keyvalue_weight, seq_count, frame_count, 4
    )
    width = query_weight.shape[1]
    token_pos = token_pos.reshape(-1)
    llm_query = place(token_pos, first, text_query, gathered[:, :width])
    llm_pair = place(token_pos, 0, text_pair_all, gathered[:, width:])
    return causal_attention(seq_index, llm_query, llm_pair[:, :HDIM], llm_pair[:, HDIM:])


def solution(mesh):
    return jax.shard_map(
        local,
        mesh=mesh,
        in_specs=(
            P("frame", None),
            P(),
            P(None, "seq"),
            P("seq", None),
            P(),
            P(),
            P(None, "seq"),
            P("seq", None),
            P(),
            P(("seq", "frame"), None),
            P(),
            P(None, "frame"),
            P(None, "frame"),
        ),
        out_specs=P("seq", "frame"),
        check_vma=False,
    )
```

```python
import functools
import math

import jax
import jax.numpy as jnp
from jax import lax
from jax.experimental import pallas as pl
from jax.experimental.pallas import tpu as pltpu
from jax.sharding import PartitionSpec as P

VIT_HDIM = 80
VIDEOS = 3
HDIM = 128


epsilon = 1e-06
rope_base = 1000000.0
lowest = -1e30
vmem_limit = 56 * 1024 * 1024

MESH = pl.DeviceIdType.MESH
ANY = pl.BlockSpec(memory_space=pl.ANY)
VMEM = pl.BlockSpec(memory_space=pltpu.VMEM)


def ring_grid(count):
    narrow = 1 << ((count.bit_length() - 1) // 2)
    return count // narrow, narrow


def ring_position(index, count):
    tall, narrow = ring_grid(count)
    if narrow < 2 or tall % 2:
        return index
    row, column = lax.div(index, narrow), lax.rem(index, narrow)
    odd = lax.rem(row, 2)
    inner = lax.div(column + narrow - 1, narrow)
    along = (column - 1) * (1 - odd) + (narrow - 1 - column) * odd
    return (1 - inner) * (count - 1 - row) + inner * (row * (narrow - 1) + along)


def ring_index(position, count):
    tall, narrow = ring_grid(count)
    if narrow < 2 or tall % 2:
        return position
    back = lax.div(position, tall * (narrow - 1))
    row, along = lax.div(position, narrow - 1), lax.rem(position, narrow - 1)
    odd = lax.rem(row, 2)
    column = 1 + along * (1 - odd) + (narrow - 2 - along) * odd
    return (1 - back) * (row * narrow + column) + back * (count - 1 - position) * narrow


class Ring:
    def __init__(self, count):
        self.count = count
        self.here = ring_position(lax.axis_index("seq"), count)
        self.right = {"seq": self.index(1)}
        self.left = {"seq": self.index(-1)}

    def index(self, offset):
        return ring_index(lax.rem(self.here + (offset + 2 * self.count), self.count), self.count)


def greet(partners):
    barrier = pltpu.get_barrier_semaphore()
    for partner in partners:
        pl.semaphore_signal(barrier, inc=1, device_id=partner, device_id_type=MESH)
    pl.semaphore_wait(barrier, len(partners))


def remote(source, target, send, recv, partner):
    return pltpu.make_async_remote_copy(
        src_ref=source,
        dst_ref=target,
        send_sem=send,
        recv_sem=recv,
        device_id=partner,
        device_id_type=MESH,
    )


class RingGather:
    def __init__(self, ring, block, out, send, recv, pieces):
        self.ring, self.block, self.out, self.send, self.recv = ring, block, out, send, recv
        self.pieces = pieces
        self.steps = ring.count // 2

    def moves(self, step):
        last = step == self.steps - 1
        for piece in range(self.pieces):
            if not last or piece < self.pieces // 2:
                yield 0, piece
            if not last or piece >= self.pieces // 2:
                yield 1, piece

    def copy(self, step, way, piece):
        offset = -step if way == 0 else step
        owner = self.ring.index(offset)
        source = self.block.at[piece] if step == 0 else self.out(owner, piece)
        return remote(
            source,
            self.out(owner, piece),
            self.send.at[way, step, piece],
            self.recv.at[way, step, piece],
            self.ring.right if way == 0 else self.ring.left,
        )

    def start(self):
        for way, piece in self.moves(0):
            self.copy(0, way, piece).start()

    def advance(self, step, landed=None):
        ahead = list(self.moves(step + 1)) if step + 1 < self.steps else []
        for way, piece in self.moves(step):
            self.copy(step, way, piece).wait_recv()
            if (way, piece) in ahead:
                self.copy(step + 1, way, piece).start()
            if landed is not None:
                landed(self.ring.index(-(step + 1) if way == 0 else step + 1), piece, way, step)

    def finish(self):
        for step in range(self.steps):
            for way, piece in self.moves(step):
                self.copy(step, way, piece).wait_send()


def ring_sems(count, pieces):
    return [pltpu.SemaphoreType.DMA((2, count // 2, pieces))] * 2


class FrameGather:
    def __init__(self, count, block, out, sends, recvs, pieces):
        self.block, self.out, self.pieces = block, out, pieces
        self.sends, self.recvs = sends, recvs
        self.chips = count // 2
        me = lax.axis_index("frame")
        self.me, self.chip, self.core = me, lax.div(me, 2), lax.rem(me, 2)
        self.twin = {"frame": self.chip * 2 + 1 - self.core}

    def peer(self, distance):
        return lax.rem(self.chip + distance + self.chips, self.chips) * 2 + self.core

    def partners(self):
        return [self.twin] + [{"frame": self.peer(d)} for d in range(1, self.chips)]

    def across(self, distance, piece):
        return remote(
            self.block.at[piece],
            self.out.at[self.me, piece],
            self.sends.at[0, distance, piece],
            self.recvs.at[0, distance, piece],
            {"frame": self.peer(distance)},
        )

    def inside(self, distance, piece):
        slot = self.peer(-distance)
        return remote(
            self.block.at[piece] if distance == 0 else self.out.at[slot, piece],
            self.out.at[slot, piece],
            self.sends.at[1, distance, piece],
            self.recvs.at[1, distance, piece],
            self.twin,
        )

    def start(self):
        for piece in range(self.pieces):
            for d in range(1, self.chips):
                self.across(d, piece).start()
        for piece in range(self.pieces):
            self.inside(0, piece).start()

    def relay(self, piece):
        for d in range(1, self.chips):
            self.across(d, piece).wait_recv()
            self.inside(d, piece).start()

    def settle(self, piece):
        for d in range(self.chips):
            self.inside(d, piece).wait_recv()

    def finish(self):
        for piece in range(self.pieces):
            for d in range(self.chips):
                self.inside(d, piece).wait_send()
                if d:
                    self.across(d, piece).wait_send()


def frame_sems(count, pieces):
    return [pltpu.SemaphoreType.DMA((2, count // 2, pieces))] * 2


def comm_params(collective):
    return pltpu.CompilerParams(
        collective_id=collective, has_side_effects=True, vmem_limit_bytes=vmem_limit
    )


def encode_kernel(
    seq_count, frame_count, patches, gain, weight, ids, out_weight, text, text_gain, context, weight_out, text_out, *scratch
):
    mine, query, held, flat, peak, mass, blend, fsend, frecv, rsend, rrecv, tsend, trecv, own = scratch
    ring = Ring(seq_count)
    heads, tall, rows = mine.shape
    frames = FrameGather(frame_count, mine, held, fsend, frecv, heads)
    core, twin = frames.core, frames.twin
    pieces = out_weight.shape[1]
    gather = RingGather(
        ring, out_weight.at[core], lambda i, piece: weight_out.at[i, core, piece], rsend, rrecv, pieces
    )
    greet([ring.left, ring.right] + frames.partners())
    gather.start()
    keep = pltpu.make_async_copy(out_weight, weight_out.at[ring.index(0)], own.at[0])
    keep.start()
    handed = []

    def landed(index, piece, way, step):
        spot = weight_out.at[index, core, piece]
        copy = remote(spot, spot, tsend.at[way, step, piece], trecv.at[way, step, piece], twin)
        copy.start()
        handed.append(copy)

    widened = patches[...].astype(jnp.float32)
    factor = lax.rsqrt(jnp.mean(widened * widened, axis=-1, keepdims=True) + epsilon)
    normed = (widened * factor * gain[...]).astype(jnp.bfloat16)
    projected = lax.dot_general(
        weight[...], normed, (((1,), (1,)), ((), ())), preferred_element_type=jnp.float32
    ).astype(jnp.bfloat16)
    for head in range(heads):
        base = head * 3 * VIT_HDIM
        query[head] = projected[base : base + VIT_HDIM]
        mine[head] = projected[base + VIT_HDIM : base + 3 * VIT_HDIM]
    frames.start()
    local = pltpu.make_async_copy(mine, held.at[frames.me], own.at[1])
    local.start()
    per_token = frame_count * rows // ids.shape[1]
    ends = [
        per_token * jnp.sum((ids[...] <= video).astype(jnp.int32), axis=1, keepdims=True)
        for video in range(VIDEOS - 1)
    ]
    local.wait()
    near = [frames.chip * 2, frames.chip * 2 + 1]
    far = [
        lax.rem(frames.chip + d, frames.chips) * 2 + c for d in range(1, frames.chips) for c in range(2)
    ]
    tile = math.gcd(rows, 256)
    scale = VIT_HDIM ** (-0.5) * math.log2(math.e)

    def flatten(slots, head):
        for slot in slots:
            flat[slot, head] = held[slot, head, :VIT_HDIM, :].T

    def attend(slots, head, start):
        columns = pl.ds(start, tile)
        queries = query[head, :, columns]
        places = frames.me * rows + start + lax.broadcasted_iota(jnp.int32, (1, tile), 1)
        first = jnp.zeros((1, tile), jnp.int32)
        past = jnp.full((1, tile), frame_count * rows, jnp.int32)
        for end in ends:
            first = jnp.where(places >= end, end, first)
        for end in reversed(ends):
            past = jnp.where(places < end, end, past)
        scores = []
        for slot in slots:
            part = jnp.dot(flat[slot, head], queries, preferred_element_type=jnp.float32)
            spot = slot * rows + lax.broadcasted_iota(jnp.int32, part.shape, 0)
            scores.append(jnp.where((spot >= first) & (spot < past), part, lowest))
        scores = jnp.concatenate(scores, axis=0)
        highest = jnp.max(scores, axis=0, keepdims=True)
        weights = jnp.exp2((scores - highest) * scale)
        total = jnp.sum(weights, axis=0, keepdims=True)
        weights = weights.astype(jnp.bfloat16)
        mixed = sum(
            jnp.dot(
                held[slot, head, VIT_HDIM:, :],
                weights[i * rows : (i + 1) * rows],
                preferred_element_type=jnp.float32,
            )
            for i, slot in enumerate(slots)
        )
        return highest, total, mixed

    def first_pass(head):
        flatten(near, head)

        def one(index, carry):
            start = pl.multiple_of(index * tile, tile)
            columns = pl.ds(start, tile)
            highest, total, mixed = attend(near, head, start)
            peak[head : head + 1, columns] = highest
            mass[head : head + 1, columns] = total
            blend[head, :, columns] = mixed
            return carry

        lax.fori_loop(0, rows // tile, one, 0)

    def norm_text(index):
        words = text[index].astype(jnp.float32)
        level = lax.rsqrt(jnp.mean(words * words, axis=-1, keepdims=True) + epsilon)
        text_out[index] = (words * level * text_gain[...]).astype(text_out.dtype)

    def second_pass(head):
        if far:
            flatten(far, head)

        def one(index, carry):
            start = pl.multiple_of(index * tile, tile)
            columns = pl.ds(start, tile)
            total, mixed = mass[head : head + 1, columns], blend[head, :, columns]
            if far:
                before = peak[head : head + 1, columns]
                highest, more, extra = attend(far, head, start)
                joint = jnp.maximum(before, highest)
                old, new = jnp.exp2((before - joint) * scale), jnp.exp2((highest - joint) * scale)
                total = total * old + more * new
                mixed = mixed * old + extra * new
            context[head, :, columns] = (mixed / total).astype(context.dtype)
            return carry

        lax.fori_loop(0, rows // tile, one, 0)

    gather.advance(0, landed)
    for head in range(heads):
        frames.inside(0, head).wait_recv()
        first_pass(head)
        for index in range(head, text.shape[0], heads):
            norm_text(index)
        frames.relay(head)
        if head + 1 < gather.steps:
            gather.advance(head + 1, landed)
    for head in range(heads):
        for d in range(1, frames.chips):
            frames.inside(d, head).wait_recv()
        second_pass(head)
        if heads + head + 1 < gather.steps:
            gather.advance(heads + head + 1, landed)
    for step in range(2 * heads + 1, gather.steps):
        gather.advance(step, landed)
    keep.wait()
    frames.finish()
    gather.finish()
    for copy in handed:
        copy.wait()


def encode(patches, gain, weight, ids, out_weight, text, text_gain, seq_count, frame_count, collective):
    rows = patches.shape[0]
    heads = weight.shape[1] // (3 * VIT_HDIM)
    half = out_weight.shape[0] // 2
    tall = math.gcd(half, 16)
    pieces = half // tall
    out_weight = out_weight.reshape(2, pieces, tall, -1)
    text = text.reshape(-1, 16, text.shape[1])
    context, weight_out, text_out = pl.pallas_call(
        functools.partial(encode_kernel, seq_count, frame_count),
        in_specs=[VMEM] * 7,
        out_specs=[VMEM, ANY, VMEM],
        out_shape=[
            jax.ShapeDtypeStruct((heads, VIT_HDIM, rows), jnp.bfloat16),
            jax.ShapeDtypeStruct((seq_count,) + out_weight.shape, out_weight.dtype),
            jax.ShapeDtypeStruct(text.shape, text.dtype),
        ],
        scratch_shapes=[
            pltpu.VMEM((heads, 2 * VIT_HDIM, rows), jnp.bfloat16),
            pltpu.VMEM((heads, VIT_HDIM, rows), jnp.bfloat16),
            pltpu.VMEM((frame_count, heads, 2 * VIT_HDIM, rows), jnp.bfloat16),
            pltpu.VMEM((frame_count, heads, rows, VIT_HDIM), jnp.bfloat16),
            pltpu.VMEM((heads, rows), jnp.float32),
            pltpu.VMEM((heads, rows), jnp.float32),
            pltpu.VMEM((heads, VIT_HDIM, rows), jnp.float32),
        ]
        + frame_sems(frame_count, heads)
        + ring_sems(seq_count, pieces) * 2
        + [pltpu.SemaphoreType.DMA((2,))],
        compiler_params=comm_params(collective),
    )(patches, gain[None, :], weight.T, ids[None, :], out_weight, text, text_gain[None, :])
    return context, weight_out.reshape(seq_count, 2 * half, -1), text_out


def mid_kernel(
    count, frame_count, block, out_weight, patches, gain, text, up, hidden, text_out,
    held, up_held, total, spread, load, send, recv, fsend, frecv, own
):
    load_up = pltpu.make_async_copy(up, up_held, load)
    load_up.start()
    ring = Ring(count)
    pieces, tall, rows = block.shape
    share = pieces * tall
    gather = RingGather(ring, block, lambda i, piece: held.at[i, piece], send, recv, pieces)
    parts = text_out.shape[1]
    frames = FrameGather(frame_count, text, text_out, fsend, frecv, parts)
    greet([ring.left, ring.right] + frames.partners())
    gather.start()
    frames.start()
    keep = pltpu.make_async_copy(block, held.at[ring.index(0)], own.at[0])
    keep.start()
    aside = pltpu.make_async_copy(text.at[pl.ds(0, parts)], text_out.at[frames.me], own.at[1])
    aside.start()

    def fold(offsets, first):
        owners = [ring.index(offset) for offset in offsets]
        left = jnp.concatenate([held[i].reshape(share, rows) for i in owners], axis=0)
        right = jnp.concatenate([out_weight[i] for i in owners], axis=0)
        product = lax.dot_general(
            left, right, (((0,), (0,)), ((), ())), preferred_element_type=jnp.float32
        )
        if first:
            total[...] = patches[...].astype(jnp.float32) + product
        else:
            total[...] += product

    half = max(gather.steps // 2, 1)
    keep.wait()
    for step in range(gather.steps):
        gather.advance(step)
        if step < parts:
            frames.relay(step)
        if step == half - 1:
            fold(range(-half, half + 1), True)
    if gather.steps > half:
        rest = list(range(half + 1, gather.steps)) + list(range(-gather.steps, -half))
        fold(rest, False)
    width = total.shape[1]
    values = total[...]
    factor = lax.rsqrt(jnp.mean(values * values, axis=1, keepdims=True) + epsilon)
    values = values * factor * gain[...]
    lanes = spread.shape[2]
    for c in range(width // lanes):
        spread[c] = values[:, c * lanes : (c + 1) * lanes]
    load_up.wait()
    result = sum(
        jnp.dot(
            jnp.concatenate(
                [spread[c, pl.ds(r, rows // 4, stride=4), :] for c in range(width // lanes)], axis=1
            ).astype(jnp.bfloat16),
            up_held[r * width : (r + 1) * width, :],
            preferred_element_type=jnp.float32,
        )
        for r in range(4)
    )
    hidden[...] = (0.5 * result * (1.0 + lax.erf(result * 0.5**0.5))).astype(hidden.dtype)
    aside.wait()
    for part in range(parts):
        if part >= gather.steps:
            frames.relay(part)
        frames.settle(part)
    frames.finish()
    gather.finish()


def mid(block, out_weight, patches, gain, text, up, count, frame_count, collective):
    pieces, tall, rows = block.shape
    width = patches.shape[1]
    parts = text.shape[0] // 2
    return pl.pallas_call(
        functools.partial(mid_kernel, count, frame_count),
        in_specs=[VMEM] * 5 + [ANY],
        out_specs=[VMEM, ANY],
        out_shape=[
            jax.ShapeDtypeStruct((rows // 4, up.shape[1]), jnp.bfloat16),
            jax.ShapeDtypeStruct((frame_count, parts) + text.shape[1:], text.dtype),
        ],
        scratch_shapes=[
            pltpu.VMEM((count,) + block.shape, block.dtype),
            pltpu.VMEM(up.shape, up.dtype),
            pltpu.VMEM((rows, width), jnp.float32),
            pltpu.VMEM((width // 128, rows, 128), jnp.float32),
            pltpu.SemaphoreType.DMA,
        ]
        + ring_sems(count, pieces)
        + frame_sems(frame_count, parts)
        + [pltpu.SemaphoreType.DMA((2,))],
        compiler_params=comm_params(collective),
    )(block, out_weight, patches, gain[None, :], text, up)


def finish_kernel(
    seq_count, frame_count, tokens, text, query, covered, spots, qw, kw, cosine, sine_part, result, *scratch
):
    (held, q_held, k_held, mine, pair, vision, peak, mass, blend, select, locate,
     load, fsend, frecv, tsend, trecv, vsend, vrecv, own) = scratch
    parts, share, span = tokens.shape
    loads = []
    for part in range(parts):
        slab = pl.ds(part * span, span)
        loads.append(pltpu.make_async_copy(qw.at[slab], q_held.at[slab], load.at[0, part]))
        loads.append(pltpu.make_async_copy(kw.at[slab], k_held.at[slab], load.at[1, part]))
    for copy in loads:
        copy.start()
    ring = Ring(seq_count)
    here = ring.index(0)
    frames = FrameGather(frame_count, tokens, held, fsend, frecv, parts)
    texts = RingGather(ring, text, lambda i, piece: pair.at[i, piece], tsend, trecv, text.shape[0])
    visions = RingGather(ring, mine, lambda i, piece: vision.at[i, piece], vsend, vrecv, mine.shape[0])
    greet([ring.left, ring.right] + frames.partners())
    frames.start()
    texts.start()
    keep = [
        pltpu.make_async_copy(tokens, held.at[frames.me], own.at[0]),
        pltpu.make_async_copy(text, pair.at[here], own.at[1]),
    ]
    for copy in keep:
        copy.start()
    rows, queries = query.shape
    heads = queries // HDIM
    couple = 2 if heads % 2 == 0 else 1
    scale = HDIM ** (-0.5) * math.log2(math.e)
    total = spots.shape[1]
    slots = locate.shape[0]

    inside = (spots[...] >= here * rows) & (spots[...] < (here + 1) * rows)
    ahead = lax.broadcasted_iota(jnp.int32, (total, total), 0) < lax.broadcasted_iota(
        jnp.int32, (total, total), 1
    )
    flags = jnp.where(inside, 1.0, 0.0)
    rank = jnp.dot(
        jnp.broadcast_to(flags, (8, total)).astype(jnp.bfloat16),
        jnp.where(ahead, 1.0, 0.0).astype(jnp.bfloat16),
        preferred_element_type=jnp.float32,
    )[:1]
    slot = lax.broadcasted_iota(jnp.int32, (slots, total), 0).astype(jnp.float32)
    chosen = jnp.where(inside & (slot == rank), 1.0, 0.0)
    select[...] = chosen.astype(select.dtype)
    locate[...] = jnp.sum(chosen * (spots[...] + 1 - here * rows).astype(jnp.float32), axis=1, keepdims=True) - 1.0

    def keys_of(block):
        return pair[block].reshape(rows, 2 * HDIM)

    def weigh(scores, highest):
        weights = jnp.exp2((scores - highest) * scale)
        return weights.astype(jnp.bfloat16), jnp.sum(weights, axis=1, keepdims=True)

    def score(left, right):
        return lax.dot_general(left, right, (((1,), (1,)), ((), ())), preferred_element_type=jnp.float32)

    def fold(head, scores, values):
        before = peak[head]
        highest = jnp.maximum(before, jnp.max(scores, axis=1, keepdims=True))
        weights, more = weigh(scores, highest)
        shrink = jnp.exp2((before - highest) * scale)
        peak[head] = highest
        mass[head] = mass[head] * shrink + more
        blend[head] = blend[head] * shrink + jnp.dot(weights, values, preferred_element_type=jnp.float32)

    def query_of(group, j):
        return query[:, pl.ds(pl.multiple_of((group * couple + j) * HDIM, HDIM), HDIM)]

    groups = heads // couple

    def diagonal(group):
        block = text[...].reshape(rows, 2 * HDIM)
        lower = lax.broadcasted_iota(jnp.int32, (rows, rows), 0) >= lax.broadcasted_iota(
            jnp.int32, (rows, rows), 1
        )
        for j in range(couple):
            head = group * couple + j
            scores = score(query_of(group, j), block[:, :HDIM]) + covered[here, :1, :]
            scores = jnp.where(lower, scores, lowest)
            highest = jnp.max(scores, axis=1, keepdims=True)
            weights, more = weigh(scores, highest)
            peak[head] = highest
            mass[head] = more
            blend[head] = jnp.dot(weights, block[:, HDIM:], preferred_element_type=jnp.float32)

    def earlier(group, owner):
        block = keys_of(owner)
        for j in range(couple):
            scores = score(query_of(group, j), block[:, :HDIM]) + covered[owner, :1, :]
            fold(group * couple + j, scores, block[:, HDIM:])

    def vision_rows():
        for part in range(parts):
            frames.settle(part)
        frames.finish()
        for copy in keep:
            copy.wait()
        for copy in loads:
            copy.wait()
        q_total, k_total = None, None
        for part in range(parts):
            lines = jnp.concatenate([held[f, part] for f in range(frame_count)], axis=0)
            slab = slice(part * span, (part + 1) * span)
            q_part = jnp.dot(lines, q_held[slab], preferred_element_type=jnp.float32)
            k_part = jnp.dot(lines, k_held[slab], preferred_element_type=jnp.float32)
            q_total = q_part if part == 0 else q_total + q_part
            k_total = k_part if part == 0 else k_total + k_part
        turn, slide = cosine[...], sine_part[...]

        def turned(values):
            return values * turn + pltpu.roll(values, HDIM // 2, 1) * slide

        columns = [turned(q_total[:, c : c + HDIM]) for c in range(0, queries, HDIM)]
        columns += [turned(k_total[:, :HDIM]), k_total[:, HDIM:]]
        pieces, tall = mine.shape[:2]
        for i, values in enumerate(columns):
            for piece in range(pieces):
                mine[piece, :, i * HDIM : (i + 1) * HDIM] = values[
                    piece * tall : (piece + 1) * tall
                ].astype(mine.dtype)
        visions.start()
        pltpu.make_async_copy(mine, vision.at[here], own.at[2]).start()

    units = groups * seq_count
    events = {}

    def at(unit, action):
        events.setdefault(min(unit, units - 1), []).append(action)

    for part in range(parts):
        at([0, 1, 2, 3][part] if part < 4 else 3, functools.partial(frames.relay, part))
    stride = 2 * groups
    for step in range(texts.steps):
        at(groups - 1 + stride * step, functools.partial(texts.advance, step))
    at(groups + 2, vision_rows)
    for step in range(visions.steps):
        at(groups + 5 + 3 * step, functools.partial(visions.advance, step))

    def body(unit, carry):
        turn_of, group = lax.div(unit, groups), lax.rem(unit, groups)
        far, odd = lax.div(turn_of + 1, 2), lax.rem(turn_of, 2)
        owner = ring_index(
            lax.rem(ring.here + far * (1 - 2 * odd) + 2 * seq_count, seq_count), seq_count
        )

        @pl.when(turn_of == 0)
        def _():
            diagonal(group)

        @pl.when((turn_of > 0) & (owner < here))
        def _():
            earlier(group, owner)

        for index, actions in sorted(events.items()):

            def act(actions=actions):
                for action in actions:
                    action()

            pl.when(unit == index)(act)
        return carry

    lax.fori_loop(0, units, body, 0)
    pltpu.make_async_copy(mine, vision.at[here], own.at[2]).wait()

    both = vision[...].reshape(total, queries + 2 * HDIM)
    vision_keys, vision_values = both[:, queries : queries + HDIM], both[:, queries + HDIM :]
    places = here * rows + lax.broadcasted_iota(jnp.int32, (rows, 1), 0)
    for head in range(heads):
        scores = score(query[:, head * HDIM : (head + 1) * HDIM], vision_keys)
        fold(head, jnp.where(spots[...] <= places, scores, lowest), vision_values)

    picked = jnp.dot(select[...], both[:, :queries], preferred_element_type=jnp.float32).astype(jnp.bfloat16)
    stacked = jnp.concatenate([picked[:, c : c + HDIM] for c in range(0, queries, HDIM)], axis=0)
    spot = jnp.concatenate([locate[...]] * heads, axis=0)

    def add(state, scores, values):
        before, amount, mixed = state
        highest = jnp.maximum(before, jnp.max(scores, axis=1, keepdims=True))
        weights, more = weigh(scores, highest)
        shrink = jnp.exp2((before - highest) * scale)
        mixed = mixed * shrink + jnp.dot(weights, values, preferred_element_type=jnp.float32)
        return highest, amount * shrink + more, mixed

    tall = stacked.shape[0]
    state = (
        jnp.full((tall, 1), lowest, jnp.float32),
        jnp.zeros((tall, 1), jnp.float32),
        jnp.zeros((tall, HDIM), jnp.float32),
    )
    seen = (spots[...] - here * rows).astype(jnp.float32)
    state = add(state, jnp.where(seen <= spot, score(stacked, vision_keys), lowest), vision_values)
    block = text[...].reshape(rows, 2 * HDIM)
    column = lax.broadcasted_iota(jnp.int32, (1, rows), 1).astype(jnp.float32)
    scores = score(stacked, block[:, :HDIM]) + covered[here, :1, :]
    state = add(state, jnp.where(column <= spot, scores, lowest), block[:, HDIM:])

    def past(owner, now):
        block = keys_of(owner)
        return add(now, score(stacked, block[:, :HDIM]) + covered[owner, :1, :], block[:, HDIM:])

    _, amount, mixed = lax.fori_loop(0, here, past, state)
    mixed = (mixed / amount).astype(jnp.bfloat16)
    picked = jnp.concatenate([mixed[h * slots : (h + 1) * slots] for h in range(heads)], axis=1)
    column = lax.broadcasted_iota(jnp.int32, (slots, rows), 1).astype(jnp.float32)
    spread = jnp.where(column == locate[...], 1.0, 0.0).astype(jnp.bfloat16)
    back = (((0,), (0,)), ((), ()))
    moved = lax.dot_general(spread, picked, back, preferred_element_type=jnp.float32)
    taken = lax.dot_general(
        spread, jnp.ones((slots, HDIM), jnp.bfloat16), back, preferred_element_type=jnp.float32
    )
    for head in range(heads):
        columns = slice(head * HDIM, (head + 1) * HDIM)
        kept = blend[head] / mass[head]
        result[:, columns] = jnp.where(taken > 0.5, moved[:, columns], kept).astype(result.dtype)
    texts.finish()
    visions.finish()


def finish(tokens, text, query, covered, spots, tables, query_weight, keyvalue_weight, seq_count, frame_count, collective):
    parts, share, span = tokens.shape
    lines = frame_count * share
    rows, queries = query.shape
    heads = queries // HDIM
    width = queries + keyvalue_weight.shape[1]
    slots = frame_count * -(-3 * share // 2)
    text = text.reshape(2, -1, text.shape[1])
    mine = (2, lines // 2, width)
    cosine, sine_part = tables
    return pl.pallas_call(
        functools.partial(finish_kernel, seq_count, frame_count),
        in_specs=[VMEM] * 5 + [ANY] * 2 + [VMEM] * 2,
        out_specs=VMEM,
        out_shape=jax.ShapeDtypeStruct((rows, queries), jnp.bfloat16),
        scratch_shapes=[
            pltpu.VMEM((frame_count,) + tokens.shape, tokens.dtype),
            pltpu.VMEM(query_weight.shape, query_weight.dtype),
            pltpu.VMEM(keyvalue_weight.shape, keyvalue_weight.dtype),
            pltpu.VMEM(mine, text.dtype),
            pltpu.VMEM((seq_count,) + text.shape, text.dtype),
            pltpu.VMEM((seq_count,) + mine, text.dtype),
            pltpu.VMEM((heads, rows, 1), jnp.float32),
            pltpu.VMEM((heads, rows, 1), jnp.float32),
            pltpu.VMEM((heads, rows, HDIM), jnp.float32),
            pltpu.VMEM((slots, seq_count * lines), jnp.bfloat16),
            pltpu.VMEM((slots, 1), jnp.float32),
            pltpu.SemaphoreType.DMA((2, parts)),
        ]
        + frame_sems(frame_count, parts)
        + ring_sems(seq_count, 2) * 2
        + [pltpu.SemaphoreType.DMA((3,))],
        compiler_params=comm_params(collective),
    )(tokens, text, query, covered, spots, query_weight, keyvalue_weight, cosine, sine_part)


def scatter_kernel(
    count, frame_count, hidden, weight, gain, text, near, qw, kw, cosine, sine_part, spots,
    out, q_out, pair_out, covered, *scratch
):
    held, part, stage, land, q_held, k_held, early, late, sums, load, send, recv, fsend, frecv, own = scratch
    ring = Ring(count)
    width = weight.shape[1]
    pieces = held.shape[0]
    span = width // pieces
    share = out.shape[1]
    order = [piece for pair in zip(range(pieces // 2), range(pieces // 2, pieces)) for piece in pair]
    loads = {
        piece: pltpu.make_async_copy(
            weight.at[:, pl.ds(piece * span, span)], held.at[piece], load.at[piece]
        )
        for piece in order
    }
    for piece in order:
        loads[piece].start()
    extra = [
        pltpu.make_async_copy(near, early, own.at[0]),
        pltpu.make_async_copy(qw, q_held, own.at[1]),
        pltpu.make_async_copy(kw, k_held, own.at[2]),
    ]
    for copy in extra:
        copy.start()
    parts, tall, depth = early.shape[1:]
    last = text.at[pl.ds(text.shape[0] - late.shape[1], late.shape[1])]
    frames = FrameGather(frame_count, last, late, fsend, frecv, late.shape[1])
    greet([ring.left, ring.right] + frames.partners())
    frames.start()
    aside = pltpu.make_async_copy(last, late.at[frames.me], own.at[3])
    aside.start()
    forward = [piece < pieces // 2 for piece in range(pieces)]

    def hop(piece, step):
        return remote(
            stage.at[piece, step],
            land.at[piece, step],
            send.at[piece, step],
            recv.at[piece, step],
            ring.right if forward[piece] else ring.left,
        )

    for piece in order:
        loads[piece].wait()
        product = jnp.dot(hidden[...], held[piece], preferred_element_type=jnp.float32)
        for i in range(count):
            part[piece, i] = product[i * share : (i + 1) * share]
        first = ring.index(-1 if forward[piece] else 1)
        stage[piece, 0] = part[piece, first].astype(jnp.bfloat16)
        hop(piece, 0).start()
    for copy in extra:
        copy.wait()
    sums[...] = jnp.zeros_like(sums)
    slabs = 8
    slab = depth // slabs
    queries = qw.shape[1]

    def project(source, spot, index):
        columns = pl.ds(pl.multiple_of(index * slab, slab), slab)
        rows = source[:, :, :, columns].reshape(-1, slab)
        count_rows = rows.shape[0]
        sums[spot, :, :queries] += jnp.dot(rows, q_held[columns, :], preferred_element_type=jnp.float32)
        sums[spot, :, queries:] += jnp.dot(rows, k_held[columns, :], preferred_element_type=jnp.float32)

    def advance(step, group):
        for piece in group:
            hop(piece, step - 1).wait_recv()
            owner = ring.index(-1 - step if forward[piece] else 1 + step)
            total = land[piece, step - 1].astype(jnp.float32) + part[piece, owner]
            stage[piece, step] = total.astype(jnp.bfloat16)
            hop(piece, step).start()

    def cover(block):
        shape = (covered.shape[2], spots.shape[1])
        keys = block * shape[0] + lax.broadcasted_iota(jnp.int32, shape, 0)
        hits = (keys == spots[...]).astype(jnp.float32).astype(jnp.bfloat16)
        total = lax.dot_general(
            jnp.ones((covered.shape[1], shape[1]), jnp.bfloat16),
            hits,
            (((1,), (1,)), ((), ())),
            preferred_element_type=jnp.float32,
        )
        covered[block] = jnp.where(total > 0.5, lowest, 0.0)

    groups = [order[:2], order[2:]]
    turn_over = 1 + slabs // 2

    def opening(step, carry):
        for i, group in enumerate(groups):
            advance(step, group)
            project(early, 0, 2 * (step - 1) + i)
            for block in range(count // slabs):
                cover((2 * (step - 1) + i) * (count // slabs) + block)

        @pl.when(step <= late.shape[1])
        def _():
            frames.relay(step - 1)

        return carry

    lax.fori_loop(1, turn_over, opening, 0)
    aside.wait()
    for piece in range(late.shape[1]):
        frames.settle(piece)
    each = -(-slabs // (2 * (count - 1 - turn_over)))

    def closing(step, carry):
        for i, group in enumerate(groups):
            advance(step, group)
            unit = 2 * (step - turn_over) + i
            start = jnp.minimum(unit * each, slabs)
            stop = jnp.minimum(start + each, slabs)

            def fold(index, inner):
                project(late, 1, index)
                return inner

            lax.fori_loop(start, stop, fold, 0)
        return carry

    lax.fori_loop(turn_over, count - 1, closing, 0)
    block = 2 * parts * tall
    for f in range(frame_count):
        for spot in range(2):
            source = slice(f * parts * tall, (f + 1) * parts * tall)
            begin = f * block + spot * parts * tall
            target = slice(begin, begin + parts * tall)
            turn, slide = cosine[target], sine_part[target]
            for c in range(0, queries + HDIM, HDIM):
                values = sums[spot, source, c : c + HDIM]
                values = (values * turn + pltpu.roll(values, HDIM // 2, 1) * slide).astype(q_out.dtype)
                if c < queries:
                    q_out[target, c : c + HDIM] = values
                else:
                    pair_out[target, :HDIM] = values
            pair_out[target, HDIM:] = sums[spot, source, queries + HDIM :].astype(pair_out.dtype)
    here = ring.index(0)
    squares = jnp.zeros((share, 1), jnp.float32)
    for piece in order:
        hop(piece, count - 2).wait_recv()
        total = land[piece, count - 2].astype(jnp.float32) + part[piece, here]
        total = total.astype(jnp.bfloat16).astype(jnp.float32)
        part[piece, here] = total
        squares += jnp.sum(total * total, axis=1, keepdims=True)
    factor = lax.rsqrt(squares / width + epsilon)
    for piece in order:
        columns = slice(piece * span, (piece + 1) * span)
        out[piece] = (part[piece, here] * factor * gain[:, columns]).astype(out.dtype)

    def drain(step, carry):
        for piece in order:
            hop(piece, step).wait_send()
        return carry

    lax.fori_loop(0, count - 1, drain, 0)
    frames.finish()


def scatter(hidden, weight, gain, text, near, query_weight, keyvalue_weight, tables, spots, count, frame_count, collective):
    rows, depth = hidden.shape
    width = weight.shape[1]
    share = rows // count
    pieces = 4
    span = width // pieces
    parts, tall = text.shape[:2]
    tokens = frame_count * parts * tall
    queries, pairs = query_weight.shape[1], keyvalue_weight.shape[1]
    left = parts - near.shape[1]
    cosine, sine_part = tables
    return pl.pallas_call(
        functools.partial(scatter_kernel, count, frame_count),
        in_specs=[VMEM, ANY, VMEM, VMEM, ANY, ANY, ANY, VMEM, VMEM, VMEM],
        out_specs=[VMEM, VMEM, VMEM, VMEM],
        out_shape=[
            jax.ShapeDtypeStruct((pieces, share, span), jnp.bfloat16),
            jax.ShapeDtypeStruct((tokens, queries), jnp.bfloat16),
            jax.ShapeDtypeStruct((tokens, pairs), jnp.bfloat16),
            jax.ShapeDtypeStruct((count, 8, tokens), jnp.float32),
        ],
        scratch_shapes=[
            pltpu.VMEM((pieces, depth, span), jnp.bfloat16),
            pltpu.VMEM((pieces, count, share, span), jnp.float32),
            pltpu.VMEM((pieces, count - 1, share, span), jnp.bfloat16),
            pltpu.VMEM((pieces, count - 1, share, span), jnp.bfloat16),
            pltpu.VMEM(query_weight.shape, query_weight.dtype),
            pltpu.VMEM(keyvalue_weight.shape, keyvalue_weight.dtype),
            pltpu.VMEM(near.shape, near.dtype),
            pltpu.VMEM((frame_count, left) + text.shape[1:], text.dtype),
            pltpu.VMEM((2, tokens // 2, queries + pairs), jnp.float32),
            pltpu.SemaphoreType.DMA((pieces,)),
            pltpu.SemaphoreType.DMA((pieces, count - 1)),
            pltpu.SemaphoreType.DMA((pieces, count - 1)),
        ]
        + frame_sems(frame_count, left)
        + [pltpu.SemaphoreType.DMA((4,))],
        compiler_params=pltpu.CompilerParams(
            collective_id=collective, has_side_effects=True, vmem_limit_bytes=63 * 1024 * 1024
        ),
    )(hidden, weight, gain[None, :], text, near, query_weight, keyvalue_weight, cosine, sine_part, spots)


def turns(positions):
    lanes = jnp.arange(HDIM, dtype=jnp.int32)
    inverse = rope_base ** (-2.0 * (lanes % (HDIM // 2)).astype(jnp.float32) / HDIM)
    angles = positions.astype(jnp.float32)[:, None] * inverse[None, :]
    return jnp.cos(angles), jnp.where(lanes < HDIM // 2, -1.0, 1.0) * jnp.sin(angles)


def local(
    patches,
    vit_gain,
    vision_qkv,
    vision_out,
    video_ids,
    merge_gain,
    merge_up,
    merge_down,
    vision_pos,
    text_embed,
    llm_gain,
    query_weight,
    keyvalue_weight,
):
    frame_index = lax.axis_index("frame")
    seq_index = lax.axis_index("seq")
    frame_count = lax.axis_size("frame")
    seq_count = lax.axis_size("seq")
    patch_rows = patches.shape[0]
    context, out_full, text_own = encode(
        patches, vit_gain, vision_qkv, video_ids, vision_out, text_embed, llm_gain, seq_count, frame_count, 1
    )
    merge_hidden, text_near = mid(
        context, out_full, patches, merge_gain, text_own, merge_up, seq_count, frame_count, 2
    )
    seq_block = text_embed.shape[0] * frame_count
    share = patch_rows // (4 * seq_count)
    token_pos = vision_pos.reshape(frame_count, seq_count, share).transpose(1, 0, 2)
    here = lax.dynamic_index_in_dim(token_pos, seq_index, 0, keepdims=False).reshape(-1)
    spots = token_pos.reshape(1, -1)
    vision_normed, text_query, text_pair, covered = scatter(
        merge_hidden, merge_down, llm_gain, text_own, text_near, query_weight, keyvalue_weight,
        turns(seq_index * seq_block + jnp.arange(seq_block, dtype=jnp.int32)), spots,
        seq_count, frame_count, 3,
    )
    return finish(
        vision_normed, text_pair, text_query, covered, spots, turns(here), query_weight, keyvalue_weight,
        seq_count, frame_count, 4,
    )


def solution(mesh):
    return jax.shard_map(
        local,
        mesh=mesh,
        in_specs=(
            P("frame", None),
            P(),
            P(None, "seq"),
            P("seq", None),
            P(),
            P(),
            P(None, "seq"),
            P("seq", None),
            P(),
            P(("seq", "frame"), None),
            P(),
            P(None, "frame"),
            P(None, "frame"),
        ),
        out_specs=P("seq", "frame"),
        check_vma=False,
    )
```

```python
import functools
import math

import jax
import jax.numpy as jnp
from jax import lax
from jax.experimental import pallas as pl
from jax.experimental.pallas import tpu as pltpu
from jax.sharding import PartitionSpec as P

VIT_HDIM = 80
VIDEOS = 3
HDIM = 128


epsilon = 1e-06
rope_base = 1000000.0
lowest = -1e30
vmem_limit = 56 * 1024 * 1024

MESH = pl.DeviceIdType.MESH
ANY = pl.BlockSpec(memory_space=pl.ANY)
VMEM = pl.BlockSpec(memory_space=pltpu.VMEM)


def ring_grid(count):
    narrow = 1 << ((count.bit_length() - 1) // 2)
    return count // narrow, narrow


def ring_position(index, count):
    tall, narrow = ring_grid(count)
    if narrow < 2 or tall % 2:
        return index
    row, column = lax.div(index, narrow), lax.rem(index, narrow)
    odd = lax.rem(row, 2)
    inner = lax.div(column + narrow - 1, narrow)
    along = (column - 1) * (1 - odd) + (narrow - 1 - column) * odd
    return (1 - inner) * (count - 1 - row) + inner * (row * (narrow - 1) + along)


def ring_index(position, count):
    tall, narrow = ring_grid(count)
    if narrow < 2 or tall % 2:
        return position
    back = lax.div(position, tall * (narrow - 1))
    row, along = lax.div(position, narrow - 1), lax.rem(position, narrow - 1)
    odd = lax.rem(row, 2)
    column = 1 + along * (1 - odd) + (narrow - 2 - along) * odd
    return (1 - back) * (row * narrow + column) + back * (count - 1 - position) * narrow


class Ring:
    def __init__(self, count):
        self.count = count
        self.here = ring_position(lax.axis_index("seq"), count)
        self.right = {"seq": self.index(1)}
        self.left = {"seq": self.index(-1)}

    def index(self, offset):
        return ring_index(lax.rem(self.here + (offset + 2 * self.count), self.count), self.count)


def greet(partners):
    barrier = pltpu.get_barrier_semaphore()
    for partner in partners:
        pl.semaphore_signal(barrier, inc=1, device_id=partner, device_id_type=MESH)
    pl.semaphore_wait(barrier, len(partners))


def remote(source, target, send, recv, partner):
    return pltpu.make_async_remote_copy(
        src_ref=source,
        dst_ref=target,
        send_sem=send,
        recv_sem=recv,
        device_id=partner,
        device_id_type=MESH,
    )


class RingGather:
    def __init__(self, ring, block, out, send, recv, pieces):
        self.ring, self.block, self.out, self.send, self.recv = ring, block, out, send, recv
        self.pieces = pieces
        self.steps = ring.count // 2

    def moves(self, step):
        last = step == self.steps - 1
        for piece in range(self.pieces):
            if not last or piece < self.pieces // 2:
                yield 0, piece
            if not last or piece >= self.pieces // 2:
                yield 1, piece

    def copy(self, step, way, piece):
        offset = -step if way == 0 else step
        owner = self.ring.index(offset)
        source = self.block.at[piece] if step == 0 else self.out(owner, piece)
        return remote(
            source,
            self.out(owner, piece),
            self.send.at[way, step, piece],
            self.recv.at[way, step, piece],
            self.ring.right if way == 0 else self.ring.left,
        )

    def start(self, only=None):
        for way, piece in self.moves(0):
            if only is None or piece == only:
                self.copy(0, way, piece).start()

    def advance(self, step, landed=None):
        ahead = list(self.moves(step + 1)) if step + 1 < self.steps else []
        for way, piece in self.moves(step):
            self.copy(step, way, piece).wait_recv()
            if (way, piece) in ahead:
                self.copy(step + 1, way, piece).start()
            if landed is not None:
                landed(self.ring.index(-(step + 1) if way == 0 else step + 1), piece, way, step)

    def finish(self):
        for step in range(self.steps):
            for way, piece in self.moves(step):
                self.copy(step, way, piece).wait_send()


def ring_sems(count, pieces):
    return [pltpu.SemaphoreType.DMA((2, count // 2, pieces))] * 2


class FrameGather:
    def __init__(self, count, block, out, sends, recvs, pieces):
        self.block, self.out, self.pieces = block, out, pieces
        self.sends, self.recvs = sends, recvs
        self.chips = count // 2
        me = lax.axis_index("frame")
        self.me, self.chip, self.core = me, lax.div(me, 2), lax.rem(me, 2)
        self.twin = {"frame": self.chip * 2 + 1 - self.core}

    def peer(self, distance):
        return lax.rem(self.chip + distance + self.chips, self.chips) * 2 + self.core

    def partners(self):
        return [self.twin] + [{"frame": self.peer(d)} for d in range(1, self.chips)]

    def across(self, distance, piece):
        return remote(
            self.block.at[piece],
            self.out.at[self.me, piece],
            self.sends.at[0, distance, piece],
            self.recvs.at[0, distance, piece],
            {"frame": self.peer(distance)},
        )

    def inside(self, distance, piece):
        slot = self.peer(-distance)
        return remote(
            self.block.at[piece] if distance == 0 else self.out.at[slot, piece],
            self.out.at[slot, piece],
            self.sends.at[1, distance, piece],
            self.recvs.at[1, distance, piece],
            self.twin,
        )

    def start(self):
        for piece in range(self.pieces):
            for d in range(1, self.chips):
                self.across(d, piece).start()
        for piece in range(self.pieces):
            self.inside(0, piece).start()

    def relay(self, piece):
        for d in range(1, self.chips):
            self.across(d, piece).wait_recv()
            self.inside(d, piece).start()

    def settle(self, piece):
        for d in range(self.chips):
            self.inside(d, piece).wait_recv()

    def finish(self):
        for piece in range(self.pieces):
            for d in range(self.chips):
                self.inside(d, piece).wait_send()
                if d:
                    self.across(d, piece).wait_send()


def frame_sems(count, pieces):
    return [pltpu.SemaphoreType.DMA((2, count // 2, pieces))] * 2


def comm_params(collective):
    return pltpu.CompilerParams(
        collective_id=collective, has_side_effects=True, vmem_limit_bytes=vmem_limit
    )


def encode_kernel(
    seq_count, frame_count, patches, gain, weight, ids, out_weight, text, text_gain, merge_gain, up,
    hidden, text_out, text_near, *scratch
):
    (mine, query, held, flat, peak, mass, blend, context, weight_out, gathered, up_held, total, spread,
     fsend, frecv, rsend, rrecv, tsend, trecv, csend, crecv, xsend, xrecv, own) = scratch
    load_up = pltpu.make_async_copy(up, up_held, own.at[2])
    load_up.start()
    ring = Ring(seq_count)
    heads, tall, rows = mine.shape
    frames = FrameGather(frame_count, mine, held, fsend, frecv, heads)
    core, twin = frames.core, frames.twin
    pieces = out_weight.shape[1]
    gather = RingGather(
        ring, out_weight.at[core], lambda i, piece: weight_out.at[i, core, piece], rsend, rrecv, pieces
    )
    contexts = RingGather(ring, context, lambda i, piece: gathered.at[i, piece], csend, crecv, heads)
    parts = text_near.shape[1]
    words = FrameGather(frame_count, text_out, text_near, xsend, xrecv, parts)
    greet([ring.left, ring.right] + frames.partners())
    gather.start()
    keep = pltpu.make_async_copy(out_weight, weight_out.at[ring.index(0)], own.at[0])
    keep.start()
    handed = []

    def landed(index, piece, way, step):
        spot = weight_out.at[index, core, piece]
        copy = remote(spot, spot, tsend.at[way, step, piece], trecv.at[way, step, piece], twin)
        copy.start()
        handed.append(copy)

    widened = patches[...].astype(jnp.float32)
    factor = lax.rsqrt(jnp.mean(widened * widened, axis=-1, keepdims=True) + epsilon)
    normed = (widened * factor * gain[...].reshape(1, -1)).astype(jnp.bfloat16)
    projected = lax.dot_general(
        weight[...], normed, (((1,), (1,)), ((), ())), preferred_element_type=jnp.float32
    ).astype(jnp.bfloat16)
    for head in range(heads):
        base = head * 3 * VIT_HDIM
        query[head] = projected[base : base + VIT_HDIM]
        mine[head] = projected[base + VIT_HDIM : base + 3 * VIT_HDIM]
    frames.start()
    local = pltpu.make_async_copy(mine, held.at[frames.me], own.at[1])
    local.start()
    per_token = frame_count * rows // ids.shape[1]
    ends = [
        per_token * jnp.sum((ids[...] <= video).astype(jnp.int32), axis=1, keepdims=True)
        for video in range(VIDEOS - 1)
    ]
    local.wait()
    near = [frames.chip * 2, frames.chip * 2 + 1]
    far = [
        lax.rem(frames.chip + d, frames.chips) * 2 + c for d in range(1, frames.chips) for c in range(2)
    ]
    tile = math.gcd(rows, 256)
    scale = VIT_HDIM ** (-0.5) * math.log2(math.e)

    def flatten(slots, head):
        for slot in slots:
            flat[slot, head] = held[slot, head, :VIT_HDIM, :].T

    def attend(slots, head, start):
        columns = pl.ds(start, tile)
        queries = query[head, :, columns]
        places = frames.me * rows + start + lax.broadcasted_iota(jnp.int32, (1, tile), 1)
        first = jnp.zeros((1, tile), jnp.int32)
        past = jnp.full((1, tile), frame_count * rows, jnp.int32)
        for end in ends:
            first = jnp.where(places >= end, end, first)
        for end in reversed(ends):
            past = jnp.where(places < end, end, past)
        scores = []
        for slot in slots:
            part = jnp.dot(flat[slot, head], queries, preferred_element_type=jnp.float32)
            spot = slot * rows + lax.broadcasted_iota(jnp.int32, part.shape, 0)
            scores.append(jnp.where((spot >= first) & (spot < past), part, lowest))
        scores = jnp.concatenate(scores, axis=0)
        highest = jnp.max(scores, axis=0, keepdims=True)
        weights = jnp.exp2((scores - highest) * scale)
        total = jnp.sum(weights, axis=0, keepdims=True)
        weights = weights.astype(jnp.bfloat16)
        mixed = sum(
            jnp.dot(
                held[slot, head, VIT_HDIM:, :],
                weights[i * rows : (i + 1) * rows],
                preferred_element_type=jnp.float32,
            )
            for i, slot in enumerate(slots)
        )
        return highest, total, mixed

    def first_pass(head):
        flatten(near, head)

        def one(index, carry):
            start = pl.multiple_of(index * tile, tile)
            columns = pl.ds(start, tile)
            highest, total, mixed = attend(near, head, start)
            peak[head : head + 1, columns] = highest
            mass[head : head + 1, columns] = total
            blend[head, :, columns] = mixed
            return carry

        lax.fori_loop(0, rows // tile, one, 0)

    def norm_text(index):
        line = text[index].astype(jnp.float32)
        level = lax.rsqrt(jnp.mean(line * line, axis=-1, keepdims=True) + epsilon)
        text_out[index] = (line * level * text_gain[...].reshape(1, -1)).astype(text_out.dtype)

    def second_pass(head):
        if far:
            flatten(far, head)

        def one(index, carry):
            start = pl.multiple_of(index * tile, tile)
            columns = pl.ds(start, tile)
            total, mixed = mass[head : head + 1, columns], blend[head, :, columns]
            if far:
                before = peak[head : head + 1, columns]
                highest, more, extra = attend(far, head, start)
                joint = jnp.maximum(before, highest)
                old, new = jnp.exp2((before - joint) * scale), jnp.exp2((highest - joint) * scale)
                total = total * old + more * new
                mixed = mixed * old + extra * new
            context[head, :, columns] = (mixed / total).astype(context.dtype)
            return carry

        lax.fori_loop(0, rows // tile, one, 0)

    gather.advance(0, landed)
    for head in range(heads):
        frames.inside(0, head).wait_recv()
        first_pass(head)
    for head in range(heads):
        frames.relay(head)
        if head + 1 < gather.steps:
            gather.advance(head + 1, landed)
        for index in range(head, text.shape[0], heads):
            norm_text(index)
        if head == heads - 1:
            words.start()
            aside = pltpu.make_async_copy(
                text_out.at[pl.ds(0, parts)], text_near.at[frames.me], own.at[3]
            )
            aside.start()
        for d in range(1, frames.chips):
            frames.inside(d, head).wait_recv()
        second_pass(head)
        contexts.start(head)
    for step in range(heads + 1, gather.steps):
        gather.advance(step, landed)
    own_context = pltpu.make_async_copy(context, gathered.at[ring.index(0)], own.at[1])
    own_context.start()
    keep.wait()
    frames.finish()
    gather.finish()
    for copy in handed:
        copy.wait()
    own_context.wait()
    share = heads * VIT_HDIM

    def fold(offsets, first):
        owners = [ring.index(offset) for offset in offsets]
        left = jnp.concatenate([gathered[i].reshape(share, rows) for i in owners], axis=0)
        right = jnp.concatenate([weight_out[i].reshape(share, -1) for i in owners], axis=0)
        product = lax.dot_general(
            left, right, (((0,), (0,)), ((), ())), preferred_element_type=jnp.float32
        )
        if first:
            total[...] = patches[...].astype(jnp.float32) + product
        else:
            total[...] += product

    half = max(contexts.steps // 2, 1)
    early = min(parts, contexts.steps - 1)
    for step in range(contexts.steps):
        contexts.advance(step)
        if step == half - 1:
            fold(range(-half, half + 1), True)
        if step < early:
            words.relay(step)
    if contexts.steps > half:
        rest = list(range(half + 1, contexts.steps)) + list(range(-contexts.steps, -half))
        fold(rest, False)
    width = total.shape[1]
    values = total[...]
    factor = lax.rsqrt(jnp.mean(values * values, axis=1, keepdims=True) + epsilon)
    values = values * factor * merge_gain[...].reshape(1, -1)
    lanes = spread.shape[2]
    for c in range(width // lanes):
        spread[c] = values[:, c * lanes : (c + 1) * lanes]
    for part in range(early, parts):
        words.relay(part)
    load_up.wait()
    result = sum(
        jnp.dot(
            jnp.concatenate(
                [spread[c, pl.ds(r, rows // 4, stride=4), :] for c in range(width // lanes)], axis=1
            ).astype(jnp.bfloat16),
            up_held[r * width : (r + 1) * width, :],
            preferred_element_type=jnp.float32,
        )
        for r in range(4)
    )
    hidden[...] = (0.5 * result * (1.0 + lax.erf(result * 0.5**0.5))).astype(hidden.dtype)
    aside.wait()
    for part in range(parts):
        words.settle(part)
    words.finish()
    contexts.finish()


def encode(
    patches, gain, weight, ids, out_weight, text, text_gain, merge_gain, up, seq_count, frame_count, collective
):
    rows, width = patches.shape
    heads = weight.shape[1] // (3 * VIT_HDIM)
    half = out_weight.shape[0] // 2
    tall = math.gcd(half, 16)
    pieces = half // tall
    out_weight = out_weight.reshape(2, pieces, tall, -1)
    text = text.reshape(-1, 16, text.shape[1])
    parts = text.shape[0] // 2
    own = (heads, VIT_HDIM, rows)
    return pl.pallas_call(
        functools.partial(encode_kernel, seq_count, frame_count),
        in_specs=[VMEM] * 8 + [ANY],
        out_specs=[VMEM, VMEM, ANY],
        out_shape=[
            jax.ShapeDtypeStruct((rows // 4, up.shape[1]), jnp.bfloat16),
            jax.ShapeDtypeStruct(text.shape, text.dtype),
            jax.ShapeDtypeStruct((frame_count, parts) + text.shape[1:], text.dtype),
        ],
        scratch_shapes=[
            pltpu.VMEM((heads, 2 * VIT_HDIM, rows), jnp.bfloat16),
            pltpu.VMEM(own, jnp.bfloat16),
            pltpu.VMEM((frame_count, heads, 2 * VIT_HDIM, rows), jnp.bfloat16),
            pltpu.VMEM((frame_count, heads, rows, VIT_HDIM), jnp.bfloat16),
            pltpu.VMEM((heads, rows), jnp.float32),
            pltpu.VMEM((heads, rows), jnp.float32),
            pltpu.VMEM(own, jnp.float32),
            pltpu.VMEM(own, jnp.bfloat16),
            pltpu.VMEM((seq_count,) + out_weight.shape, out_weight.dtype),
            pltpu.VMEM((seq_count,) + own, jnp.bfloat16),
            pltpu.VMEM(up.shape, up.dtype),
            pltpu.VMEM((rows, width), jnp.float32),
            pltpu.VMEM((width // 128, rows, 128), jnp.float32),
        ]
        + frame_sems(frame_count, heads)
        + ring_sems(seq_count, pieces) * 2
        + ring_sems(seq_count, heads)
        + frame_sems(frame_count, parts)
        + [pltpu.SemaphoreType.DMA((4,))],
        compiler_params=comm_params(collective),
    )(patches, gain, weight.T, ids[None, :], out_weight, text, text_gain, merge_gain, up)


def finish_kernel(
    seq_count, frame_count, tokens, text, query, covered, spots, qw, kw, cosine, sine_part, result, *scratch
):
    (held, q_held, k_held, mine, pair, vision, peak, mass, blend, select, locate,
     load, fsend, frecv, tsend, trecv, vsend, vrecv, own) = scratch
    parts, share, span = tokens.shape
    loads = []
    for part in range(parts):
        slab = pl.ds(part * span, span)
        loads.append(pltpu.make_async_copy(qw.at[slab], q_held.at[slab], load.at[0, part]))
        loads.append(pltpu.make_async_copy(kw.at[slab], k_held.at[slab], load.at[1, part]))
    for copy in loads:
        copy.start()
    ring = Ring(seq_count)
    here = ring.index(0)
    frames = FrameGather(frame_count, tokens, held, fsend, frecv, parts)
    texts = RingGather(ring, text, lambda i, piece: pair.at[i, piece], tsend, trecv, text.shape[0])
    visions = RingGather(ring, mine, lambda i, piece: vision.at[i, piece], vsend, vrecv, mine.shape[0])
    greet([ring.left, ring.right] + frames.partners())
    frames.start()
    texts.start()
    keep = [
        pltpu.make_async_copy(tokens, held.at[frames.me], own.at[0]),
        pltpu.make_async_copy(text, pair.at[here], own.at[1]),
    ]
    for copy in keep:
        copy.start()
    rows, queries = query.shape
    heads = queries // HDIM
    couple = 2 if heads % 2 == 0 else 1
    scale = HDIM ** (-0.5) * math.log2(math.e)
    total = spots.shape[1]
    slots = locate.shape[0]

    inside = (spots[...] >= here * rows) & (spots[...] < (here + 1) * rows)
    ahead = lax.broadcasted_iota(jnp.int32, (total, total), 0) < lax.broadcasted_iota(
        jnp.int32, (total, total), 1
    )
    flags = jnp.where(inside, 1.0, 0.0)
    rank = jnp.dot(
        jnp.broadcast_to(flags, (8, total)).astype(jnp.bfloat16),
        jnp.where(ahead, 1.0, 0.0).astype(jnp.bfloat16),
        preferred_element_type=jnp.float32,
    )[:1]
    slot = lax.broadcasted_iota(jnp.int32, (slots, total), 0).astype(jnp.float32)
    chosen = jnp.where(inside & (slot == rank), 1.0, 0.0)
    select[...] = chosen.astype(select.dtype)
    locate[...] = jnp.sum(chosen * (spots[...] + 1 - here * rows).astype(jnp.float32), axis=1, keepdims=True) - 1.0

    def keys_of(block):
        return pair[block].reshape(rows, 2 * HDIM)

    def weigh(scores, highest):
        weights = jnp.exp2((scores - highest) * scale)
        return weights.astype(jnp.bfloat16), jnp.sum(weights, axis=1, keepdims=True)

    def score(left, right):
        return lax.dot_general(left, right, (((1,), (1,)), ((), ())), preferred_element_type=jnp.float32)

    strip = math.gcd(rows, 256)

    def fold(head, lines, scores, values):
        before = peak[head, lines]
        highest = jnp.maximum(before, jnp.max(scores, axis=1, keepdims=True))
        weights, more = weigh(scores, highest)
        shrink = jnp.exp2((before - highest) * scale)
        peak[head, lines] = highest
        mass[head, lines] = mass[head, lines] * shrink + more
        blend[head, lines] = blend[head, lines] * shrink + jnp.dot(
            weights, values, preferred_element_type=jnp.float32
        )

    def query_of(group, j):
        return query[:, pl.ds(pl.multiple_of((group * couple + j) * HDIM, HDIM), HDIM)]

    groups = heads // couple

    def diagonal(group):
        block = text[...].reshape(rows, 2 * HDIM)
        lower = lax.broadcasted_iota(jnp.int32, (rows, rows), 0) >= lax.broadcasted_iota(
            jnp.int32, (rows, rows), 1
        )
        several = [group * couple + j for j in range(couple)]
        scores = [score(query_of(group, j), block[:, :HDIM]) + covered[here, :1, :] for j in range(couple)]
        scores = [jnp.where(lower, part, lowest) for part in scores]
        tops = [jnp.max(part, axis=1, keepdims=True) for part in scores]
        weighed = [weigh(part, top) for part, top in zip(scores, tops)]
        products = [
            jnp.dot(weights, block[:, HDIM:], preferred_element_type=jnp.float32) for weights, _ in weighed
        ]
        for head, top, (_, more), product in zip(several, tops, weighed, products):
            peak[head] = top
            mass[head] = more
            blend[head] = product

    def earlier(group, owner):
        block = keys_of(owner)
        keys, values, bias = block[:, :HDIM], block[:, HDIM:], covered[owner, :1, :]
        for j in range(couple):
            queries_now = query_of(group, j)
            for line in range(0, rows, strip):
                lines = slice(line, line + strip)
                fold(group * couple + j, lines, score(queries_now[lines], keys) + bias, values)

    def vision_rows():
        for part in range(parts):
            frames.settle(part)
        frames.finish()
        for copy in keep:
            copy.wait()
        for copy in loads:
            copy.wait()
        q_total, k_total = None, None
        for part in range(parts):
            lines = jnp.concatenate([held[f, part] for f in range(frame_count)], axis=0)
            slab = slice(part * span, (part + 1) * span)
            q_part = jnp.dot(lines, q_held[slab], preferred_element_type=jnp.float32)
            k_part = jnp.dot(lines, k_held[slab], preferred_element_type=jnp.float32)
            q_total = q_part if part == 0 else q_total + q_part
            k_total = k_part if part == 0 else k_total + k_part
        turn, slide = cosine[...], sine_part[...]

        def turned(values):
            return values * turn + pltpu.roll(values, HDIM // 2, 1) * slide

        columns = [turned(q_total[:, c : c + HDIM]) for c in range(0, queries, HDIM)]
        columns += [turned(k_total[:, :HDIM]), k_total[:, HDIM:]]
        pieces, tall = mine.shape[:2]
        for i, values in enumerate(columns):
            for piece in range(pieces):
                mine[piece, :, i * HDIM : (i + 1) * HDIM] = values[
                    piece * tall : (piece + 1) * tall
                ].astype(mine.dtype)
        visions.start()
        pltpu.make_async_copy(mine, vision.at[here], own.at[2]).start()

    units = groups * seq_count
    events = {}

    def at(unit, action):
        events.setdefault(min(unit, units - 1), []).append(action)

    for part in range(parts):
        at([0, 1, 2, 3][part] if part < 4 else 3, functools.partial(frames.relay, part))
    stride = 2 * groups
    for step in range(texts.steps):
        at(groups - 1 + stride * step, functools.partial(texts.advance, step))
    at(groups + 2, vision_rows)
    for step in range(visions.steps):
        at(groups + 4 + 2 * step, functools.partial(visions.advance, step))

    def body(unit, carry):
        turn_of, group = lax.div(unit, groups), lax.rem(unit, groups)
        far, odd = lax.div(turn_of + 1, 2), lax.rem(turn_of, 2)
        owner = ring_index(
            lax.rem(ring.here + far * (1 - 2 * odd) + 2 * seq_count, seq_count), seq_count
        )

        @pl.when(turn_of == 0)
        def _():
            diagonal(group)

        @pl.when((turn_of > 0) & (owner < here))
        def _():
            earlier(group, owner)

        for index, actions in sorted(events.items()):

            def act(actions=actions):
                for action in actions:
                    action()

            pl.when(unit == index)(act)
        return carry

    lax.fori_loop(0, units, body, 0)
    pltpu.make_async_copy(mine, vision.at[here], own.at[2]).wait()

    both = vision[...].reshape(total, queries + 2 * HDIM)
    vision_keys, vision_values = both[:, queries : queries + HDIM], both[:, queries + HDIM :]
    places = here * rows + lax.broadcasted_iota(jnp.int32, (rows, 1), 0)
    for head in range(heads):
        for line in range(0, rows, strip):
            lines = slice(line, line + strip)
            scores = score(query[lines, head * HDIM : (head + 1) * HDIM], vision_keys)
            fold(head, lines, jnp.where(spots[...] <= places[lines], scores, lowest), vision_values)

    picked = jnp.dot(select[...], both[:, :queries], preferred_element_type=jnp.float32).astype(jnp.bfloat16)
    stacked = jnp.concatenate([picked[:, c : c + HDIM] for c in range(0, queries, HDIM)], axis=0)
    spot = jnp.concatenate([locate[...]] * heads, axis=0)

    def add(state, scores, values):
        before, amount, mixed = state
        highest = jnp.maximum(before, jnp.max(scores, axis=1, keepdims=True))
        weights, more = weigh(scores, highest)
        shrink = jnp.exp2((before - highest) * scale)
        mixed = mixed * shrink + jnp.dot(weights, values, preferred_element_type=jnp.float32)
        return highest, amount * shrink + more, mixed

    tall = stacked.shape[0]
    state = (
        jnp.full((tall, 1), lowest, jnp.float32),
        jnp.zeros((tall, 1), jnp.float32),
        jnp.zeros((tall, HDIM), jnp.float32),
    )
    seen = (spots[...] - here * rows).astype(jnp.float32)
    state = add(state, jnp.where(seen <= spot, score(stacked, vision_keys), lowest), vision_values)
    block = text[...].reshape(rows, 2 * HDIM)
    column = lax.broadcasted_iota(jnp.int32, (1, rows), 1).astype(jnp.float32)
    scores = score(stacked, block[:, :HDIM]) + covered[here, :1, :]
    state = add(state, jnp.where(column <= spot, scores, lowest), block[:, HDIM:])

    def past(owner, now):
        block = keys_of(owner)
        return add(now, score(stacked, block[:, :HDIM]) + covered[owner, :1, :], block[:, HDIM:])

    _, amount, mixed = lax.fori_loop(0, here, past, state)
    mixed = (mixed / amount).astype(jnp.bfloat16)
    picked = jnp.concatenate([mixed[h * slots : (h + 1) * slots] for h in range(heads)], axis=1)
    column = lax.broadcasted_iota(jnp.int32, (slots, rows), 1).astype(jnp.float32)
    spread = jnp.where(column == locate[...], 1.0, 0.0).astype(jnp.bfloat16)
    back = (((0,), (0,)), ((), ()))
    moved = lax.dot_general(spread, picked, back, preferred_element_type=jnp.float32)
    taken = lax.dot_general(
        spread, jnp.ones((slots, HDIM), jnp.bfloat16), back, preferred_element_type=jnp.float32
    )
    for head in range(heads):
        columns = slice(head * HDIM, (head + 1) * HDIM)
        kept = blend[head] / mass[head]
        result[:, columns] = jnp.where(taken > 0.5, moved[:, columns], kept).astype(result.dtype)
    texts.finish()
    visions.finish()


def finish(tokens, text, query, covered, spots, tables, query_weight, keyvalue_weight, seq_count, frame_count, collective):
    parts, share, span = tokens.shape
    lines = frame_count * share
    rows, queries = query.shape
    heads = queries // HDIM
    width = queries + keyvalue_weight.shape[1]
    slots = frame_count * -(-3 * share // 2)
    text = text.reshape(2, -1, text.shape[1])
    mine = (2, lines // 2, width)
    cosine, sine_part = tables
    return pl.pallas_call(
        functools.partial(finish_kernel, seq_count, frame_count),
        in_specs=[VMEM] * 5 + [ANY] * 2 + [VMEM] * 2,
        out_specs=VMEM,
        out_shape=jax.ShapeDtypeStruct((rows, queries), jnp.bfloat16),
        scratch_shapes=[
            pltpu.VMEM((frame_count,) + tokens.shape, tokens.dtype),
            pltpu.VMEM(query_weight.shape, query_weight.dtype),
            pltpu.VMEM(keyvalue_weight.shape, keyvalue_weight.dtype),
            pltpu.VMEM(mine, text.dtype),
            pltpu.VMEM((seq_count,) + text.shape, text.dtype),
            pltpu.VMEM((seq_count,) + mine, text.dtype),
            pltpu.VMEM((heads, rows, 1), jnp.float32),
            pltpu.VMEM((heads, rows, 1), jnp.float32),
            pltpu.VMEM((heads, rows, HDIM), jnp.float32),
            pltpu.VMEM((slots, seq_count * lines), jnp.bfloat16),
            pltpu.VMEM((slots, 1), jnp.float32),
            pltpu.SemaphoreType.DMA((2, parts)),
        ]
        + frame_sems(frame_count, parts)
        + ring_sems(seq_count, 2) * 2
        + [pltpu.SemaphoreType.DMA((3,))],
        compiler_params=comm_params(collective),
    )(tokens, text, query, covered, spots, query_weight, keyvalue_weight, cosine, sine_part)


def scatter_kernel(
    count, frame_count, hidden, weight, gain, text, near, qw, kw, cosine, sine_part, spots,
    out, q_out, pair_out, covered, *scratch
):
    held, part, stage, land, q_held, k_held, early, late, sums, load, send, recv, fsend, frecv, own = scratch
    ring = Ring(count)
    width = weight.shape[1]
    pieces = held.shape[0]
    span = width // pieces
    share = out.shape[1]
    order = [piece for pair in zip(range(pieces // 2), range(pieces // 2, pieces)) for piece in pair]
    loads = {
        piece: pltpu.make_async_copy(
            weight.at[:, pl.ds(piece * span, span)], held.at[piece], load.at[piece]
        )
        for piece in order
    }
    for piece in order:
        loads[piece].start()
    extra = [
        pltpu.make_async_copy(near, early, own.at[0]),
        pltpu.make_async_copy(qw, q_held, own.at[1]),
        pltpu.make_async_copy(kw, k_held, own.at[2]),
    ]
    for copy in extra:
        copy.start()
    parts, tall, depth = early.shape[1:]
    last = text.at[pl.ds(text.shape[0] - late.shape[1], late.shape[1])]
    frames = FrameGather(frame_count, last, late, fsend, frecv, late.shape[1])
    greet([ring.left, ring.right] + frames.partners())
    frames.start()
    aside = pltpu.make_async_copy(last, late.at[frames.me], own.at[3])
    aside.start()
    forward = [piece < pieces // 2 for piece in range(pieces)]

    def hop(piece, step):
        return remote(
            stage.at[piece, step],
            land.at[piece, step],
            send.at[piece, step],
            recv.at[piece, step],
            ring.right if forward[piece] else ring.left,
        )

    for piece in order:
        loads[piece].wait()
        product = jnp.dot(hidden[...], held[piece], preferred_element_type=jnp.float32)
        for i in range(count):
            part[piece, i] = product[i * share : (i + 1) * share]
        first = ring.index(-1 if forward[piece] else 1)
        stage[piece, 0] = part[piece, first].astype(jnp.bfloat16)
        hop(piece, 0).start()
    for copy in extra:
        copy.wait()
    sums[...] = jnp.zeros_like(sums)
    slabs = 8
    slab = depth // slabs
    queries = qw.shape[1]

    def project(source, spot, index):
        columns = pl.ds(pl.multiple_of(index * slab, slab), slab)
        rows = source[:, :, :, columns].reshape(-1, slab)
        count_rows = rows.shape[0]
        sums[spot, :, :queries] += jnp.dot(rows, q_held[columns, :], preferred_element_type=jnp.float32)
        sums[spot, :, queries:] += jnp.dot(rows, k_held[columns, :], preferred_element_type=jnp.float32)

    def advance(step, group):
        for piece in group:
            hop(piece, step - 1).wait_recv()
            owner = ring.index(-1 - step if forward[piece] else 1 + step)
            total = land[piece, step - 1].astype(jnp.float32) + part[piece, owner]
            stage[piece, step] = total.astype(jnp.bfloat16)
            hop(piece, step).start()

    def cover(block):
        shape = (covered.shape[2], spots.shape[1])
        keys = block * shape[0] + lax.broadcasted_iota(jnp.int32, shape, 0)
        hits = (keys == spots[...]).astype(jnp.float32).astype(jnp.bfloat16)
        total = lax.dot_general(
            jnp.ones((covered.shape[1], shape[1]), jnp.bfloat16),
            hits,
            (((1,), (1,)), ((), ())),
            preferred_element_type=jnp.float32,
        )
        covered[block] = jnp.where(total > 0.5, lowest, 0.0)

    groups = [order[:2], order[2:]]
    turn_over = 1 + slabs // 2

    def opening(step, carry):
        for i, group in enumerate(groups):
            advance(step, group)
            project(early, 0, 2 * (step - 1) + i)
            for block in range(count // slabs):
                cover((2 * (step - 1) + i) * (count // slabs) + block)

        @pl.when(step <= late.shape[1])
        def _():
            frames.relay(step - 1)

        return carry

    lax.fori_loop(1, turn_over, opening, 0)
    aside.wait()
    for piece in range(late.shape[1]):
        frames.settle(piece)
    each = -(-slabs // (2 * (count - 1 - turn_over)))

    def closing(step, carry):
        for i, group in enumerate(groups):
            advance(step, group)
            unit = 2 * (step - turn_over) + i
            start = jnp.minimum(unit * each, slabs)
            stop = jnp.minimum(start + each, slabs)

            def fold(index, inner):
                project(late, 1, index)
                return inner

            lax.fori_loop(start, stop, fold, 0)
        return carry

    lax.fori_loop(turn_over, count - 1, closing, 0)
    block = 2 * parts * tall
    for f in range(frame_count):
        for spot in range(2):
            source = slice(f * parts * tall, (f + 1) * parts * tall)
            begin = f * block + spot * parts * tall
            target = slice(begin, begin + parts * tall)
            turn, slide = cosine[target], sine_part[target]
            for c in range(0, queries + HDIM, HDIM):
                values = sums[spot, source, c : c + HDIM]
                values = (values * turn + pltpu.roll(values, HDIM // 2, 1) * slide).astype(q_out.dtype)
                if c < queries:
                    q_out[target, c : c + HDIM] = values
                else:
                    pair_out[target, :HDIM] = values
            pair_out[target, HDIM:] = sums[spot, source, queries + HDIM :].astype(pair_out.dtype)
    here = ring.index(0)
    squares = jnp.zeros((share, 1), jnp.float32)
    for piece in order:
        hop(piece, count - 2).wait_recv()
        total = land[piece, count - 2].astype(jnp.float32) + part[piece, here]
        total = total.astype(jnp.bfloat16).astype(jnp.float32)
        part[piece, here] = total
        squares += jnp.sum(total * total, axis=1, keepdims=True)
    factor = lax.rsqrt(squares / width + epsilon)
    for piece in order:
        columns = slice(piece * span, (piece + 1) * span)
        out[piece] = (part[piece, here] * factor * gain[columns].reshape(1, -1)).astype(out.dtype)

    def drain(step, carry):
        for piece in order:
            hop(piece, step).wait_send()
        return carry

    lax.fori_loop(0, count - 1, drain, 0)
    frames.finish()


def scatter(hidden, weight, gain, text, near, query_weight, keyvalue_weight, tables, spots, count, frame_count, collective):
    rows, depth = hidden.shape
    width = weight.shape[1]
    share = rows // count
    pieces = 4
    span = width // pieces
    parts, tall = text.shape[:2]
    tokens = frame_count * parts * tall
    queries, pairs = query_weight.shape[1], keyvalue_weight.shape[1]
    left = parts - near.shape[1]
    cosine, sine_part = tables
    return pl.pallas_call(
        functools.partial(scatter_kernel, count, frame_count),
        in_specs=[VMEM, ANY, VMEM, VMEM, ANY, ANY, ANY, VMEM, VMEM, VMEM],
        out_specs=[VMEM, VMEM, VMEM, VMEM],
        out_shape=[
            jax.ShapeDtypeStruct((pieces, share, span), jnp.bfloat16),
            jax.ShapeDtypeStruct((tokens, queries), jnp.bfloat16),
            jax.ShapeDtypeStruct((tokens, pairs), jnp.bfloat16),
            jax.ShapeDtypeStruct((count, 8, tokens), jnp.float32),
        ],
        scratch_shapes=[
            pltpu.VMEM((pieces, depth, span), jnp.bfloat16),
            pltpu.VMEM((pieces, count, share, span), jnp.float32),
            pltpu.VMEM((pieces, count - 1, share, span), jnp.bfloat16),
            pltpu.VMEM((pieces, count - 1, share, span), jnp.bfloat16),
            pltpu.VMEM(query_weight.shape, query_weight.dtype),
            pltpu.VMEM(keyvalue_weight.shape, keyvalue_weight.dtype),
            pltpu.VMEM(near.shape, near.dtype),
            pltpu.VMEM((frame_count, left) + text.shape[1:], text.dtype),
            pltpu.VMEM((2, tokens // 2, queries + pairs), jnp.float32),
            pltpu.SemaphoreType.DMA((pieces,)),
            pltpu.SemaphoreType.DMA((pieces, count - 1)),
            pltpu.SemaphoreType.DMA((pieces, count - 1)),
        ]
        + frame_sems(frame_count, left)
        + [pltpu.SemaphoreType.DMA((4,))],
        compiler_params=pltpu.CompilerParams(
            collective_id=collective, has_side_effects=True, vmem_limit_bytes=63 * 1024 * 1024
        ),
    )(hidden, weight, gain, text, near, query_weight, keyvalue_weight, cosine, sine_part, spots)


def turns(positions):
    lanes = jnp.arange(HDIM, dtype=jnp.int32)
    inverse = rope_base ** (-2.0 * (lanes % (HDIM // 2)).astype(jnp.float32) / HDIM)
    angles = positions.astype(jnp.float32)[:, None] * inverse[None, :]
    return jnp.cos(angles), jnp.where(lanes < HDIM // 2, -1.0, 1.0) * jnp.sin(angles)


def local(
    patches,
    vit_gain,
    vision_qkv,
    vision_out,
    video_ids,
    merge_gain,
    merge_up,
    merge_down,
    vision_pos,
    text_embed,
    llm_gain,
    query_weight,
    keyvalue_weight,
):
    frame_index = lax.axis_index("frame")
    seq_index = lax.axis_index("seq")
    frame_count = lax.axis_size("frame")
    seq_count = lax.axis_size("seq")
    patch_rows = patches.shape[0]
    merge_hidden, text_own, text_near = encode(
        patches, vit_gain, vision_qkv, video_ids, vision_out, text_embed, llm_gain, merge_gain, merge_up,
        seq_count, frame_count, 1,
    )
    seq_block = text_embed.shape[0] * frame_count
    share = patch_rows // (4 * seq_count)
    token_pos = vision_pos.reshape(frame_count, seq_count, share).transpose(1, 0, 2)
    here = lax.dynamic_index_in_dim(token_pos, seq_index, 0, keepdims=False).reshape(-1)
    spots = token_pos.reshape(1, -1)
    vision_normed, text_query, text_pair, covered = scatter(
        merge_hidden, merge_down, llm_gain, text_own, text_near, query_weight, keyvalue_weight,
        turns(seq_index * seq_block + jnp.arange(seq_block, dtype=jnp.int32)), spots,
        seq_count, frame_count, 3,
    )
    return finish(
        vision_normed, text_pair, text_query, covered, spots, turns(here), query_weight, keyvalue_weight,
        seq_count, frame_count, 4,
    )


def solution(mesh):
    return jax.shard_map(
        local,
        mesh=mesh,
        in_specs=(
            P("frame", None),
            P(),
            P(None, "seq"),
            P("seq", None),
            P(),
            P(),
            P(None, "seq"),
            P("seq", None),
            P(),
            P(("seq", "frame"), None),
            P(),
            P(None, "frame"),
            P(None, "frame"),
        ),
        out_specs=P("seq", "frame"),
        check_vma=False,
    )
```

```python
import functools
import math

import jax
import jax.numpy as jnp
from jax import lax
from jax.experimental import pallas as pl
from jax.experimental.pallas import tpu as pltpu
from jax.sharding import PartitionSpec as P

VIT_HDIM = 80
VIDEOS = 3
HDIM = 128


epsilon = 1e-06
rope_base = 1000000.0
lowest = -1e30
vmem_limit = 56 * 1024 * 1024

MESH = pl.DeviceIdType.MESH
ANY = pl.BlockSpec(memory_space=pl.ANY)
VMEM = pl.BlockSpec(memory_space=pltpu.VMEM)


def ring_grid(count):
    narrow = 1 << ((count.bit_length() - 1) // 2)
    return count // narrow, narrow


def ring_position(index, count):
    tall, narrow = ring_grid(count)
    if narrow < 2 or tall % 2:
        return index
    row, column = lax.div(index, narrow), lax.rem(index, narrow)
    odd = lax.rem(row, 2)
    inner = lax.div(column + narrow - 1, narrow)
    along = (column - 1) * (1 - odd) + (narrow - 1 - column) * odd
    return (1 - inner) * (count - 1 - row) + inner * (row * (narrow - 1) + along)


def ring_index(position, count):
    tall, narrow = ring_grid(count)
    if narrow < 2 or tall % 2:
        return position
    back = lax.div(position, tall * (narrow - 1))
    row, along = lax.div(position, narrow - 1), lax.rem(position, narrow - 1)
    odd = lax.rem(row, 2)
    column = 1 + along * (1 - odd) + (narrow - 2 - along) * odd
    return (1 - back) * (row * narrow + column) + back * (count - 1 - position) * narrow


class Ring:
    def __init__(self, count):
        self.count = count
        self.here = ring_position(lax.axis_index("seq"), count)
        self.right = {"seq": self.index(1)}
        self.left = {"seq": self.index(-1)}

    def index(self, offset):
        return ring_index(lax.rem(self.here + (offset + 2 * self.count), self.count), self.count)


def greet(partners):
    barrier = pltpu.get_barrier_semaphore()
    for partner in partners:
        pl.semaphore_signal(barrier, inc=1, device_id=partner, device_id_type=MESH)
    pl.semaphore_wait(barrier, len(partners))


def remote(source, target, send, recv, partner):
    return pltpu.make_async_remote_copy(
        src_ref=source,
        dst_ref=target,
        send_sem=send,
        recv_sem=recv,
        device_id=partner,
        device_id_type=MESH,
    )


class RingGather:
    def __init__(self, ring, block, out, send, recv, pieces):
        self.ring, self.block, self.out, self.send, self.recv = ring, block, out, send, recv
        self.pieces = pieces
        self.steps = ring.count // 2

    def moves(self, step):
        last = step == self.steps - 1
        for piece in range(self.pieces):
            if not last or piece < self.pieces // 2:
                yield 0, piece
            if not last or piece >= self.pieces // 2:
                yield 1, piece

    def copy(self, step, way, piece):
        offset = -step if way == 0 else step
        owner = self.ring.index(offset)
        source = self.block.at[piece] if step == 0 else self.out(owner, piece)
        return remote(
            source,
            self.out(owner, piece),
            self.send.at[way, step, piece],
            self.recv.at[way, step, piece],
            self.ring.right if way == 0 else self.ring.left,
        )

    def start(self, only=None):
        for way, piece in self.moves(0):
            if only is None or piece == only:
                self.copy(0, way, piece).start()

    def advance(self, step, landed=None):
        ahead = list(self.moves(step + 1)) if step + 1 < self.steps else []
        for way, piece in self.moves(step):
            self.copy(step, way, piece).wait_recv()
            if (way, piece) in ahead:
                self.copy(step + 1, way, piece).start()
            if landed is not None:
                landed(self.ring.index(-(step + 1) if way == 0 else step + 1), piece, way, step)

    def finish(self):
        for step in range(self.steps):
            for way, piece in self.moves(step):
                self.copy(step, way, piece).wait_send()


def ring_sems(count, pieces):
    return [pltpu.SemaphoreType.DMA((2, count // 2, pieces))] * 2


class FrameGather:
    def __init__(self, count, block, out, sends, recvs, pieces):
        self.block, self.out, self.pieces = block, out, pieces
        self.sends, self.recvs = sends, recvs
        self.chips = count // 2
        me = lax.axis_index("frame")
        self.me, self.chip, self.core = me, lax.div(me, 2), lax.rem(me, 2)
        self.twin = {"frame": self.chip * 2 + 1 - self.core}

    def peer(self, distance):
        return lax.rem(self.chip + distance + self.chips, self.chips) * 2 + self.core

    def partners(self):
        return [self.twin] + [{"frame": self.peer(d)} for d in range(1, self.chips)]

    def across(self, distance, piece):
        return remote(
            self.block.at[piece],
            self.out.at[self.me, piece],
            self.sends.at[0, distance, piece],
            self.recvs.at[0, distance, piece],
            {"frame": self.peer(distance)},
        )

    def inside(self, distance, piece):
        slot = self.peer(-distance)
        return remote(
            self.block.at[piece] if distance == 0 else self.out.at[slot, piece],
            self.out.at[slot, piece],
            self.sends.at[1, distance, piece],
            self.recvs.at[1, distance, piece],
            self.twin,
        )

    def start(self):
        for piece in range(self.pieces):
            for d in range(1, self.chips):
                self.across(d, piece).start()
        for piece in range(self.pieces):
            self.inside(0, piece).start()

    def relay(self, piece):
        for d in range(1, self.chips):
            self.across(d, piece).wait_recv()
            self.inside(d, piece).start()

    def settle(self, piece):
        for d in range(self.chips):
            self.inside(d, piece).wait_recv()

    def finish(self):
        for piece in range(self.pieces):
            for d in range(self.chips):
                self.inside(d, piece).wait_send()
                if d:
                    self.across(d, piece).wait_send()


def frame_sems(count, pieces):
    return [pltpu.SemaphoreType.DMA((2, count // 2, pieces))] * 2


def comm_params(collective):
    return pltpu.CompilerParams(
        collective_id=collective, has_side_effects=True, vmem_limit_bytes=vmem_limit
    )


def encode_kernel(
    seq_count, frame_count, patches, gain, weight, ids, out_weight, text, text_gain, merge_gain, up,
    hidden, text_out, text_near, *scratch
):
    (mine, query, held, flat, peak, mass, blend, context, weight_out, gathered, up_held, total, spread,
     fsend, frecv, rsend, rrecv, tsend, trecv, csend, crecv, xsend, xrecv, own) = scratch
    load_up = pltpu.make_async_copy(up, up_held, own.at[2])
    load_up.start()
    ring = Ring(seq_count)
    heads, tall, rows = mine.shape
    frames = FrameGather(frame_count, mine, held, fsend, frecv, heads)
    core, twin = frames.core, frames.twin
    pieces = out_weight.shape[1]
    gather = RingGather(
        ring, out_weight.at[core], lambda i, piece: weight_out.at[i, core, piece], rsend, rrecv, pieces
    )
    contexts = RingGather(ring, context, lambda i, piece: gathered.at[i, piece], csend, crecv, heads)
    parts = text_near.shape[1]
    words = FrameGather(frame_count, text_out, text_near, xsend, xrecv, parts)
    greet([ring.left, ring.right] + frames.partners())
    gather.start()
    keep = pltpu.make_async_copy(out_weight, weight_out.at[ring.index(0)], own.at[0])
    keep.start()
    handed = []

    def landed(index, piece, way, step):
        spot = weight_out.at[index, core, piece]
        copy = remote(spot, spot, tsend.at[way, step, piece], trecv.at[way, step, piece], twin)
        copy.start()
        handed.append(copy)

    widened = patches[...].astype(jnp.float32)
    factor = lax.rsqrt(jnp.mean(widened * widened, axis=-1, keepdims=True) + epsilon)
    normed = (widened * factor * gain[...].reshape(1, -1)).astype(jnp.bfloat16)
    projected = lax.dot_general(
        weight[...], normed, (((1,), (1,)), ((), ())), preferred_element_type=jnp.float32
    ).astype(jnp.bfloat16)
    for head in range(heads):
        base = head * 3 * VIT_HDIM
        query[head] = projected[base : base + VIT_HDIM]
        mine[head] = projected[base + VIT_HDIM : base + 3 * VIT_HDIM]
    frames.start()
    local = pltpu.make_async_copy(mine, held.at[frames.me], own.at[1])
    local.start()
    per_token = frame_count * rows // ids.shape[1]
    ends = [
        per_token * jnp.sum((ids[...] <= video).astype(jnp.int32), axis=1, keepdims=True)
        for video in range(VIDEOS - 1)
    ]
    local.wait()
    near = [frames.chip * 2, frames.chip * 2 + 1]
    far = [
        lax.rem(frames.chip + d, frames.chips) * 2 + c for d in range(1, frames.chips) for c in range(2)
    ]
    tile = math.gcd(rows, 256)
    scale = VIT_HDIM ** (-0.5) * math.log2(math.e)

    def flatten(slots, head):
        for slot in slots:
            flat[slot, head] = held[slot, head, :VIT_HDIM, :].T

    def attend(slots, head, start):
        columns = pl.ds(start, tile)
        queries = query[head, :, columns]
        places = frames.me * rows + start + lax.broadcasted_iota(jnp.int32, (1, tile), 1)
        first = jnp.zeros((1, tile), jnp.int32)
        past = jnp.full((1, tile), frame_count * rows, jnp.int32)
        for end in ends:
            first = jnp.where(places >= end, end, first)
        for end in reversed(ends):
            past = jnp.where(places < end, end, past)
        scores = []
        for slot in slots:
            part = jnp.dot(flat[slot, head], queries, preferred_element_type=jnp.float32)
            spot = slot * rows + lax.broadcasted_iota(jnp.int32, part.shape, 0)
            scores.append(jnp.where((spot >= first) & (spot < past), part, lowest))
        scores = jnp.concatenate(scores, axis=0)
        highest = jnp.max(scores, axis=0, keepdims=True)
        weights = jnp.exp2((scores - highest) * scale)
        total = jnp.sum(weights, axis=0, keepdims=True)
        weights = weights.astype(jnp.bfloat16)
        mixed = sum(
            jnp.dot(
                held[slot, head, VIT_HDIM:, :],
                weights[i * rows : (i + 1) * rows],
                preferred_element_type=jnp.float32,
            )
            for i, slot in enumerate(slots)
        )
        return highest, total, mixed

    def first_pass(head):
        flatten(near, head)

        def one(index, carry):
            start = pl.multiple_of(index * tile, tile)
            columns = pl.ds(start, tile)
            highest, total, mixed = attend(near, head, start)
            peak[head : head + 1, columns] = highest
            mass[head : head + 1, columns] = total
            blend[head, :, columns] = mixed
            return carry

        lax.fori_loop(0, rows // tile, one, 0)

    def norm_text(index):
        line = text[index].astype(jnp.float32)
        level = lax.rsqrt(jnp.mean(line * line, axis=-1, keepdims=True) + epsilon)
        text_out[index] = (line * level * text_gain[...].reshape(1, -1)).astype(text_out.dtype)

    def second_pass(head):
        if far:
            flatten(far, head)

        def one(index, carry):
            start = pl.multiple_of(index * tile, tile)
            columns = pl.ds(start, tile)
            total, mixed = mass[head : head + 1, columns], blend[head, :, columns]
            if far:
                before = peak[head : head + 1, columns]
                highest, more, extra = attend(far, head, start)
                joint = jnp.maximum(before, highest)
                old, new = jnp.exp2((before - joint) * scale), jnp.exp2((highest - joint) * scale)
                total = total * old + more * new
                mixed = mixed * old + extra * new
            context[head, :, columns] = (mixed / total).astype(context.dtype)
            return carry

        lax.fori_loop(0, rows // tile, one, 0)

    gather.advance(0, landed)
    for head in range(heads):
        frames.inside(0, head).wait_recv()
        first_pass(head)
    for head in range(heads):
        frames.relay(head)
        if head + 1 < gather.steps:
            gather.advance(head + 1, landed)
        for index in range(head, text.shape[0], heads):
            norm_text(index)
        if head == heads - 1:
            words.start()
            aside = pltpu.make_async_copy(
                text_out.at[pl.ds(0, parts)], text_near.at[frames.me], own.at[3]
            )
            aside.start()
        for d in range(1, frames.chips):
            frames.inside(d, head).wait_recv()
        second_pass(head)
        contexts.start(head)
    for step in range(heads + 1, gather.steps):
        gather.advance(step, landed)
    own_context = pltpu.make_async_copy(context, gathered.at[ring.index(0)], own.at[1])
    own_context.start()
    keep.wait()
    frames.finish()
    gather.finish()
    for copy in handed:
        copy.wait()
    own_context.wait()
    share = heads * VIT_HDIM

    def fold(offsets, first):
        owners = [ring.index(offset) for offset in offsets]
        left = jnp.concatenate([gathered[i].reshape(share, rows) for i in owners], axis=0)
        right = jnp.concatenate([weight_out[i].reshape(share, -1) for i in owners], axis=0)
        product = lax.dot_general(
            left, right, (((0,), (0,)), ((), ())), preferred_element_type=jnp.float32
        )
        if first:
            total[...] = patches[...].astype(jnp.float32) + product
        else:
            total[...] += product

    half = max(contexts.steps // 2, 1)
    early = min(parts, contexts.steps - 1)
    for step in range(contexts.steps):
        contexts.advance(step)
        if step == half - 1:
            fold(range(-half, half + 1), True)
        if step < early:
            words.relay(step)
    if contexts.steps > half:
        rest = list(range(half + 1, contexts.steps)) + list(range(-contexts.steps, -half))
        fold(rest, False)
    width = total.shape[1]
    values = total[...]
    factor = lax.rsqrt(jnp.mean(values * values, axis=1, keepdims=True) + epsilon)
    values = values * factor * merge_gain[...].reshape(1, -1)
    lanes = spread.shape[2]
    for c in range(width // lanes):
        spread[c] = values[:, c * lanes : (c + 1) * lanes]
    for part in range(early, parts):
        words.relay(part)
    load_up.wait()
    result = sum(
        jnp.dot(
            jnp.concatenate(
                [spread[c, pl.ds(r, rows // 4, stride=4), :] for c in range(width // lanes)], axis=1
            ).astype(jnp.bfloat16),
            up_held[r * width : (r + 1) * width, :],
            preferred_element_type=jnp.float32,
        )
        for r in range(4)
    )
    hidden[...] = (0.5 * result * (1.0 + lax.erf(result * 0.5**0.5))).astype(hidden.dtype)
    aside.wait()
    for part in range(parts):
        words.settle(part)
    words.finish()
    contexts.finish()


def encode(
    patches, gain, weight, ids, out_weight, text, text_gain, merge_gain, up, seq_count, frame_count, collective
):
    rows, width = patches.shape
    heads = weight.shape[1] // (3 * VIT_HDIM)
    half = out_weight.shape[0] // 2
    tall = math.gcd(half, 16)
    pieces = half // tall
    out_weight = out_weight.reshape(2, pieces, tall, -1)
    text = text.reshape(-1, 16, text.shape[1])
    parts = text.shape[0] // 2
    own = (heads, VIT_HDIM, rows)
    return pl.pallas_call(
        functools.partial(encode_kernel, seq_count, frame_count),
        in_specs=[VMEM] * 8 + [ANY],
        out_specs=[VMEM, VMEM, ANY],
        out_shape=[
            jax.ShapeDtypeStruct((rows // 4, up.shape[1]), jnp.bfloat16),
            jax.ShapeDtypeStruct(text.shape, text.dtype),
            jax.ShapeDtypeStruct((frame_count, parts) + text.shape[1:], text.dtype),
        ],
        scratch_shapes=[
            pltpu.VMEM((heads, 2 * VIT_HDIM, rows), jnp.bfloat16),
            pltpu.VMEM(own, jnp.bfloat16),
            pltpu.VMEM((frame_count, heads, 2 * VIT_HDIM, rows), jnp.bfloat16),
            pltpu.VMEM((frame_count, heads, rows, VIT_HDIM), jnp.bfloat16),
            pltpu.VMEM((heads, rows), jnp.float32),
            pltpu.VMEM((heads, rows), jnp.float32),
            pltpu.VMEM(own, jnp.float32),
            pltpu.VMEM(own, jnp.bfloat16),
            pltpu.VMEM((seq_count,) + out_weight.shape, out_weight.dtype),
            pltpu.VMEM((seq_count,) + own, jnp.bfloat16),
            pltpu.VMEM(up.shape, up.dtype),
            pltpu.VMEM((rows, width), jnp.float32),
            pltpu.VMEM((width // 128, rows, 128), jnp.float32),
        ]
        + frame_sems(frame_count, heads)
        + ring_sems(seq_count, pieces) * 2
        + ring_sems(seq_count, heads)
        + frame_sems(frame_count, parts)
        + [pltpu.SemaphoreType.DMA((4,))],
        compiler_params=comm_params(collective),
    )(patches, gain, weight.T, ids[None, :], out_weight, text, text_gain, merge_gain, up)


def finish_kernel(
    seq_count, frame_count, tokens, text, query, covered, spots, qw, kw, cosine, sine_part, result, *scratch
):
    (held, q_held, k_held, mine, pair, vision, peak, mass, blend, select, locate,
     load, fsend, frecv, tsend, trecv, vsend, vrecv, own) = scratch
    parts, share, span = tokens.shape
    loads = []
    for part in range(parts):
        slab = pl.ds(part * span, span)
        loads.append(pltpu.make_async_copy(qw.at[slab], q_held.at[slab], load.at[0, part]))
        loads.append(pltpu.make_async_copy(kw.at[slab], k_held.at[slab], load.at[1, part]))
    for copy in loads:
        copy.start()
    ring = Ring(seq_count)
    here = ring.index(0)
    frames = FrameGather(frame_count, tokens, held, fsend, frecv, parts)
    texts = RingGather(ring, text, lambda i, piece: pair.at[i, piece], tsend, trecv, text.shape[0])
    visions = RingGather(ring, mine, lambda i, piece: vision.at[i, piece], vsend, vrecv, mine.shape[0])
    greet([ring.left, ring.right] + frames.partners())
    frames.start()
    texts.start()
    keep = [
        pltpu.make_async_copy(tokens, held.at[frames.me], own.at[0]),
        pltpu.make_async_copy(text, pair.at[here], own.at[1]),
    ]
    for copy in keep:
        copy.start()
    rows, queries = query.shape
    heads = queries // HDIM
    couple = 2 if heads % 2 == 0 else 1
    scale = HDIM ** (-0.5) * math.log2(math.e)
    total = spots.shape[1]
    slots = locate.shape[0]

    inside = (spots[...] >= here * rows) & (spots[...] < (here + 1) * rows)
    ahead = lax.broadcasted_iota(jnp.int32, (total, total), 0) < lax.broadcasted_iota(
        jnp.int32, (total, total), 1
    )
    flags = jnp.where(inside, 1.0, 0.0)
    rank = jnp.dot(
        jnp.broadcast_to(flags, (8, total)).astype(jnp.bfloat16),
        jnp.where(ahead, 1.0, 0.0).astype(jnp.bfloat16),
        preferred_element_type=jnp.float32,
    )[:1]
    slot = lax.broadcasted_iota(jnp.int32, (slots, total), 0).astype(jnp.float32)
    chosen = jnp.where(inside & (slot == rank), 1.0, 0.0)
    select[...] = chosen.astype(select.dtype)
    locate[...] = jnp.sum(chosen * (spots[...] + 1 - here * rows).astype(jnp.float32), axis=1, keepdims=True) - 1.0

    def keys_of(block):
        return pair[block].reshape(rows, 2 * HDIM)

    def weigh(scores, highest):
        weights = jnp.exp2((scores - highest) * scale)
        return weights.astype(jnp.bfloat16), jnp.sum(weights, axis=1, keepdims=True)

    def score(left, right):
        return lax.dot_general(left, right, (((1,), (1,)), ((), ())), preferred_element_type=jnp.float32)

    strip = math.gcd(rows, 256)

    def fold(head, lines, scores, values):
        before = peak[head, lines]
        highest = jnp.maximum(before, jnp.max(scores, axis=1, keepdims=True))
        weights, more = weigh(scores, highest)
        shrink = jnp.exp2((before - highest) * scale)
        peak[head, lines] = highest
        mass[head, lines] = mass[head, lines] * shrink + more
        blend[head, lines] = blend[head, lines] * shrink + jnp.dot(
            weights, values, preferred_element_type=jnp.float32
        )

    def query_of(group, j):
        return query[:, pl.ds(pl.multiple_of((group * couple + j) * HDIM, HDIM), HDIM)]

    groups = heads // couple

    def diagonal(group):
        block = text[...].reshape(rows, 2 * HDIM)
        lower = lax.broadcasted_iota(jnp.int32, (rows, rows), 0) >= lax.broadcasted_iota(
            jnp.int32, (rows, rows), 1
        )
        several = [group * couple + j for j in range(couple)]
        scores = [score(query_of(group, j), block[:, :HDIM]) + covered[here, :1, :] for j in range(couple)]
        scores = [jnp.where(lower, part, lowest) for part in scores]
        tops = [jnp.max(part, axis=1, keepdims=True) for part in scores]
        weighed = [weigh(part, top) for part, top in zip(scores, tops)]
        products = [
            jnp.dot(weights, block[:, HDIM:], preferred_element_type=jnp.float32) for weights, _ in weighed
        ]
        for head, top, (_, more), product in zip(several, tops, weighed, products):
            peak[head] = top
            mass[head] = more
            blend[head] = product

    def earlier(group, owner):
        block = keys_of(owner)
        keys, values, bias = block[:, :HDIM], block[:, HDIM:], covered[owner, :1, :]
        for j in range(couple):
            queries_now = query_of(group, j)
            for line in range(0, rows, strip):
                lines = slice(line, line + strip)
                fold(group * couple + j, lines, score(queries_now[lines], keys) + bias, values)

    def vision_rows():
        for part in range(parts):
            frames.settle(part)
        frames.finish()
        for copy in keep:
            copy.wait()
        for copy in loads:
            copy.wait()
        q_total, k_total = None, None
        for part in range(parts):
            lines = jnp.concatenate([held[f, part] for f in range(frame_count)], axis=0)
            slab = slice(part * span, (part + 1) * span)
            q_part = jnp.dot(lines, q_held[slab], preferred_element_type=jnp.float32)
            k_part = jnp.dot(lines, k_held[slab], preferred_element_type=jnp.float32)
            q_total = q_part if part == 0 else q_total + q_part
            k_total = k_part if part == 0 else k_total + k_part
        turn, slide = cosine[...], sine_part[...]

        def turned(values):
            return values * turn + pltpu.roll(values, HDIM // 2, 1) * slide

        columns = [turned(q_total[:, c : c + HDIM]) for c in range(0, queries, HDIM)]
        columns += [turned(k_total[:, :HDIM]), k_total[:, HDIM:]]
        pieces, tall = mine.shape[:2]
        for i, values in enumerate(columns):
            for piece in range(pieces):
                mine[piece, :, i * HDIM : (i + 1) * HDIM] = values[
                    piece * tall : (piece + 1) * tall
                ].astype(mine.dtype)
        visions.start()
        pltpu.make_async_copy(mine, vision.at[here], own.at[2]).start()

    units = groups * seq_count
    events = {}

    def at(unit, action):
        events.setdefault(min(unit, units - 1), []).append(action)

    for part in range(parts):
        at([0, 1, 2, 3][part] if part < 4 else 3, functools.partial(frames.relay, part))
    stride = 2 * groups
    for step in range(texts.steps):
        at(groups - 1 + stride * step, functools.partial(texts.advance, step))
    at(groups + 2, vision_rows)
    for step in range(visions.steps):
        at(groups + 5 + 3 * step, functools.partial(visions.advance, step))

    def body(unit, carry):
        turn_of, group = lax.div(unit, groups), lax.rem(unit, groups)
        far, odd = lax.div(turn_of + 1, 2), lax.rem(turn_of, 2)
        owner = ring_index(
            lax.rem(ring.here + far * (1 - 2 * odd) + 2 * seq_count, seq_count), seq_count
        )

        @pl.when(turn_of == 0)
        def _():
            diagonal(group)

        @pl.when((turn_of > 0) & (owner < here))
        def _():
            earlier(group, owner)

        for index, actions in sorted(events.items()):

            def act(actions=actions):
                for action in actions:
                    action()

            pl.when(unit == index)(act)
        return carry

    lax.fori_loop(0, units, body, 0)
    pltpu.make_async_copy(mine, vision.at[here], own.at[2]).wait()

    both = vision[...].reshape(total, queries + 2 * HDIM)
    vision_keys, vision_values = both[:, queries : queries + HDIM], both[:, queries + HDIM :]
    places = here * rows + lax.broadcasted_iota(jnp.int32, (rows, 1), 0)
    for head in range(heads):
        for line in range(0, rows, strip):
            lines = slice(line, line + strip)
            scores = score(query[lines, head * HDIM : (head + 1) * HDIM], vision_keys)
            fold(head, lines, jnp.where(spots[...] <= places[lines], scores, lowest), vision_values)

    picked = jnp.dot(select[...], both[:, :queries], preferred_element_type=jnp.float32).astype(jnp.bfloat16)
    stacked = jnp.concatenate([picked[:, c : c + HDIM] for c in range(0, queries, HDIM)], axis=0)
    spot = jnp.concatenate([locate[...]] * heads, axis=0)

    def add(state, scores, values):
        before, amount, mixed = state
        highest = jnp.maximum(before, jnp.max(scores, axis=1, keepdims=True))
        weights, more = weigh(scores, highest)
        shrink = jnp.exp2((before - highest) * scale)
        mixed = mixed * shrink + jnp.dot(weights, values, preferred_element_type=jnp.float32)
        return highest, amount * shrink + more, mixed

    tall = stacked.shape[0]
    state = (
        jnp.full((tall, 1), lowest, jnp.float32),
        jnp.zeros((tall, 1), jnp.float32),
        jnp.zeros((tall, HDIM), jnp.float32),
    )
    seen = (spots[...] - here * rows).astype(jnp.float32)
    state = add(state, jnp.where(seen <= spot, score(stacked, vision_keys), lowest), vision_values)
    block = text[...].reshape(rows, 2 * HDIM)
    column = lax.broadcasted_iota(jnp.int32, (1, rows), 1).astype(jnp.float32)
    scores = score(stacked, block[:, :HDIM]) + covered[here, :1, :]
    state = add(state, jnp.where(column <= spot, scores, lowest), block[:, HDIM:])

    def past(owner, now):
        block = keys_of(owner)
        return add(now, score(stacked, block[:, :HDIM]) + covered[owner, :1, :], block[:, HDIM:])

    _, amount, mixed = lax.fori_loop(0, here, past, state)
    mixed = (mixed / amount).astype(jnp.bfloat16)
    picked = jnp.concatenate([mixed[h * slots : (h + 1) * slots] for h in range(heads)], axis=1)
    column = lax.broadcasted_iota(jnp.int32, (slots, rows), 1).astype(jnp.float32)
    spread = jnp.where(column == locate[...], 1.0, 0.0).astype(jnp.bfloat16)
    back = (((0,), (0,)), ((), ()))
    moved = lax.dot_general(spread, picked, back, preferred_element_type=jnp.float32)
    taken = lax.dot_general(
        spread, jnp.ones((slots, HDIM), jnp.bfloat16), back, preferred_element_type=jnp.float32
    )
    for head in range(heads):
        columns = slice(head * HDIM, (head + 1) * HDIM)
        kept = blend[head] / mass[head]
        result[:, columns] = jnp.where(taken > 0.5, moved[:, columns], kept).astype(result.dtype)
    texts.finish()
    visions.finish()


def finish(tokens, text, query, covered, spots, tables, query_weight, keyvalue_weight, seq_count, frame_count, collective):
    parts, share, span = tokens.shape
    lines = frame_count * share
    rows, queries = query.shape
    heads = queries // HDIM
    width = queries + keyvalue_weight.shape[1]
    slots = frame_count * -(-3 * share // 2)
    text = text.reshape(2, -1, text.shape[1])
    mine = (2, lines // 2, width)
    cosine, sine_part = tables
    return pl.pallas_call(
        functools.partial(finish_kernel, seq_count, frame_count),
        in_specs=[VMEM] * 5 + [ANY] * 2 + [VMEM] * 2,
        out_specs=VMEM,
        out_shape=jax.ShapeDtypeStruct((rows, queries), jnp.bfloat16),
        scratch_shapes=[
            pltpu.VMEM((frame_count,) + tokens.shape, tokens.dtype),
            pltpu.VMEM(query_weight.shape, query_weight.dtype),
            pltpu.VMEM(keyvalue_weight.shape, keyvalue_weight.dtype),
            pltpu.VMEM(mine, text.dtype),
            pltpu.VMEM((seq_count,) + text.shape, text.dtype),
            pltpu.VMEM((seq_count,) + mine, text.dtype),
            pltpu.VMEM((heads, rows, 1), jnp.float32),
            pltpu.VMEM((heads, rows, 1), jnp.float32),
            pltpu.VMEM((heads, rows, HDIM), jnp.float32),
            pltpu.VMEM((slots, seq_count * lines), jnp.bfloat16),
            pltpu.VMEM((slots, 1), jnp.float32),
            pltpu.SemaphoreType.DMA((2, parts)),
        ]
        + frame_sems(frame_count, parts)
        + ring_sems(seq_count, 2) * 2
        + [pltpu.SemaphoreType.DMA((3,))],
        compiler_params=comm_params(collective),
    )(tokens, text, query, covered, spots, query_weight, keyvalue_weight, cosine, sine_part)


def scatter_kernel(
    count, frame_count, hidden, weight, gain, text, near, qw, kw, cosine, sine_part, spots,
    out, q_out, pair_out, covered, *scratch
):
    held, part, stage, land, q_held, k_held, early, late, sums, load, send, recv, fsend, frecv, own = scratch
    ring = Ring(count)
    width = weight.shape[1]
    pieces = held.shape[0]
    span = width // pieces
    share = out.shape[1]
    order = [piece for pair in zip(range(pieces // 2), range(pieces // 2, pieces)) for piece in pair]
    loads = {
        piece: pltpu.make_async_copy(
            weight.at[:, pl.ds(piece * span, span)], held.at[piece], load.at[piece]
        )
        for piece in order
    }
    for piece in order:
        loads[piece].start()
    extra = [
        pltpu.make_async_copy(near, early, own.at[0]),
        pltpu.make_async_copy(qw, q_held, own.at[1]),
        pltpu.make_async_copy(kw, k_held, own.at[2]),
    ]
    for copy in extra:
        copy.start()
    parts, tall, depth = early.shape[1:]
    last = text.at[pl.ds(text.shape[0] - late.shape[1], late.shape[1])]
    frames = FrameGather(frame_count, last, late, fsend, frecv, late.shape[1])
    greet([ring.left, ring.right] + frames.partners())
    frames.start()
    aside = pltpu.make_async_copy(last, late.at[frames.me], own.at[3])
    aside.start()
    forward = [piece < pieces // 2 for piece in range(pieces)]

    def hop(piece, step):
        return remote(
            stage.at[piece, step],
            land.at[piece, step],
            send.at[piece, step],
            recv.at[piece, step],
            ring.right if forward[piece] else ring.left,
        )

    for piece in order:
        loads[piece].wait()
        product = jnp.dot(hidden[...], held[piece], preferred_element_type=jnp.float32)
        for i in range(count):
            part[piece, i] = product[i * share : (i + 1) * share]
        first = ring.index(-1 if forward[piece] else 1)
        stage[piece, 0] = part[piece, first].astype(jnp.bfloat16)
        hop(piece, 0).start()
    sums[...] = jnp.zeros_like(sums)
    slabs = 8
    slab = depth // slabs
    queries = qw.shape[1]

    def project(source, spot, index):
        columns = pl.ds(pl.multiple_of(index * slab, slab), slab)
        rows = source[:, :, :, columns].reshape(-1, slab)
        count_rows = rows.shape[0]
        sums[spot, :, :queries] += jnp.dot(rows, q_held[columns, :], preferred_element_type=jnp.float32)
        sums[spot, :, queries:] += jnp.dot(rows, k_held[columns, :], preferred_element_type=jnp.float32)

    def advance(step, group):
        for piece in group:
            hop(piece, step - 1).wait_recv()
            owner = ring.index(-1 - step if forward[piece] else 1 + step)
            total = land[piece, step - 1].astype(jnp.float32) + part[piece, owner]
            stage[piece, step] = total.astype(jnp.bfloat16)
            hop(piece, step).start()

    def cover(block):
        shape = (covered.shape[2], spots.shape[1])
        keys = block * shape[0] + lax.broadcasted_iota(jnp.int32, shape, 0)
        hits = (keys == spots[...]).astype(jnp.float32).astype(jnp.bfloat16)
        total = lax.dot_general(
            jnp.ones((covered.shape[1], shape[1]), jnp.bfloat16),
            hits,
            (((1,), (1,)), ((), ())),
            preferred_element_type=jnp.float32,
        )
        covered[block] = jnp.where(total > 0.5, lowest, 0.0)

    groups = [order[:2], order[2:]]
    turn_over = 1 + slabs // 2

    def opening(step, carry):
        for i, group in enumerate(groups):
            advance(step, group)
            if i == 0:

                @pl.when(step == 1)
                def _():
                    for copy in extra:
                        copy.wait()

            project(early, 0, 2 * (step - 1) + i)
            for block in range(count // slabs):
                cover((2 * (step - 1) + i) * (count // slabs) + block)

        @pl.when(step <= late.shape[1])
        def _():
            frames.relay(step - 1)

        return carry

    lax.fori_loop(1, turn_over, opening, 0)
    aside.wait()
    for piece in range(late.shape[1]):
        frames.settle(piece)
    each = -(-slabs // (2 * (count - 1 - turn_over)))

    def closing(step, carry):
        for i, group in enumerate(groups):
            advance(step, group)
            unit = 2 * (step - turn_over) + i
            start = jnp.minimum(unit * each, slabs)
            stop = jnp.minimum(start + each, slabs)

            def fold(index, inner):
                project(late, 1, index)
                return inner

            lax.fori_loop(start, stop, fold, 0)
        return carry

    lax.fori_loop(turn_over, count - 1, closing, 0)
    block = 2 * parts * tall
    for f in range(frame_count):
        for spot in range(2):
            source = slice(f * parts * tall, (f + 1) * parts * tall)
            begin = f * block + spot * parts * tall
            target = slice(begin, begin + parts * tall)
            turn, slide = cosine[target], sine_part[target]
            for c in range(0, queries + HDIM, HDIM):
                values = sums[spot, source, c : c + HDIM]
                values = (values * turn + pltpu.roll(values, HDIM // 2, 1) * slide).astype(q_out.dtype)
                if c < queries:
                    q_out[target, c : c + HDIM] = values
                else:
                    pair_out[target, :HDIM] = values
            pair_out[target, HDIM:] = sums[spot, source, queries + HDIM :].astype(pair_out.dtype)
    here = ring.index(0)
    squares = jnp.zeros((share, 1), jnp.float32)
    for piece in order:
        hop(piece, count - 2).wait_recv()
        total = land[piece, count - 2].astype(jnp.float32) + part[piece, here]
        total = total.astype(jnp.bfloat16).astype(jnp.float32)
        part[piece, here] = total
        squares += jnp.sum(total * total, axis=1, keepdims=True)
    factor = lax.rsqrt(squares / width + epsilon)
    for piece in order:
        columns = slice(piece * span, (piece + 1) * span)
        out[piece] = (part[piece, here] * factor * gain[columns].reshape(1, -1)).astype(out.dtype)

    def drain(step, carry):
        for piece in order:
            hop(piece, step).wait_send()
        return carry

    lax.fori_loop(0, count - 1, drain, 0)
    frames.finish()


def scatter(hidden, weight, gain, text, near, query_weight, keyvalue_weight, tables, spots, count, frame_count, collective):
    rows, depth = hidden.shape
    width = weight.shape[1]
    share = rows // count
    pieces = 4
    span = width // pieces
    parts, tall = text.shape[:2]
    tokens = frame_count * parts * tall
    queries, pairs = query_weight.shape[1], keyvalue_weight.shape[1]
    left = parts - near.shape[1]
    cosine, sine_part = tables
    return pl.pallas_call(
        functools.partial(scatter_kernel, count, frame_count),
        in_specs=[VMEM, ANY, VMEM, VMEM, ANY, ANY, ANY, VMEM, VMEM, VMEM],
        out_specs=[VMEM, VMEM, VMEM, VMEM],
        out_shape=[
            jax.ShapeDtypeStruct((pieces, share, span), jnp.bfloat16),
            jax.ShapeDtypeStruct((tokens, queries), jnp.bfloat16),
            jax.ShapeDtypeStruct((tokens, pairs), jnp.bfloat16),
            jax.ShapeDtypeStruct((count, 8, tokens), jnp.float32),
        ],
        scratch_shapes=[
            pltpu.VMEM((pieces, depth, span), jnp.bfloat16),
            pltpu.VMEM((pieces, count, share, span), jnp.float32),
            pltpu.VMEM((pieces, count - 1, share, span), jnp.bfloat16),
            pltpu.VMEM((pieces, count - 1, share, span), jnp.bfloat16),
            pltpu.VMEM(query_weight.shape, query_weight.dtype),
            pltpu.VMEM(keyvalue_weight.shape, keyvalue_weight.dtype),
            pltpu.VMEM(near.shape, near.dtype),
            pltpu.VMEM((frame_count, left) + text.shape[1:], text.dtype),
            pltpu.VMEM((2, tokens // 2, queries + pairs), jnp.float32),
            pltpu.SemaphoreType.DMA((pieces,)),
            pltpu.SemaphoreType.DMA((pieces, count - 1)),
            pltpu.SemaphoreType.DMA((pieces, count - 1)),
        ]
        + frame_sems(frame_count, left)
        + [pltpu.SemaphoreType.DMA((4,))],
        compiler_params=pltpu.CompilerParams(
            collective_id=collective, has_side_effects=True, vmem_limit_bytes=63 * 1024 * 1024
        ),
    )(hidden, weight, gain, text, near, query_weight, keyvalue_weight, cosine, sine_part, spots)


def turns(positions):
    lanes = jnp.arange(HDIM, dtype=jnp.int32)
    inverse = rope_base ** (-2.0 * (lanes % (HDIM // 2)).astype(jnp.float32) / HDIM)
    angles = positions.astype(jnp.float32)[:, None] * inverse[None, :]
    return jnp.cos(angles), jnp.where(lanes < HDIM // 2, -1.0, 1.0) * jnp.sin(angles)


def local(
    patches,
    vit_gain,
    vision_qkv,
    vision_out,
    video_ids,
    merge_gain,
    merge_up,
    merge_down,
    vision_pos,
    text_embed,
    llm_gain,
    query_weight,
    keyvalue_weight,
):
    frame_index = lax.axis_index("frame")
    seq_index = lax.axis_index("seq")
    frame_count = lax.axis_size("frame")
    seq_count = lax.axis_size("seq")
    patch_rows = patches.shape[0]
    merge_hidden, text_own, text_near = encode(
        patches, vit_gain, vision_qkv, video_ids, vision_out, text_embed, llm_gain, merge_gain, merge_up,
        seq_count, frame_count, 1,
    )
    seq_block = text_embed.shape[0] * frame_count
    share = patch_rows // (4 * seq_count)
    token_pos = vision_pos.reshape(frame_count, seq_count, share).transpose(1, 0, 2)
    here = lax.dynamic_index_in_dim(token_pos, seq_index, 0, keepdims=False).reshape(-1)
    spots = token_pos.reshape(1, -1)
    vision_normed, text_query, text_pair, covered = scatter(
        merge_hidden, merge_down, llm_gain, text_own, text_near, query_weight, keyvalue_weight,
        turns(seq_index * seq_block + jnp.arange(seq_block, dtype=jnp.int32)), spots,
        seq_count, frame_count, 3,
    )
    return finish(
        vision_normed, text_pair, text_query, covered, spots, turns(here), query_weight, keyvalue_weight,
        seq_count, frame_count, 4,
    )


def solution(mesh):
    return jax.shard_map(
        local,
        mesh=mesh,
        in_specs=(
            P("frame", None),
            P(),
            P(None, "seq"),
            P("seq", None),
            P(),
            P(),
            P(None, "seq"),
            P("seq", None),
            P(),
            P(("seq", "frame"), None),
            P(),
            P(None, "frame"),
            P(None, "frame"),
        ),
        out_specs=P("seq", "frame"),
        check_vma=False,
    )
```
